32 devices in a mesh: sub: 8 (over z, x), rng: 4 (over y, core).
Axes of the slice: x: 2, y: 2, z: 4, core: 2. Of those that a mesh axis runs over, the one named last changes fastest.
Arguments:
- echoes: bfloat16 [2, 4, 1024, 2048], P(None, None, 'sub', 'rng'), may hold values from -6 to 6
- steering: bfloat16 [2, 256, 256], replicated, may hold values from -0.25 to 0.25
- sub_map: int32 [8], replicated, may hold values from 0 to 7, each once
- band_offset: int32 [8, 3, 2, 256], P('sub'), may hold values from 0 to 248, as said below
- interp_weight: bfloat16 [8, 3, 2, 8, 256], P('sub'), may hold values from -1.5 to 1.5
- range_frac: float32 [8, 3, 2, 256], P('sub'), may hold values from 0 to 1
- phase_rate: float32 [8, 3, 2, 256], P('sub'), may hold values from -40 to 40
Outputs:
- image: bfloat16 [2, 4096, 2048], P(None, 'rng', 'sub')
The draws below stay inside these ranges and needn't reach their ends.
Inputs may be any that keep to these rules, and one draw needn't show every extreme that they name: `sub_map`: each number appears once. `band_offset`: an entry for section i and segment s lies in h * 128 to (h + 1) * 128 - 8, where h is bit s of i.
All inputs are finite; a program needn't handle non-finite values.
Results may differ from the reference program's by a relative error of at most 0.0062.
Values may be sent and summed in bfloat16 or wider, within the bound.
No kernel may reach another device: no remote copies, remote signals or barrier semaphores. Data moves between devices by JAX's collectives and lax.ppermute only.
A program may use at most 64 MiB of HBM per device.

```python
import jax
import jax.numpy as jnp
from jax import lax

PD = 256
RD = 1024
A = 256
TAPS = 8
SEGMENTS = 3
PULSES = 2048
RANGE = 4096
N_SUB = 8
N_RNG = 4


def draw_band_offset(key, part):
    within = jax.random.randint(jax.random.fold_in(key, 11), (N_SUB, SEGMENTS, 2, A), 0, A // 2 - TAPS + 1, dtype=jnp.int32)
    device = jnp.arange(N_SUB, dtype=jnp.int32)[:, None, None, None]
    doubling = jnp.arange(SEGMENTS, dtype=jnp.int32)[None, :, None, None]
    parity = jnp.bitwise_and(jnp.right_shift(device, doubling), 1)
    return within + parity * (A // 2)


def block_levels(own_key, shape, split, least, largest):
    factor_of = 1.0
    for dim, parts in split:
        draws = jax.random.uniform(jax.random.fold_in(jax.random.fold_in(own_key, 6), dim), (parts,), jnp.float32, least / len(split), largest / len(split))
        factor_of = factor_of * jnp.repeat(jnp.exp(draws), shape[dim] // parts).reshape((-1,) + (1,) * (len(shape) - 1 - dim))
    return factor_of


def bell_draw(key, shape, width, limit, cuts=(), kind=jnp.bfloat16):
    level = block_levels(key, shape, cuts, -0.22, 0.18) if cuts else 1.0
    drawn = jax.random.normal(key, shape, jnp.float32) * width * level
    return jnp.minimum(jnp.maximum(drawn, -limit), limit).astype(kind)


def setup_inputs(seed: int = 0) -> dict:
    splits = jax.random.split(jax.random.key(seed), 8)
    return {
        "echoes": bell_draw(splits[0], (2, N_RNG, RD, PULSES), 1.0, 6.0, ((2, 8), (3, 4))),
        "steering": bell_draw(splits[1], (2, A, PD), (2 * PD) ** -0.5, 0.25),
        "sub_map": jax.random.permutation(splits[2], N_SUB).astype(jnp.int32),
        "band_offset": draw_band_offset(jax.random.fold_in(splits[7], 71), 0),
        "interp_weight": bell_draw(splits[4], (N_SUB, SEGMENTS, 2, TAPS, A), 0.25, 1.5, ((0, 8),)),
        "range_frac": jnp.clip(1.0 * jax.random.uniform(splits[5], (N_SUB, SEGMENTS, 2, A), jnp.float32) ** block_levels(splits[5], (N_SUB, SEGMENTS, 2, A), ((0, 8),), -0.2, 0.2), 0.0, 1.0),
        "phase_rate": jnp.clip(jax.random.uniform(splits[6], (N_SUB, SEGMENTS, 2, A), jnp.float32, -40.0, 40.0) * block_levels(splits[6], (N_SUB, SEGMENTS, 2, A), ((0, 8),), -0.4, 0.0), -40.0, 40.0),
    }


def band_matrix(offset, weight, window_base, window_width):
    window_rows = jnp.arange(window_width, dtype=jnp.int32)[None, :, None] + window_base
    tap_index = jnp.arange(weight.shape[0], dtype=jnp.int32)[:, None, None]
    matched = window_rows == offset[None, None, :] + tap_index
    spread = jnp.where(matched, weight[:, None, :].astype(jnp.float32), jnp.float32(0.0))
    return jnp.sum(spread, axis=0).astype(jnp.bfloat16)


def beamform(pulses, steering):
    real_part = jnp.dot(pulses[0], steering[0].T, preferred_element_type=jnp.float32) - jnp.dot(pulses[1], steering[1].T, preferred_element_type=jnp.float32)
    imag_part = jnp.dot(pulses[0], steering[1].T, preferred_element_type=jnp.float32) + jnp.dot(pulses[1], steering[0].T, preferred_element_type=jnp.float32)
    return jnp.stack([real_part, imag_part]).astype(jnp.bfloat16)


def rotate(interp, shifted, fraction, spin_rate, positions):
    blended = (1.0 - fraction) * interp + fraction * shifted
    phase_angle = positions[:, None] * spin_rate[None, :]
    cosine = jnp.cos(phase_angle)
    sine_part = jnp.sin(phase_angle)
    return cosine * blended[0] - sine_part * blended[1], sine_part * blended[0] + cosine * blended[1]


def child_term(child_image, offset, weight, fraction, spin_rate, positions):
    angle_count = child_image.shape[2]
    matrix = band_matrix(offset, weight, 0, angle_count)
    interp = jnp.dot(child_image.reshape(2 * RANGE, angle_count), matrix, preferred_element_type=jnp.float32).reshape(2, RANGE, angle_count)
    shifted = jnp.concatenate([interp[:, 1:, :], jnp.zeros((2, 1, angle_count), jnp.float32)], axis=1)
    return rotate(interp, shifted, fraction, spin_rate, positions)


def reference(echoes, steering, sub_map, band_offset, interp_weight, range_frac, phase_rate):
    blocks = echoes.reshape(2, N_RNG, RD, N_SUB, PD)
    devices = jnp.arange(N_SUB, dtype=jnp.int32)

    def initial(device):
        pulses = lax.dynamic_index_in_dim(blocks, sub_map[device], 3, keepdims=False).reshape(2, RANGE, PD)
        return beamform(pulses, steering)

    images = lax.map(initial, devices)
    positions = jnp.arange(RANGE, dtype=jnp.int32).astype(jnp.float32) / float(RANGE)
    for doubling in range(SEGMENTS):
        def merging(device):
            lower_index = device - jnp.bitwise_and(device, 1 << doubling)
            upper_index = lower_index + (1 << doubling)
            lower_re, lower_im = child_term(images[lower_index], band_offset[device, doubling, 0], interp_weight[device, doubling, 0], range_frac[device, doubling, 0], phase_rate[device, doubling, 0], positions)
            upper_re, upper_im = child_term(images[upper_index], band_offset[device, doubling, 1], interp_weight[device, doubling, 1], range_frac[device, doubling, 1], phase_rate[device, doubling, 1], positions)
            return jnp.stack([lower_re + upper_re, lower_im + upper_im]).astype(jnp.bfloat16)

        images = lax.map(merging, devices)
    return images.transpose(1, 2, 0, 3).reshape(2, RANGE, N_SUB * A)
```

```python
import functools

import jax
import jax.numpy as jnp
from jax import lax
from jax.experimental import pallas as pl
from jax.experimental.pallas import tpu as pltpu
from jax.sharding import PartitionSpec as P


HALO = 8
PACK_ROWS = 16
MIB = 1 << 20


def exchanged(block, axis, mask):
    count = lax.axis_size(axis)
    return lax.ppermute(block, axis, [(source, source ^ mask) for source in range(count)])


def split_parts(value, count):
    parts = []
    rest = value
    for _ in range(count):
        part = lax.reduce_precision(rest, 8, 7)
        parts.append(part)
        rest = rest - part
    return parts


def packed_parameters(offset, weight, fraction, rate, member, half):
    segments, _, taps, angles = weight.shape
    bit = jnp.right_shift(member, jnp.arange(segments, dtype=jnp.int32)) & 1
    inside = (offset - (bit * half)[:, None, None]).astype(jnp.float32)
    rows = [inside] + split_parts(fraction, 2) + split_parts(rate, 3)
    rows += [jnp.zeros_like(inside)] * (PACK_ROWS - taps - len(rows))
    tail = jnp.stack(rows, axis=2).astype(jnp.bfloat16)
    return jnp.concatenate([weight, tail], axis=2).reshape(segments * 2, PACK_ROWS, angles)


def table_kernel(group, terms, taps, half, lines, total_range, meta, *refs):
    pieces, (bands, waves, table) = refs[:group], refs[group:]
    angles = bands.shape[-1]
    member, first_row = meta[0], meta[1]
    for mask in range(group):
        table[member ^ mask] = pieces[mask][...]
    sub_rows = lax.broadcasted_iota(jnp.int32, (8, 128), 0)

    def entry(index, carry):
        section, term = index // terms, index % terms
        for part in range(angles // 128):
            lanes = pl.ds(part * 128, 128)
            weight = table[section, term, 0:taps, lanes].astype(jnp.float32)
            tail = table[section, term, taps:PACK_ROWS, lanes].astype(jnp.float32)
            offset = tail[0:1].astype(jnp.int32)
            fraction = tail[1:2] + tail[2:3]
            rate = tail[3:4] + tail[4:5] + tail[5:6]
            near, far = weight * (1.0 - fraction), weight * fraction
            for block in range(half // 16):
                spread = []
                for source in (near, far):
                    pair = []
                    for step in range(2):
                        tap = sub_rows + (block * 16 + step * 8) - offset
                        picked = jnp.take_along_axis(source, tap & (taps - 1), axis=0)
                        pair.append(jnp.where((tap >= 0) & (tap < taps), picked, 0.0))
                    spread.append(jnp.concatenate(pair, axis=0).astype(jnp.bfloat16))
                bands[section, term, block * 16 : (block + 1) * 16, lanes] = spread[0]
                bands[section, term, half + block * 16 : half + (block + 1) * 16, lanes] = spread[1]
            position = (first_row + sub_rows).astype(jnp.float32) / float(total_range)
            angle = position * rate
            wave_re, wave_im = jnp.cos(angle), jnp.sin(angle)
            four_re = wave_re[4:5] * wave_re[0:1] + wave_im[4:5] * wave_im[0:1]
            four_im = wave_im[4:5] * wave_re[0:1] - wave_re[4:5] * wave_im[0:1]
            eight_re = four_re * four_re - four_im * four_im
            eight_im = 2.0 * four_re * four_im
            for block in range(lines // 8):
                waves[section, term, 0, block * 8 : (block + 1) * 8, lanes] = wave_re
                waves[section, term, 1, block * 8 : (block + 1) * 8, lanes] = wave_im
                wave_re, wave_im = (
                    wave_re * eight_re - wave_im * eight_im,
                    wave_re * eight_im + wave_im * eight_re,
                )
        return carry

    lax.fori_loop(0, group * terms, entry, 0)


def merge_kernel(group, segments, rows, lines, pulse_count, sources, meta, *refs):
    blocks = refs[:sources]
    edge, steering, bands, waves = refs[sources : sources + 4]
    outs = refs[sources + 4 : sources + 4 + group]
    first, even, odd = refs[sources + 4 + group :]
    angles = steering.shape[1]
    half = angles // 2
    member = meta[0]
    per_source = group // sources
    real_weight, imag_weight = steering[0], steering[1]
    negated = -imag_weight

    def product(left, right):
        return lax.dot_general(
            left, right, (((1,), (1,)), ((), ())), preferred_element_type=jnp.float32
        )

    def formed(re_part, im_part):
        return (
            product(re_part, real_weight) + product(im_part, negated),
            product(re_part, imag_weight) + product(im_part, real_weight),
        )

    edge_parts = [[], []]
    for source in range(sources):
        for piece in range(per_source):
            columns = slice(piece * pulse_count, (piece + 1) * pulse_count)
            target = meta[2 + source * per_source + piece]
            if len(blocks[source].shape) == 4:
                parts = [blocks[source][c, 0, :, columns] for c in range(2)]
            else:
                parts = [blocks[source][c, :, columns] for c in range(2)]
            for c, value in enumerate(formed(*parts)):
                first[target, c, 0:rows, :] = value
            for c in range(2):
                edge_parts[c].append(edge[source, c, :, columns])
    edges = formed(*[jnp.concatenate(parts, axis=0) for parts in edge_parts])
    for index in range(group):
        target = meta[2 + group + index]
        for c in range(2):
            first[target, c, rows : rows + HALO, :] = edges[c][index * HALO : (index + 1) * HALO]
            first[target, c, rows + HALO : lines, :] = jnp.zeros(
                (lines - rows - HALO, angles), jnp.float32
            )

    def put(store, section, c, value):
        here = value.astype(jnp.bfloat16)
        below = pltpu.roll(value, lines - 1, 0).astype(jnp.bfloat16)
        for window in range(2):
            columns = slice(window * half, (window + 1) * half)
            store[section, window, c * lines : (c + 1) * lines, 0:half] = here[:, columns]
            store[section, window, c * lines : (c + 1) * lines, half:angles] = below[:, columns]

    def start(section, carry):
        for c in range(2):
            put(even, section, c, first[section, c])
        return carry

    lax.fori_loop(0, group, start, 0)

    def merged(store, section, segment):
        low = section & ~(1 << segment)
        window = (section >> segment) & 1
        total_re = total_im = None
        for child in range(2):
            term = segment * 2 + child
            value = jnp.dot(
                store[low | (child << segment), window],
                bands[section, term],
                preferred_element_type=jnp.float32,
            )
            re_part, im_part = value[:lines], value[lines:]
            wave_re, wave_im = waves[section, term, 0], waves[section, term, 1]
            new_re = wave_re * re_part - wave_im * im_part
            new_im = wave_im * re_part + wave_re * im_part
            total_re = new_re if child == 0 else total_re + new_re
            total_im = new_im if child == 0 else total_im + new_im
        return total_re, total_im

    stores = (even, odd)
    for segment in range(segments - 1):
        source, target = stores[segment % 2], stores[(segment + 1) % 2]

        def step(section, carry, segment=segment, source=source, target=target):
            for c, value in enumerate(merged(source, section, segment)):
                put(target, section, c, value)
            return carry

        lax.fori_loop(0, group, step, 0)
    for mask in range(group):
        values = merged(stores[(segments - 1) % 2], member ^ mask, segments - 1)
        for c, value in enumerate(values):
            outs[mask][c] = value[:rows].astype(jnp.bfloat16)


def on_device(echoes, steering, sub_map, band_offset, interp_weight, range_frac, phase_rate):
    slabs = lax.axis_size("rng")
    subs = lax.axis_size("sub")
    segments, taps = interp_weight.shape[1], interp_weight.shape[3]
    group = 1 << segments
    groups = subs // group
    angles, pulse_count = steering.shape[1], steering.shape[2]
    half = angles // 2
    terms = segments * 2
    slab = lax.axis_index("rng")
    sub = lax.axis_index("sub")
    member = sub % group
    range_rows = echoes.shape[2] * subs
    rows = range_rows // group
    lines = rows + 2 * HALO

    received = []
    for mask in range(1, slabs):
        outgoing = lax.dynamic_index_in_dim(echoes, slab ^ mask, 1, keepdims=False)
        received.append(exchanged(outgoing, "rng", mask))

    own_pack = packed_parameters(
        band_offset[0], interp_weight[0], range_frac[0], phase_rate[0], member, half
    )
    packs = [own_pack] + [exchanged(own_pack, "sub", mask) for mask in range(1, group)]

    below_slab = slab + jnp.where(member == group - 1, 1, 0)
    numbers = jnp.arange(group, dtype=jnp.int32)
    own_rows = lax.dynamic_index_in_dim(echoes, slab, 1, keepdims=False)
    if groups == 1:
        blocks = [echoes] + received
        own_spec = pl.BlockSpec(
            (2, 1, rows, echoes.shape[3]), lambda _, meta: (0, meta[2 + 2 * group], 0, 0)
        )
        edge_rows = jnp.stack([block[:, :HALO] for block in [own_rows] + received])
        place = jnp.sum(
            jnp.where(sub_map[None, :] == numbers[:, None], numbers[None, :], 0), axis=1
        )
        per_slab = group // slabs
        masks, pieces = numbers // per_slab, numbers % per_slab
        main_place = place[(slab ^ masks) * per_slab + pieces]
        edge_place = place[(jnp.minimum(below_slab, slabs - 1) ^ masks) * per_slab + pieces]
    else:
        ordered = jnp.zeros((slabs,) + own_rows.shape, own_rows.dtype)
        for mask, block in enumerate([own_rows] + received):
            ordered = lax.dynamic_update_index_in_dim(ordered, block, slab ^ mask, 0)
        every = jnp.moveaxis(ordered, 0, 2).reshape(2, -1, subs, pulse_count)
        every = jnp.take(every, sub_map, axis=2)
        every = lax.ppermute(
            every,
            "sub",
            [(old, (old % groups) * group + old // groups) for old in range(subs)],
        ).reshape(2, -1, groups, group * pulse_count)
        lanes = [[g * group + m for g in range(groups)] for m in range(group)]
        every = lax.all_to_all(every, "sub", 2, 1, axis_index_groups=lanes, tiled=True)
        blocks = [every.reshape(2, rows, group * pulse_count)]
        own_spec = pl.BlockSpec(memory_space=pltpu.VMEM)
        edge_rows = blocks[0][None, :, :HALO]
        main_place = edge_place = numbers

    route = []
    for number in range(subs):
        for q in range(slabs):
            if number % group > 0:
                route.append((number * slabs + q, (number - 1) * slabs + q))
            elif q > 0:
                route.append((number * slabs + q, (number + group - 1) * slabs + q - 1))
    edge = lax.ppermute(edge_rows, ("sub", "rng"), route)

    first_row = slab * range_rows + member * rows
    meta = jnp.concatenate(
        [jnp.stack([member, first_row]), main_place, edge_place, slab[None]]
    ).astype(jnp.int32)

    whole = pl.BlockSpec(memory_space=pltpu.VMEM)
    bands, waves = pl.pallas_call(
        functools.partial(table_kernel, group, terms, taps, half, lines, slabs * range_rows),
        out_shape=(
            jax.ShapeDtypeStruct((group, terms, angles, angles), jnp.bfloat16),
            jax.ShapeDtypeStruct((group, terms, 2, lines, angles), jnp.float32),
        ),
        in_specs=[pl.BlockSpec(memory_space=pltpu.SMEM)] + [whole] * group,
        out_specs=(whole, whole),
        scratch_shapes=[pltpu.VMEM((group, terms, PACK_ROWS, angles), jnp.bfloat16)],
        compiler_params=pltpu.CompilerParams(vmem_limit_bytes=4 * MIB),
        cost_estimate=pl.CostEstimate(
            flops=4_000_000_000, bytes_accessed=20 * MIB, transcendentals=0
        ),
        name="tables",
    )(meta, *packs)

    merged = pl.pallas_call(
        functools.partial(
            merge_kernel, group, segments, rows, lines, pulse_count, len(blocks)
        ),
        grid_spec=pltpu.PrefetchScalarGridSpec(
            num_scalar_prefetch=1,
            grid=(1,),
            in_specs=[own_spec] + [whole] * (len(blocks) - 1) + [whole] * 4,
            out_specs=[whole] * group,
            scratch_shapes=[
                pltpu.VMEM((group, 2, lines, angles), jnp.float32),
                pltpu.VMEM((group, 2, 2 * lines, angles), jnp.bfloat16),
                pltpu.VMEM((group, 2, 2 * lines, angles), jnp.bfloat16),
            ],
        ),
        out_shape=[jax.ShapeDtypeStruct((2, rows, angles), jnp.bfloat16)] * group,
        compiler_params=pltpu.CompilerParams(vmem_limit_bytes=16 * MIB),
        cost_estimate=pl.CostEstimate(
            flops=6_000_000_000, bytes_accessed=24 * MIB, transcendentals=0
        ),
        name="merge",
    )(meta, *blocks, edge, steering, bands, waves)

    image = jnp.zeros((2, range_rows, angles), jnp.bfloat16)
    for mask in range(group):
        part = merged[0] if mask == 0 else exchanged(merged[mask], "sub", mask)
        image = lax.dynamic_update_slice(image, part, (0, (member ^ mask) * rows, 0))
    return image


def solution(mesh):
    in_specs = (
        P(None, None, "sub", "rng"),
        P(),
        P(),
        P("sub", None, None, None),
        P("sub", None, None, None, None),
        P("sub", None, None, None),
        P("sub", None, None, None),
    )
    return jax.shard_map(
        on_device, mesh=mesh, in_specs=in_specs, out_specs=P(None, "rng", "sub"), check_vma=False
    )
```

```python
import functools

import jax
import jax.numpy as jnp
from jax import lax
from jax.experimental import pallas as pl
from jax.experimental.pallas import tpu as pltpu
from jax.sharding import PartitionSpec as P


HALO = 8
KINDS = 6
MIB = 1 << 20
WHOLE = pl.BlockSpec(memory_space=pltpu.VMEM)
SCALARS = pl.BlockSpec(memory_space=pltpu.SMEM)
FAR = pl.BlockSpec(memory_space=pltpu.HBM)


def exchanged(block, axis, mask):
    count = lax.axis_size(axis)
    return lax.ppermute(block, axis, [(source, source ^ mask) for source in range(count)])


def params(mib):
    return pltpu.CompilerParams(vmem_limit_bytes=mib * MIB)


def cost(flops):
    return pl.CostEstimate(flops=flops, bytes_accessed=MIB, transcendentals=0)


def product(left, right):
    return (
        left[0] * right[0] - left[1] * right[1],
        left[0] * right[1] + left[1] * right[0],
    )


def pack_rows(terms, taps):
    return -(-(terms * (taps + KINDS)) // 8) * 8


def cut_kernel(slabs, segments, taps, half, echoes, offset, weight, fraction, rate, *refs):
    slices, packs = refs[:slabs], refs[slabs : slabs + 2]
    held, semaphores, small = refs[slabs + 2 : slabs + 6], refs[slabs + 6], refs[slabs + 7]
    group = 1 << segments
    member = lax.axis_index("sub") & (group - 1)
    slab = lax.axis_index("rng")
    loads = [
        pltpu.make_async_copy(source, target, small.at[index])
        for index, (source, target) in enumerate(zip((offset, weight, fraction, rate), held))
    ]
    copies = []
    for mask in range(slabs - 1, -1, -1):
        for c in range(2):
            copies.append(
                pltpu.make_async_copy(
                    echoes.at[c, slab ^ mask], slices[mask].at[c], semaphores.at[mask, c]
                )
            )
    for copy in loads + copies:
        copy.start()
    for copy in loads:
        copy.wait()
    offset, weight, fraction, rate = held
    angles = weight.shape[-1]
    for pack, chosen in ((packs[0], range(segments - 1)), (packs[1], (segments - 1,))):
        kinds = [[] for _ in range(KINDS)]
        terms = 2 * len(chosen)
        for index, segment in enumerate(chosen):
            base = ((member >> segment) & 1) * half
            kinds[0].append((offset[0, segment] - base).astype(jnp.float32))
            slot = 1
            for source, count in ((fraction, 2), (rate, 3)):
                rest = source[0, segment]
                for _ in range(count):
                    part = rest.astype(jnp.bfloat16).astype(jnp.float32)
                    kinds[slot].append(part)
                    rest = rest - part
                    slot += 1
            for child in range(2):
                term = index * 2 + child
                pack[term * taps : (term + 1) * taps, :] = weight[0, segment, child]
        rows = [piece for kind in kinds for piece in kind]
        padding = pack_rows(terms, taps) - terms * (taps + KINDS)
        if padding:
            rows.append(jnp.zeros((padding, angles), jnp.float32))
        pack[terms * taps :, :] = jnp.concatenate(rows, axis=0).astype(jnp.bfloat16)
    for copy in copies:
        copy.wait()


def table_kernel(members, terms, masks, taps, half, rows, lines, range_rows, total_range, *refs):
    steps = len(masks[0]) if masks else 0
    own, mine, theirs = refs[0], refs[1 : 1 + steps], refs[1 + steps : 1 + 2 * steps]
    bands, waves, weights, raw, dense = refs[1 + 2 * steps :]
    angles = bands.shape[-1]
    member = lax.axis_index("sub") & (members - 1)
    slab = lax.axis_index("rng")

    def fill(piece, section):
        values = piece[...].astype(jnp.float32)
        for term in range(terms):
            weights[section, term] = values[term * taps : (term + 1) * taps]
        start = terms * taps
        kind = [values[start + k * terms : start + (k + 1) * terms] for k in range(KINDS)]
        raw[section, 0] = kind[0]
        raw[section, 1] = kind[1] + kind[2]
        raw[section, 2] = kind[3] + kind[4] + kind[5]

    if masks:
        core = slab & 1
        fill(own, member)
        for side, received in ((0, mine), (1, theirs)):
            holder = core if side == 0 else 1 - core
            for step in range(steps):
                pair = [masks[c][step] if step < len(masks[c]) else 0 for c in range(2)]
                mask = jnp.where(holder == 0, pair[0], pair[1])

                @pl.when(mask != 0)
                def _(step=step, received=received, mask=mask):
                    fill(received[step], member ^ mask)

        first_row, row_step = slab * range_rows + member * rows, 0
    else:
        for section in range(members):
            fill(own, section)
        first_row, row_step = slab * range_rows, rows

    for start in range(0, members * terms, 8):
        place = slice(start, start + 8)
        sections = range(start // terms, (start + 8) // terms)

        def keep(kind, value):
            for part in range(angles // 128):
                dense[kind, part, place] = value[:, part * 128 : (part + 1) * 128]

        given = [
            jnp.concatenate([raw[section, kind] for section in sections], axis=0)
            for kind in range(3)
        ]
        keep(0, given[0])
        keep(1, given[1])
        rate = given[2]
        number = start + lax.broadcasted_iota(jnp.int32, (8, angles), 0)
        first = first_row + (number // terms) * row_step
        angle = first.astype(jnp.float32) / float(total_range) * rate
        keep(3, jnp.cos(angle))
        keep(4, jnp.sin(angle))
        angle = rate / float(total_range)
        turn = jnp.cos(angle), jnp.sin(angle)
        for power in range(5):
            keep(5 + 2 * power, turn[0])
            keep(6 + 2 * power, turn[1])
            turn = product(turn, turn)

    sub_rows = lax.broadcasted_iota(jnp.int32, (8, 128), 0)

    def entry(index, carry):
        section, term = index // terms, index % terms
        for part in range(angles // 128):
            lanes = pl.ds(part * 128, 128)

            def row(kind):
                return dense[kind, part, pl.ds(index, 1), :]

            def bands_of():
                weight = weights[section, term, :, lanes]
                offset = row(0).astype(jnp.int32)
                fraction = row(1)
                tap = sub_rows - offset
                block_of = -(tap >> 3)
                picked = jnp.take_along_axis(weight, tap & 7, axis=0)
                near, far = picked * (1.0 - fraction), picked * fraction
                for block in range(half // 16):
                    hits = [block_of == 2 * block + step for step in range(2)]
                    for source, base in ((near, 0), (far, half)):
                        pair = [jnp.where(hit, source, 0.0) for hit in hits]
                        place = slice(base + block * 16, base + (block + 1) * 16)
                        bands[section, term, place, lanes] = jnp.concatenate(pair, axis=0).astype(
                            jnp.bfloat16
                        )

            if masks:
                bands_of()
            else:
                pl.when(section == 0)(bands_of)
            wave = tuple(jnp.broadcast_to(row(3 + c), (8, 128)) for c in range(2))
            for power in range(3):
                chosen = (sub_rows >> power) & 1 == 1
                wave = product(
                    wave,
                    (
                        jnp.where(chosen, row(5 + 2 * power), 1.0),
                        jnp.where(chosen, row(6 + 2 * power), 0.0),
                    ),
                )
            eight, sixteen = (row(11), row(12)), (row(13), row(14))
            chain = [wave, product(wave, eight)]
            for block in range(lines // 8):
                wave = chain[block % 2]
                for c in range(2):
                    waves[section, term, c, block * 8 : (block + 1) * 8, lanes] = wave[c]
                chain[block % 2] = product(wave, sixteen)
        return carry

    lax.fori_loop(0, members * terms, entry, 0)


def formed(steering, re_part, im_part):
    def dot(left, right):
        return lax.dot_general(
            left, right, (((1,), (1,)), ((), ())), preferred_element_type=jnp.float32
        )

    real_weight, imag_weight = steering[0], steering[1]
    return (
        dot(re_part, real_weight) + dot(im_part, -imag_weight),
        dot(re_part, imag_weight) + dot(im_part, real_weight),
    )


def place_of(sub_map, group, slabs, slab, index):
    if slabs == 1:
        return index
    per_slab = group // slabs
    block = (slab ^ (index // per_slab)) * per_slab + index % per_slab
    place = 0
    for section in range(group):
        place = jnp.where(sub_map[section] == block, section, place)
    return place


def form_kernel(group, pulse_count, sources, sub_map, *refs):
    blocks, steering, image = refs[:sources], refs[sources], refs[sources + 1]
    half = image.shape[-1]
    per_source = group // sources
    slab = lax.axis_index("rng")
    for source in range(sources):
        for piece in range(per_source):
            columns = slice(piece * pulse_count, (piece + 1) * pulse_count)
            target = place_of(sub_map, group, sources, slab, source * per_source + piece)
            parts = [blocks[source][c, :, columns] for c in range(2)]
            for c, value in enumerate(formed(steering, *parts)):
                for window in range(2):
                    image[target, c, window] = value[:, window * half : (window + 1) * half]


def turned(values, block):
    total = None
    for value, wave in values:
        part = value[block * 16 : block * 16 + 8], value[block * 16 + 8 : block * 16 + 16]
        turn = tuple(wave[c, block * 8 : block * 8 + 8] for c in range(2))
        term = product(turn, part)
        total = term if total is None else (total[0] + term[0], total[1] + term[1])
    return total


def contracted(rows_of, lines, matrix):
    pieces = []
    for block in range(lines // 8):
        sides = []
        for start in (block * 8, block * 8 + 1):
            both = [rows_of(c, start) for c in range(2)]
            sides.append(jnp.concatenate(both, axis=0).astype(jnp.bfloat16))
        pieces.append(jnp.concatenate(sides, axis=1))
    return jnp.dot(jnp.concatenate(pieces, axis=0), matrix, preferred_element_type=jnp.float32)


def merge_kernel(group, segments, rows, pulse_count, sources, sub_map, *refs):
    image, edge, steering, bands, waves = refs[:5]
    outs, edges = refs[5 : 5 + group], refs[5 + group]
    stores = refs[6 + group :]
    half = image.shape[-1]
    member = lax.axis_index("sub") & (group - 1)
    per_source = group // sources
    below = lax.axis_index("rng")
    if sources > 1:
        below = jnp.minimum(below + jnp.where(member == group - 1, 1, 0), sources - 1)

    edge_parts = [[], []]
    for source in range(sources):
        for piece in range(per_source):
            columns = slice(piece * pulse_count, (piece + 1) * pulse_count)
            for c in range(2):
                edge_parts[c].append(edge[source, c, :, columns])
    values = formed(steering, *[jnp.concatenate(parts, axis=0) for parts in edge_parts])
    for index in range(group):
        target = place_of(sub_map, group, sources, below, index)
        for c in range(2):
            value = values[c][index * HALO : (index + 1) * HALO]
            for window in range(2):
                edges[target, c, window, 0:HALO] = value[:, window * half : (window + 1) * half]
                edges[target, c, window, HALO:] = jnp.zeros((8, half), jnp.float32)

    def rows_of(segment, section, window, c, start):
        if segment > 0:
            return stores[segment - 1][section, c, window, start : start + 8]
        if start + 8 <= rows:
            return image[section, c, window, start : start + 8]
        if start >= rows:
            return edges[section, c, window, start - rows : start - rows + 8]
        return jnp.concatenate(
            [
                image[section, c, window, start:rows],
                edges[section, c, window, 0 : start + 8 - rows],
            ],
            axis=0,
        )

    for segment in range(segments - 1):

        def step(section, carry, segment=segment):
            low = section & ~(1 << segment)
            window = (section >> segment) & 1
            values = []
            for child in range(2):
                source, term = low | (child << segment), segment * 2 + child
                reader = functools.partial(rows_of, segment, source, window)
                value = contracted(reader, rows + 8, bands[section, term])
                values.append((value, waves.at[section, term]))
            for block in range(rows // 8 + 1):
                for c, total in enumerate(turned(values, block)):
                    for side in range(2):
                        stores[segment][section, c, side, block * 8 : block * 8 + 8] = total[
                            :, side * half : (side + 1) * half
                        ]
            for c in range(2):
                for side in range(2):
                    stores[segment][section, c, side, rows + 8 :] = jnp.zeros(
                        (8, half), jnp.float32
                    )
            return carry

        lax.fori_loop(0, group, step, 0, unroll=4)

    last = stores[segments - 2]
    for mask in range(group):
        section = member ^ mask
        low = section & ~(1 << (segments - 1))
        window = (section >> (segments - 1)) & 1
        extra = []
        for child in range(2):
            for c in range(2):
                start = (child * 2 + c) * rows
                source = last.at[low | (child << (segments - 1)), c, window]
                outs[mask][start : start + rows] = source[0:rows].astype(jnp.bfloat16)
                extra.append(source[rows : rows + 1])
        extra.append(jnp.zeros((4, half), jnp.float32))
        outs[mask][4 * rows :] = jnp.concatenate(extra, axis=0).astype(jnp.bfloat16)


def final_kernel(masks, group, rows, first, *refs):
    count = len(masks)
    parts, (bands, waves) = refs[:count], refs[count : count + 2]
    result, store, mine, semaphores = refs[count + (2 if first else 3) :]
    half = store.shape[-1]
    member = lax.axis_index("sub") & (group - 1)
    copies = []
    for index, mask in enumerate(masks):
        part = parts[index]
        extra = part[4 * rows :].astype(jnp.float32)
        for side in range(4):
            store[index, side, 0:rows] = part[side * rows : (side + 1) * rows].astype(jnp.float32)
            store[index, side, rows:] = jnp.broadcast_to(extra[side : side + 1], (8, half))
        values = []
        for child in range(2):

            def rows_of(c, start, index=index, child=child):
                return store[index, child * 2 + c, start : start + 8]

            value = contracted(rows_of, rows, bands[0, child])
            values.append((value, waves.at[member ^ mask, child]))
        held = None
        for block in range(rows // 8):
            totals = turned(values, block)
            if block % 2 == 0:
                held = totals
                continue
            for c in range(2):
                mine[index, c, block * 8 - 8 : block * 8 + 8] = jnp.concatenate(
                    [held[c], totals[c]], axis=0
                ).astype(jnp.bfloat16)
        start = pl.multiple_of((member ^ mask) * rows, rows)
        for c in range(2):
            copy = pltpu.make_async_copy(
                mine.at[index, c], result.at[c, pl.ds(start, rows)], semaphores.at[index, c]
            )
            copy.start()
            copies.append(copy)
    for copy in copies:
        copy.wait()


def send_order(group):
    masks = list(range(1, group))
    far = sorted([mask for mask in masks if mask >= group // 2], reverse=True)
    near = sorted([mask for mask in masks if mask < group // 2], reverse=True)
    return far[:2] + near + far[2:]


def on_device(echoes, steering, sub_map, band_offset, interp_weight, range_frac, phase_rate):
    slabs = lax.axis_size("rng")
    subs = lax.axis_size("sub")
    segments, taps = interp_weight.shape[1], interp_weight.shape[3]
    group = 1 << segments
    groups = subs // group
    angles, pulse_count = steering.shape[1], steering.shape[2]
    half = angles // 2
    slab = lax.axis_index("rng")
    range_rows = echoes.shape[2] * subs
    rows = range_rows // group
    early, late = 2 * (segments - 1), 2

    cut = (2,) + echoes.shape[2:]
    tables_in = (band_offset, interp_weight, range_frac, phase_rate)
    *quarters, early_pack, late_pack = pl.pallas_call(
        functools.partial(cut_kernel, slabs, segments, taps, half),
        out_shape=[jax.ShapeDtypeStruct(cut, jnp.bfloat16)] * slabs
        + [
            jax.ShapeDtypeStruct((pack_rows(terms, taps), angles), jnp.bfloat16)
            for terms in (early, late)
        ],
        in_specs=[FAR] * 5,
        out_specs=[WHOLE] * (slabs + 2),
        scratch_shapes=[pltpu.VMEM(value.shape, value.dtype) for value in tables_in]
        + [pltpu.SemaphoreType.DMA((slabs, 2)), pltpu.SemaphoreType.DMA((4,))],
        compiler_params=params(60),
        cost_estimate=cost(1_000_000_000),
        name="cut",
    )(echoes, *tables_in)

    received = [quarters[0]] + [None] * (slabs - 1)
    for mask in range(slabs - 1, 0, -1):
        received[mask] = exchanged(quarters[mask], "rng", mask)

    masks = list(range(group - 1, 0, -1))
    masks = (masks[0::2], masks[1::2])
    mine, theirs = [], []
    for step in range(len(masks[0])):
        route = []
        for s in range(subs):
            for q in range(slabs):
                if step < len(masks[q & 1]):
                    route.append((s * slabs + q, (s ^ masks[q & 1][step]) * slabs + q))
        mine.append(lax.ppermute(early_pack, ("sub", "rng"), route))
    for piece in mine:
        theirs.append(exchanged(piece, "rng", 1))

    if groups == 1:
        blocks = received
    else:
        ordered = jnp.zeros((slabs,) + received[0].shape, received[0].dtype)
        for mask, block in enumerate(received):
            ordered = lax.dynamic_update_index_in_dim(ordered, block, slab ^ mask, 0)
        every = jnp.moveaxis(ordered, 0, 2).reshape(2, -1, subs, pulse_count)
        every = jnp.take(every, sub_map, axis=2)
        every = lax.ppermute(
            every,
            "sub",
            [(old, (old % groups) * group + old // groups) for old in range(subs)],
        ).reshape(2, -1, groups, group * pulse_count)
        lanes = [[g * group + m for g in range(groups)] for m in range(group)]
        every = lax.all_to_all(every, "sub", 2, 1, axis_index_groups=lanes, tiled=True)
        blocks = [every.reshape(2, rows, group * pulse_count)]

    edge_rows = jnp.stack([block[:, :HALO] for block in blocks])
    route = []
    for number in range(subs):
        for q in range(slabs):
            if number % group > 0:
                route.append((number * slabs + q, (number - 1) * slabs + q))
            elif q > 0:
                route.append((number * slabs + q, (number + group - 1) * slabs + q - 1))
    edge = lax.ppermute(edge_rows, ("sub", "rng"), route)

    def tables(terms, sources, held, lines, arrays):
        return pl.pallas_call(
            functools.partial(
                table_kernel,
                group,
                terms,
                sources,
                taps,
                half,
                rows,
                lines,
                range_rows,
                slabs * range_rows,
            ),
            out_shape=(
                jax.ShapeDtypeStruct((held, terms, angles, angles), jnp.bfloat16),
                jax.ShapeDtypeStruct((group, terms, 2, lines, angles), jnp.float32),
            ),
            in_specs=[WHOLE] * len(arrays),
            out_specs=(WHOLE, WHOLE),
            scratch_shapes=[
                pltpu.VMEM((group, terms, taps, angles), jnp.float32),
                pltpu.VMEM((group, 3, terms, angles), jnp.float32),
                pltpu.VMEM((15, angles // 128, group * terms, 128), jnp.float32),
            ],
            compiler_params=params(4),
            cost_estimate=cost(2_000_000_000),
        )(*arrays)

    bands, waves = tables(early, masks, group, rows + 8, [early_pack, *mine, *theirs])

    image = pl.pallas_call(
        functools.partial(form_kernel, group, pulse_count, len(blocks)),
        out_shape=jax.ShapeDtypeStruct((group, 2, 2, rows, half), jnp.float32),
        in_specs=[SCALARS] + [WHOLE] * (len(blocks) + 1),
        out_specs=WHOLE,
        compiler_params=params(8),
        cost_estimate=cost(1_000_000_000),
        name="form",
    )(sub_map, *blocks, steering)

    sent = pl.pallas_call(
        functools.partial(merge_kernel, group, segments, rows, pulse_count, len(blocks)),
        out_shape=[jax.ShapeDtypeStruct((4 * rows + 8, half), jnp.bfloat16)] * group,
        in_specs=[SCALARS] + [WHOLE] * 5,
        out_specs=[WHOLE] * group,
        scratch_shapes=[pltpu.VMEM((group, 2, 2, 16, half), jnp.float32)]
        + [pltpu.VMEM((group, 2, 2, rows + 16, half), jnp.float32)] * (segments - 1),
        compiler_params=params(12),
        cost_estimate=cost(4_000_000_000),
        name="merge",
    )(sub_map, image, edge, steering, bands, waves)

    order = send_order(group)
    arrived = {0: sent[0]}
    for mask in order:
        arrived[mask] = exchanged(sent[mask], "sub", mask)
    last_bands, last_waves = tables(late, None, 1, rows, [late_pack])
    result = None
    turns = [[0] + order[:1] + order[2:-2], order[1:2], order[-2:-1], order[-1:]]
    for chosen in turns:
        count = len(chosen)
        shape = jax.ShapeDtypeStruct((2, range_rows, angles), jnp.bfloat16)
        previous = [] if result is None else [result]
        result = pl.pallas_call(
            functools.partial(final_kernel, chosen, group, rows, result is None),
            out_shape=shape,
            in_specs=[WHOLE] * (count + 2) + [FAR] * len(previous),
            out_specs=FAR,
            scratch_shapes=[
                pltpu.VMEM((count, 4, rows + 8, half), jnp.float32),
                pltpu.VMEM((count, 2, rows, angles), jnp.bfloat16),
                pltpu.SemaphoreType.DMA((count, 2)),
            ],
            input_output_aliases={count + 2: 0} if previous else {},
            compiler_params=params(6),
            cost_estimate=cost(1_000_000_000),
            name="final",
        )(*[arrived[mask] for mask in chosen], last_bands, last_waves, *previous)
    return result


def solution(mesh):
    in_specs = (
        P(None, None, "sub", "rng"),
        P(),
        P(),
        P("sub", None, None, None),
        P("sub", None, None, None, None),
        P("sub", None, None, None),
        P("sub", None, None, None),
    )
    return jax.shard_map(
        on_device, mesh=mesh, in_specs=in_specs, out_specs=P(None, "rng", "sub"), check_vma=False
    )
```

```python
import functools

import jax
import jax.numpy as jnp
from jax import lax
from jax.experimental import pallas as pl
from jax.experimental.pallas import tpu as pltpu
from jax.sharding import PartitionSpec as P


HALO = 8
KINDS = 6
MIB = 1 << 20
WHOLE = pl.BlockSpec(memory_space=pltpu.VMEM)
SCALARS = pl.BlockSpec(memory_space=pltpu.SMEM)
FAR = pl.BlockSpec(memory_space=pltpu.HBM)


def exchanged(block, axis, mask):
    count = lax.axis_size(axis)
    return lax.ppermute(block, axis, [(source, source ^ mask) for source in range(count)])


def params(mib):
    return pltpu.CompilerParams(vmem_limit_bytes=mib * MIB)


def cost(flops):
    return pl.CostEstimate(flops=flops, bytes_accessed=MIB, transcendentals=0)


def product(left, right):
    return (
        left[0] * right[0] - left[1] * right[1],
        left[0] * right[1] + left[1] * right[0],
    )


def pack_rows(terms, taps):
    return -(-(terms * (taps + KINDS)) // 8) * 8


def cut_kernel(slabs, segments, taps, half, echoes, offset, weight, fraction, rate, *refs):
    slices, packs = refs[:slabs], refs[slabs : slabs + 2]
    held, semaphores, small = refs[slabs + 2 : slabs + 6], refs[slabs + 6], refs[slabs + 7]
    group = 1 << segments
    member = lax.axis_index("sub") & (group - 1)
    slab = lax.axis_index("rng")
    loads = [
        pltpu.make_async_copy(source, target, small.at[index])
        for index, (source, target) in enumerate(zip((offset, weight, fraction, rate), held))
    ]
    copies = []
    for mask in range(slabs - 1, -1, -1):
        for c in range(2):
            copies.append(
                pltpu.make_async_copy(
                    echoes.at[c, slab ^ mask], slices[mask].at[c], semaphores.at[mask, c]
                )
            )
    for copy in loads + copies:
        copy.start()
    for copy in loads:
        copy.wait()
    offset, weight, fraction, rate = held
    angles = weight.shape[-1]
    for pack, chosen in ((packs[0], range(segments - 1)), (packs[1], (segments - 1,))):
        kinds = [[] for _ in range(KINDS)]
        terms = 2 * len(chosen)
        for index, segment in enumerate(chosen):
            base = ((member >> segment) & 1) * half
            kinds[0].append((offset[0, segment] - base).astype(jnp.float32))
            slot = 1
            for source, count in ((fraction, 2), (rate, 3)):
                rest = source[0, segment]
                for _ in range(count):
                    part = rest.astype(jnp.bfloat16).astype(jnp.float32)
                    kinds[slot].append(part)
                    rest = rest - part
                    slot += 1
            for child in range(2):
                term = index * 2 + child
                pack[term * taps : (term + 1) * taps, :] = weight[0, segment, child]
        rows = [piece for kind in kinds for piece in kind]
        padding = pack_rows(terms, taps) - terms * (taps + KINDS)
        if padding:
            rows.append(jnp.zeros((padding, angles), jnp.float32))
        pack[terms * taps :, :] = jnp.concatenate(rows, axis=0).astype(jnp.bfloat16)
    for copy in copies:
        copy.wait()


def table_kernel(members, terms, masks, taps, half, rows, lines, range_rows, total_range, *refs):
    steps = len(masks[0]) if masks else 0
    own, mine, theirs = refs[0], refs[1 : 1 + steps], refs[1 + steps : 1 + 2 * steps]
    bands, waves, weights, raw, dense = refs[1 + 2 * steps :]
    angles = bands.shape[-1]
    member = lax.axis_index("sub") & (members - 1)
    slab = lax.axis_index("rng")

    def fill(piece, section):
        values = piece[...].astype(jnp.float32)
        for term in range(terms):
            weights[section, term] = values[term * taps : (term + 1) * taps]
        start = terms * taps
        kind = [values[start + k * terms : start + (k + 1) * terms] for k in range(KINDS)]
        raw[section, 0] = kind[0]
        raw[section, 1] = kind[1] + kind[2]
        raw[section, 2] = kind[3] + kind[4] + kind[5]

    if masks:
        core = slab & 1
        fill(own, member)
        for side, received in ((0, mine), (1, theirs)):
            holder = core if side == 0 else 1 - core
            for step in range(steps):
                pair = [masks[c][step] if step < len(masks[c]) else 0 for c in range(2)]
                mask = jnp.where(holder == 0, pair[0], pair[1])

                @pl.when(mask != 0)
                def _(step=step, received=received, mask=mask):
                    fill(received[step], member ^ mask)

        first_row, row_step = slab * range_rows + member * rows, 0
    else:
        for section in range(members):
            fill(own, section)
        first_row, row_step = slab * range_rows, rows

    for start in range(0, members * terms, 8):
        place = slice(start, start + 8)
        sections = range(start // terms, (start + 8) // terms)

        def keep(kind, value):
            for part in range(angles // 128):
                dense[kind, part, place] = value[:, part * 128 : (part + 1) * 128]

        given = [
            jnp.concatenate([raw[section, kind] for section in sections], axis=0)
            for kind in range(3)
        ]
        keep(0, given[0])
        keep(1, given[1])
        rate = given[2]
        number = start + lax.broadcasted_iota(jnp.int32, (8, angles), 0)
        first = first_row + (number // terms) * row_step
        angle = first.astype(jnp.float32) / float(total_range) * rate
        keep(3, jnp.cos(angle))
        keep(4, jnp.sin(angle))
        angle = rate / float(total_range)
        turn = jnp.cos(angle), jnp.sin(angle)
        for power in range(5):
            keep(5 + 2 * power, turn[0])
            keep(6 + 2 * power, turn[1])
            turn = product(turn, turn)

    sub_rows = lax.broadcasted_iota(jnp.int32, (8, 128), 0)

    def entry(index, carry):
        section, term = index // terms, index % terms
        for part in range(angles // 128):
            lanes = pl.ds(part * 128, 128)

            def row(kind):
                return dense[kind, part, pl.ds(index, 1), :]

            def bands_of():
                weight = weights[section, term, :, lanes]
                offset = row(0).astype(jnp.int32)
                fraction = row(1)
                tap = sub_rows - offset
                block_of = -(tap >> 3)
                picked = jnp.take_along_axis(weight, tap & 7, axis=0)
                near, far = picked * (1.0 - fraction), picked * fraction
                for block in range(half // 16):
                    hits = [block_of == 2 * block + step for step in range(2)]
                    for source, base in ((near, 0), (far, half)):
                        pair = [jnp.where(hit, source, 0.0) for hit in hits]
                        place = slice(base + block * 16, base + (block + 1) * 16)
                        bands[section, term, place, lanes] = jnp.concatenate(pair, axis=0).astype(
                            jnp.bfloat16
                        )

            if masks:
                bands_of()
            else:
                pl.when(section == 0)(bands_of)
            wave = tuple(jnp.broadcast_to(row(3 + c), (8, 128)) for c in range(2))
            for power in range(3):
                chosen = (sub_rows >> power) & 1 == 1
                wave = product(
                    wave,
                    (
                        jnp.where(chosen, row(5 + 2 * power), 1.0),
                        jnp.where(chosen, row(6 + 2 * power), 0.0),
                    ),
                )
            eight, sixteen = (row(11), row(12)), (row(13), row(14))
            chain = [wave, product(wave, eight)]
            for block in range(lines // 8):
                wave = chain[block % 2]
                for c in range(2):
                    waves[section, term, c, block * 8 : (block + 1) * 8, lanes] = wave[c]
                chain[block % 2] = product(wave, sixteen)
        return carry

    lax.fori_loop(0, members * terms, entry, 0)


def formed(steering, re_part, im_part):
    def dot(left, right):
        return lax.dot_general(
            left, right, (((1,), (1,)), ((), ())), preferred_element_type=jnp.float32
        )

    real_weight, imag_weight = steering[0], steering[1]
    return (
        dot(re_part, real_weight) + dot(im_part, -imag_weight),
        dot(re_part, imag_weight) + dot(im_part, real_weight),
    )


def place_of(sub_map, group, slabs, slab, index):
    if slabs == 1:
        return index
    per_slab = group // slabs
    block = (slab ^ (index // per_slab)) * per_slab + index % per_slab
    place = 0
    for section in range(group):
        place = jnp.where(sub_map[section] == block, section, place)
    return place


def form_kernel(group, pulse_count, sources, sub_map, *refs):
    blocks, steering, image = refs[:sources], refs[sources], refs[sources + 1]
    half = image.shape[-1]
    per_source = group // sources
    slab = lax.axis_index("rng")

    def step(piece, carry):
        columns = pl.ds(pl.multiple_of(piece * pulse_count, pulse_count), pulse_count)
        for source in range(sources):
            target = place_of(sub_map, group, sources, slab, source * per_source + piece)
            parts = [blocks[source][c, :, columns] for c in range(2)]
            for c, value in enumerate(formed(steering, *parts)):
                for window in range(2):
                    image[target, c, window] = value[:, window * half : (window + 1) * half]
        return carry

    lax.fori_loop(0, per_source, step, 0)


def turned(values, block):
    total = None
    for value, wave in values:
        part = value[block * 16 : block * 16 + 8], value[block * 16 + 8 : block * 16 + 16]
        turn = tuple(wave[c, block * 8 : block * 8 + 8] for c in range(2))
        term = product(turn, part)
        total = term if total is None else (total[0] + term[0], total[1] + term[1])
    return total


def contracted(rows_of, lines, matrix):
    pieces = []
    for block in range(lines // 8):
        sides = []
        for start in (block * 8, block * 8 + 1):
            both = [rows_of(c, start) for c in range(2)]
            sides.append(jnp.concatenate(both, axis=0).astype(jnp.bfloat16))
        pieces.append(jnp.concatenate(sides, axis=1))
    return jnp.dot(jnp.concatenate(pieces, axis=0), matrix, preferred_element_type=jnp.float32)


def merge_kernel(group, segments, rows, pulse_count, sources, sub_map, *refs):
    image, edge, steering, bands, waves = refs[:5]
    outs, edges = refs[5 : 5 + group], refs[5 + group]
    stores = refs[6 + group :]
    half = image.shape[-1]
    member = lax.axis_index("sub") & (group - 1)
    per_source = group // sources
    below = lax.axis_index("rng")
    if sources > 1:
        below = jnp.minimum(below + jnp.where(member == group - 1, 1, 0), sources - 1)

    edge_parts = [[], []]
    for source in range(sources):
        for piece in range(per_source):
            columns = slice(piece * pulse_count, (piece + 1) * pulse_count)
            for c in range(2):
                edge_parts[c].append(edge[source, c, :, columns])
    values = formed(steering, *[jnp.concatenate(parts, axis=0) for parts in edge_parts])
    for index in range(group):
        target = place_of(sub_map, group, sources, below, index)
        for c in range(2):
            value = values[c][index * HALO : (index + 1) * HALO]
            for window in range(2):
                edges[target, c, window, 0:HALO] = value[:, window * half : (window + 1) * half]
                edges[target, c, window, HALO:] = jnp.zeros((8, half), jnp.float32)

    def rows_of(segment, section, window, c, start):
        if segment > 0:
            return stores[segment - 1][section, c, window, start : start + 8]
        if start + 8 <= rows:
            return image[section, c, window, start : start + 8]
        if start >= rows:
            return edges[section, c, window, start - rows : start - rows + 8]
        return jnp.concatenate(
            [
                image[section, c, window, start:rows],
                edges[section, c, window, 0 : start + 8 - rows],
            ],
            axis=0,
        )

    for segment in range(segments - 1):

        def step(section, carry, segment=segment):
            low = section & ~(1 << segment)
            window = (section >> segment) & 1
            values = []
            for child in range(2):
                source, term = low | (child << segment), segment * 2 + child
                reader = functools.partial(rows_of, segment, source, window)
                value = contracted(reader, rows + 8, bands[section, term])
                values.append((value, waves.at[section, term]))
            for block in range(rows // 8 + 1):
                for c, total in enumerate(turned(values, block)):
                    for side in range(2):
                        stores[segment][section, c, side, block * 8 : block * 8 + 8] = total[
                            :, side * half : (side + 1) * half
                        ]
            for c in range(2):
                for side in range(2):
                    stores[segment][section, c, side, rows + 8 :] = jnp.zeros(
                        (8, half), jnp.float32
                    )
            return carry

        lax.fori_loop(0, group, step, 0, unroll=4)

    last = stores[segments - 2]
    for mask in range(group):
        section = member ^ mask
        low = section & ~(1 << (segments - 1))
        window = (section >> (segments - 1)) & 1
        extra = []
        for child in range(2):
            for c in range(2):
                start = (child * 2 + c) * rows
                source = last.at[low | (child << (segments - 1)), c, window]
                outs[mask][start : start + rows] = source[0:rows].astype(jnp.bfloat16)
                extra.append(source[rows : rows + 1])
        extra.append(jnp.zeros((4, half), jnp.float32))
        outs[mask][4 * rows :] = jnp.concatenate(extra, axis=0).astype(jnp.bfloat16)


def final_kernel(masks, group, rows, first, *refs):
    count = len(masks)
    parts, (bands, waves) = refs[:count], refs[count : count + 2]
    result, store, mine, semaphores = refs[count + (2 if first else 3) :]
    half = store.shape[-1]
    member = lax.axis_index("sub") & (group - 1)
    copies = []
    for index, mask in enumerate(masks):
        part = parts[index]
        extra = part[4 * rows :].astype(jnp.float32)
        for side in range(4):
            store[index, side, 0:rows] = part[side * rows : (side + 1) * rows].astype(jnp.float32)
            store[index, side, rows:] = jnp.broadcast_to(extra[side : side + 1], (8, half))
        values = []
        for child in range(2):

            def rows_of(c, start, index=index, child=child):
                return store[index, child * 2 + c, start : start + 8]

            value = contracted(rows_of, rows, bands[0, child])
            values.append((value, waves.at[member ^ mask, child]))
        held = None
        for block in range(rows // 8):
            totals = turned(values, block)
            if block % 2 == 0:
                held = totals
                continue
            for c in range(2):
                mine[index, c, block * 8 - 8 : block * 8 + 8] = jnp.concatenate(
                    [held[c], totals[c]], axis=0
                ).astype(jnp.bfloat16)
        start = pl.multiple_of((member ^ mask) * rows, rows)
        for c in range(2):
            copy = pltpu.make_async_copy(
                mine.at[index, c], result.at[c, pl.ds(start, rows)], semaphores.at[index, c]
            )
            copy.start()
            copies.append(copy)
    for copy in copies:
        copy.wait()


def send_order(group):
    masks = list(range(1, group))
    far = sorted([mask for mask in masks if mask >= group // 2], reverse=True)
    near = sorted([mask for mask in masks if mask < group // 2], reverse=True)
    return far[:2] + near + far[2:]


def on_device(echoes, steering, sub_map, band_offset, interp_weight, range_frac, phase_rate):
    slabs = lax.axis_size("rng")
    subs = lax.axis_size("sub")
    segments, taps = interp_weight.shape[1], interp_weight.shape[3]
    group = 1 << segments
    groups = subs // group
    angles, pulse_count = steering.shape[1], steering.shape[2]
    half = angles // 2
    slab = lax.axis_index("rng")
    range_rows = echoes.shape[2] * subs
    rows = range_rows // group
    early, late = 2 * (segments - 1), 2

    cut = (2,) + echoes.shape[2:]
    tables_in = (band_offset, interp_weight, range_frac, phase_rate)
    *quarters, early_pack, late_pack = pl.pallas_call(
        functools.partial(cut_kernel, slabs, segments, taps, half),
        out_shape=[pltpu.VMEM(cut, jnp.bfloat16)] * slabs
        + [pltpu.VMEM((pack_rows(terms, taps), angles), jnp.bfloat16) for terms in (early, late)],
        in_specs=[FAR] * 5,
        out_specs=[WHOLE] * (slabs + 2),
        scratch_shapes=[pltpu.VMEM(value.shape, value.dtype) for value in tables_in]
        + [pltpu.SemaphoreType.DMA((slabs, 2)), pltpu.SemaphoreType.DMA((4,))],
        compiler_params=params(2),
        cost_estimate=cost(1_000_000_000),
        name="cut",
    )(*[pltpu.with_memory_space_constraint(value, pltpu.HBM) for value in (echoes,) + tables_in])

    received = [quarters[0]] + [None] * (slabs - 1)
    for mask in range(slabs - 1, 0, -1):
        received[mask] = exchanged(quarters[mask], "rng", mask)

    masks = list(range(group - 1, 0, -1))
    masks = (masks[0::2], masks[1::2])
    mine, theirs = [], []
    for step in range(len(masks[0])):
        route = []
        for s in range(subs):
            for q in range(slabs):
                if step < len(masks[q & 1]):
                    route.append((s * slabs + q, (s ^ masks[q & 1][step]) * slabs + q))
        mine.append(lax.ppermute(early_pack, ("sub", "rng"), route))
    for piece in mine:
        theirs.append(exchanged(piece, "rng", 1))

    if groups == 1:
        blocks = received
    else:
        ordered = jnp.zeros((slabs,) + received[0].shape, received[0].dtype)
        for mask, block in enumerate(received):
            ordered = lax.dynamic_update_index_in_dim(ordered, block, slab ^ mask, 0)
        every = jnp.moveaxis(ordered, 0, 2).reshape(2, -1, subs, pulse_count)
        every = jnp.take(every, sub_map, axis=2)
        every = lax.ppermute(
            every,
            "sub",
            [(old, (old % groups) * group + old // groups) for old in range(subs)],
        ).reshape(2, -1, groups, group * pulse_count)
        lanes = [[g * group + m for g in range(groups)] for m in range(group)]
        every = lax.all_to_all(every, "sub", 2, 1, axis_index_groups=lanes, tiled=True)
        blocks = [every.reshape(2, rows, group * pulse_count)]

    edge_rows = jnp.stack([block[:, :HALO] for block in blocks])
    route = []
    for number in range(subs):
        for q in range(slabs):
            if number % group > 0:
                route.append((number * slabs + q, (number - 1) * slabs + q))
            elif q > 0:
                route.append((number * slabs + q, (number + group - 1) * slabs + q - 1))
    edge = lax.ppermute(edge_rows, ("sub", "rng"), route)

    def tables(terms, sources, held, lines, arrays):
        return pl.pallas_call(
            functools.partial(
                table_kernel,
                group,
                terms,
                sources,
                taps,
                half,
                rows,
                lines,
                range_rows,
                slabs * range_rows,
            ),
            out_shape=(
                jax.ShapeDtypeStruct((held, terms, angles, angles), jnp.bfloat16),
                jax.ShapeDtypeStruct((group, terms, 2, lines, angles), jnp.float32),
            ),
            in_specs=[WHOLE] * len(arrays),
            out_specs=(WHOLE, WHOLE),
            scratch_shapes=[
                pltpu.VMEM((group, terms, taps, angles), jnp.float32),
                pltpu.VMEM((group, 3, terms, angles), jnp.float32),
                pltpu.VMEM((15, angles // 128, group * terms, 128), jnp.float32),
            ],
            compiler_params=params(4),
            cost_estimate=cost(2_000_000_000),
        )(*arrays)

    bands, waves = tables(early, masks, group, rows + 8, [early_pack, *mine, *theirs])

    image = pl.pallas_call(
        functools.partial(form_kernel, group, pulse_count, len(blocks)),
        out_shape=jax.ShapeDtypeStruct((group, 2, 2, rows, half), jnp.float32),
        in_specs=[SCALARS] + [WHOLE] * (len(blocks) + 1),
        out_specs=WHOLE,
        compiler_params=params(8),
        cost_estimate=cost(1_000_000_000),
        name="form",
    )(sub_map, *blocks, steering)

    sent = pl.pallas_call(
        functools.partial(merge_kernel, group, segments, rows, pulse_count, len(blocks)),
        out_shape=[jax.ShapeDtypeStruct((4 * rows + 8, half), jnp.bfloat16)] * group,
        in_specs=[SCALARS] + [WHOLE] * 5,
        out_specs=[WHOLE] * group,
        scratch_shapes=[pltpu.VMEM((group, 2, 2, 16, half), jnp.float32)]
        + [pltpu.VMEM((group, 2, 2, rows + 16, half), jnp.float32)] * (segments - 1),
        compiler_params=params(12),
        cost_estimate=cost(4_000_000_000),
        name="merge",
    )(sub_map, image, edge, steering, bands, waves)

    order = send_order(group)
    arrived = {0: sent[0]}
    for mask in order:
        arrived[mask] = exchanged(sent[mask], "sub", mask)
    last_bands, last_waves = tables(late, None, 1, rows, [late_pack])
    result = None
    turns = [[0] + order[:1] + order[2:-2], order[1:2], order[-2:-1], order[-1:]]
    for chosen in turns:
        count = len(chosen)
        shape = jax.ShapeDtypeStruct((2, range_rows, angles), jnp.bfloat16)
        previous = [] if result is None else [result]
        result = pl.pallas_call(
            functools.partial(final_kernel, chosen, group, rows, result is None),
            out_shape=shape,
            in_specs=[WHOLE] * (count + 2) + [FAR] * len(previous),
            out_specs=FAR,
            scratch_shapes=[
                pltpu.VMEM((count, 4, rows + 8, half), jnp.float32),
                pltpu.VMEM((count, 2, rows, angles), jnp.bfloat16),
                pltpu.SemaphoreType.DMA((count, 2)),
            ],
            input_output_aliases={count + 2: 0} if previous else {},
            compiler_params=params(6),
            cost_estimate=cost(1_000_000_000),
            name="final",
        )(*[arrived[mask] for mask in chosen], last_bands, last_waves, *previous)
    return result


def solution(mesh):
    in_specs = (
        P(None, None, "sub", "rng"),
        P(),
        P(),
        P("sub", None, None, None),
        P("sub", None, None, None, None),
        P("sub", None, None, None),
        P("sub", None, None, None),
    )
    return jax.shard_map(
        on_device, mesh=mesh, in_specs=in_specs, out_specs=P(None, "rng", "sub"), check_vma=False
    )
```

```python
import functools

import jax
import jax.numpy as jnp
from jax import lax
from jax.experimental import pallas as pl
from jax.experimental.pallas import tpu as pltpu
from jax.sharding import PartitionSpec as P


HALO = 8
KINDS = 6
MIB = 1 << 20
WHOLE = pl.BlockSpec(memory_space=pltpu.VMEM)
SCALARS = pl.BlockSpec(memory_space=pltpu.SMEM)
FAR = pl.BlockSpec(memory_space=pltpu.HBM)


def exchanged(block, axis, mask):
    count = lax.axis_size(axis)
    return lax.ppermute(block, axis, [(source, source ^ mask) for source in range(count)])


def params(mib):
    return pltpu.CompilerParams(vmem_limit_bytes=mib * MIB)


def cost(flops):
    return pl.CostEstimate(flops=flops, bytes_accessed=MIB, transcendentals=0)


def product(left, right):
    return (
        left[0] * right[0] - left[1] * right[1],
        left[0] * right[1] + left[1] * right[0],
    )


def pack_rows(terms, taps):
    return -(-(terms * (taps + KINDS)) // 8) * 8


def cut_kernel(slabs, segments, taps, half, echoes, offset, weight, fraction, rate, *refs):
    slices, packs = refs[:slabs], refs[slabs : slabs + 2]
    held, semaphores, small = refs[slabs + 2 : slabs + 6], refs[slabs + 6], refs[slabs + 7]
    group = 1 << segments
    member = lax.axis_index("sub") & (group - 1)
    slab = lax.axis_index("rng")
    loads = [
        pltpu.make_async_copy(source, target, small.at[index])
        for index, (source, target) in enumerate(zip((offset, weight, fraction, rate), held))
    ]
    copies = []
    for mask in range(slabs - 1, -1, -1):
        for c in range(2):
            copies.append(
                pltpu.make_async_copy(
                    echoes.at[c, slab ^ mask], slices[mask].at[c], semaphores.at[mask, c]
                )
            )
    for copy in loads + copies:
        copy.start()
    for copy in loads:
        copy.wait()
    offset, weight, fraction, rate = held
    angles = weight.shape[-1]
    for pack, chosen in ((packs[0], range(segments - 1)), (packs[1], (segments - 1,))):
        kinds = [[] for _ in range(KINDS)]
        terms = 2 * len(chosen)
        for index, segment in enumerate(chosen):
            base = ((member >> segment) & 1) * half
            kinds[0].append((offset[0, segment] - base).astype(jnp.float32))
            slot = 1
            for source, count in ((fraction, 2), (rate, 3)):
                rest = source[0, segment]
                for _ in range(count):
                    part = rest.astype(jnp.bfloat16).astype(jnp.float32)
                    kinds[slot].append(part)
                    rest = rest - part
                    slot += 1
            for child in range(2):
                term = index * 2 + child
                pack[term * taps : (term + 1) * taps, :] = weight[0, segment, child]
        rows = [piece for kind in kinds for piece in kind]
        padding = pack_rows(terms, taps) - terms * (taps + KINDS)
        if padding:
            rows.append(jnp.zeros((padding, angles), jnp.float32))
        pack[terms * taps :, :] = jnp.concatenate(rows, axis=0).astype(jnp.bfloat16)
    for copy in copies:
        copy.wait()


def table_kernel(members, terms, masks, taps, half, rows, lines, range_rows, total_range, *refs):
    steps = len(masks[0]) if masks else 0
    swapped = steps - 1 if masks else 0
    own, mine, theirs = refs[0], refs[1 : 1 + steps], refs[1 + steps : 1 + steps + swapped]
    bands, waves, weights, raw, dense = refs[1 + steps + swapped :]
    angles = bands.shape[-1]
    member = lax.axis_index("sub") & (members - 1)
    slab = lax.axis_index("rng")

    def fill(piece, section):
        values = piece[...].astype(jnp.float32)
        for term in range(terms):
            weights[section, term] = values[term * taps : (term + 1) * taps]
        start = terms * taps
        kind = [values[start + k * terms : start + (k + 1) * terms] for k in range(KINDS)]
        raw[section, 0] = kind[0]
        raw[section, 1] = kind[1] + kind[2]
        raw[section, 2] = kind[3] + kind[4] + kind[5]

    if masks:
        core = slab & 1
        fill(own, member)
        for received, holder in ((mine, core), (theirs, 1 - core)):
            for step, piece in enumerate(received):
                fill(piece, member ^ jnp.where(holder == 0, masks[0][step], masks[1][step]))
        first_row, row_step = slab * range_rows + member * rows, 0
    else:
        for section in range(members):
            fill(own, section)
        first_row, row_step = slab * range_rows, rows

    for start in range(0, members * terms, 8):
        place = slice(start, start + 8)
        sections = range(start // terms, (start + 8) // terms)

        def keep(kind, value):
            for part in range(angles // 128):
                dense[kind, part, place] = value[:, part * 128 : (part + 1) * 128]

        given = [
            jnp.concatenate([raw[section, kind] for section in sections], axis=0)
            for kind in range(3)
        ]
        keep(0, given[0])
        keep(1, given[1])
        rate = given[2]
        number = start + lax.broadcasted_iota(jnp.int32, (8, angles), 0)
        first = first_row + (number // terms) * row_step
        angle = first.astype(jnp.float32) / float(total_range) * rate
        keep(3, jnp.cos(angle))
        keep(4, jnp.sin(angle))
        angle = rate / float(total_range)
        turn = jnp.cos(angle), jnp.sin(angle)
        for power in range(5):
            keep(5 + 2 * power, turn[0])
            keep(6 + 2 * power, turn[1])
            turn = product(turn, turn)

    sub_rows = lax.broadcasted_iota(jnp.int32, (8, 128), 0)

    def entry(index, carry):
        section, term = index // terms, index % terms
        for part in range(angles // 128):
            lanes = pl.ds(part * 128, 128)

            def row(kind):
                return dense[kind, part, pl.ds(index, 1), :]

            def bands_of():
                weight = weights[section, term, :, lanes]
                offset = row(0).astype(jnp.int32)
                fraction = row(1)
                tap = sub_rows - offset
                block_of = -(tap >> 3)
                picked = jnp.take_along_axis(weight, tap & 7, axis=0)
                near, far = picked * (1.0 - fraction), picked * fraction
                for block in range(half // 16):
                    hits = [block_of == 2 * block + step for step in range(2)]
                    for source, base in ((near, 0), (far, half)):
                        pair = [jnp.where(hit, source, 0.0) for hit in hits]
                        place = slice(base + block * 16, base + (block + 1) * 16)
                        bands[section, term, place, lanes] = jnp.concatenate(pair, axis=0).astype(
                            jnp.bfloat16
                        )

            if masks:
                bands_of()
            else:
                pl.when(section == 0)(bands_of)
            wave = tuple(jnp.broadcast_to(row(3 + c), (8, 128)) for c in range(2))
            for power in range(3):
                chosen = (sub_rows >> power) & 1 == 1
                wave = product(
                    wave,
                    (
                        jnp.where(chosen, row(5 + 2 * power), 1.0),
                        jnp.where(chosen, row(6 + 2 * power), 0.0),
                    ),
                )
            eight, sixteen = (row(11), row(12)), (row(13), row(14))
            chain = [wave, product(wave, eight)]
            for block in range(lines // 8):
                wave = chain[block % 2]
                for c in range(2):
                    waves[section, term, c, block * 8 : (block + 1) * 8, lanes] = wave[c]
                chain[block % 2] = product(wave, sixteen)
        return carry

    lax.fori_loop(0, members * terms, entry, 0)


def formed(steering, re_parts, im_parts):
    rows = jnp.concatenate(re_parts + im_parts, axis=0)
    count = rows.shape[0] // 2
    by_real, by_imag = [
        lax.dot_general(
            rows, steering[c], (((1,), (1,)), ((), ())), preferred_element_type=jnp.float32
        )
        for c in range(2)
    ]
    return by_real[:count] - by_imag[count:], by_imag[:count] + by_real[count:]


def place_of(sub_map, group, slabs, slab, index):
    if slabs == 1:
        return index
    per_slab = group // slabs
    block = (slab ^ (index // per_slab)) * per_slab + index % per_slab
    place = 0
    for section in range(group):
        place = jnp.where(sub_map[section] == block, section, place)
    return place


def form_kernel(group, pulse_count, sources, first, count, sub_map, *refs):
    blocks, steering, image = refs[:sources], refs[sources], refs[sources + 1]
    half = image.shape[-1]
    per_source = group // sources
    slab = lax.axis_index("rng")
    for source in range(sources):
        for start in range(0, per_source, 2):
            pieces = range(start, min(start + 2, per_source))
            parts = [
                [
                    blocks[source][
                        c, first : first + count, piece * pulse_count : (piece + 1) * pulse_count
                    ]
                    for piece in pieces
                ]
                for c in range(2)
            ]
            values = formed(steering, *parts)
            for index, piece in enumerate(pieces):
                target = place_of(sub_map, group, sources, slab, source * per_source + piece)
                for c in range(2):
                    value = values[c][index * count : (index + 1) * count]
                    for window in range(2):
                        image[target, c, window] = value[:, window * half : (window + 1) * half]


def turned(values, block, first):
    total = None
    for value, wave in values:
        part = value[block * 16 : block * 16 + 8], value[block * 16 + 8 : block * 16 + 16]
        start = first + block * 8
        turn = tuple(wave[c, start : start + 8] for c in range(2))
        term = product(turn, part)
        total = term if total is None else (total[0] + term[0], total[1] + term[1])
    return total


def contracted(rows_of, lines, matrix):
    pieces = []
    for block in range(lines // 8):
        sides = []
        for start in (block * 8, block * 8 + 1):
            both = [rows_of(c, start) for c in range(2)]
            sides.append(jnp.concatenate(both, axis=0).astype(jnp.bfloat16))
        pieces.append(jnp.concatenate(sides, axis=1))
    return jnp.dot(jnp.concatenate(pieces, axis=0), matrix, preferred_element_type=jnp.float32)


def merge_kernel(group, segments, chunk, rows, pulse_count, sources, *refs):
    near = group // 2
    if chunk == 0:
        image, bands, waves = refs[:3]
        refs = refs[3:]
    else:
        sub_map, image, edge, steering, bands, waves = refs[:6]
        kept, edges, refs = refs[6 : 6 + near], refs[6 + near + group], refs[6 + near :]
        refs = refs[:group] + refs[group + 1 :]
    outs, stores = refs[:group], refs[group:]
    half = image.shape[-1]
    member = lax.axis_index("sub") & (group - 1)
    per_source = group // sources

    if chunk == 1:
        below = lax.axis_index("rng")
        if sources > 1:
            below = jnp.minimum(below + jnp.where(member == group - 1, 1, 0), sources - 1)
        parts = [[], []]
        for source in range(sources):
            for piece in range(per_source):
                columns = slice(piece * pulse_count, (piece + 1) * pulse_count)
                for c in range(2):
                    parts[c].append(edge[source, c, :, columns])
        values = formed(steering, *parts)
        for index in range(group):
            target = place_of(sub_map, group, sources, below, index)
            for c in range(2):
                value = values[c][index * HALO : (index + 1) * HALO]
                for window in range(2):
                    edges[target, c, window, 0:HALO] = value[:, window * half : (window + 1) * half]
                    edges[target, c, window, HALO:] = jnp.zeros((8, half), jnp.float32)

    def rows_of(segment, section, window, c, start):
        if segment > 0:
            return stores[segment - 1][section, c, window, start : start + 8]
        if chunk == 0 or start + 8 <= rows:
            return image[section, c, window, start : start + 8]
        if start >= rows:
            return edges[section, c, window, start - rows : start - rows + 8]
        return jnp.concatenate(
            [
                image[section, c, window, start:rows],
                edges[section, c, window, 0 : start + 8 - rows],
            ],
            axis=0,
        )

    for segment in range(segments - 1):

        def step(section, carry, segment=segment):
            low = section & ~(1 << segment)
            window = (section >> segment) & 1
            values = []
            for child in range(2):
                source, term = low | (child << segment), segment * 2 + child
                reader = functools.partial(rows_of, segment, source, window)
                value = contracted(reader, rows + 8, bands[section, term])
                values.append((value, waves.at[section, term]))
            for block in range(rows // 8 + 1):
                for c, total in enumerate(turned(values, block, chunk * rows)):
                    for side in range(2):
                        stores[segment][section, c, side, block * 8 : block * 8 + 8] = total[
                            :, side * half : (side + 1) * half
                        ]
            for c in range(2):
                for side in range(2):
                    stores[segment][section, c, side, rows + 8 :] = jnp.zeros(
                        (8, half), jnp.float32
                    )
            return carry

        lax.fori_loop(0, group, step, 0, unroll=4)

    last = stores[segments - 2]
    size = 4 * rows + 8
    for mask in range(group):
        section = member ^ mask
        low = section & ~(1 << (segments - 1))
        window = (section >> (segments - 1)) & 1
        base = 0
        if chunk == 1 and mask < near:
            outs[mask][0:size] = kept[mask][...]
            base = size
        extra = []
        for child in range(2):
            for c in range(2):
                start = base + (child * 2 + c) * rows
                source = last.at[low | (child << (segments - 1)), c, window]
                outs[mask][start : start + rows] = source[0:rows].astype(jnp.bfloat16)
                extra.append(source[rows : rows + 1])
        extra.append(jnp.zeros((4, half), jnp.float32))
        outs[mask][base + 4 * rows : base + size] = jnp.concatenate(extra, axis=0).astype(
            jnp.bfloat16
        )


def final_kernel(jobs, count, group, rows, first, *refs):
    parts, (bands, waves) = refs[:count], refs[count : count + 2]
    result, store, mine, semaphores = refs[count + (2 if first else 3) :]
    half = store.shape[-1]
    member = lax.axis_index("sub") & (group - 1)
    copies = []
    for index, (source, base, mask, chunk) in enumerate(jobs):
        part = parts[source]
        extra = part[base + 4 * rows : base + 4 * rows + 8].astype(jnp.float32)
        for side in range(4):
            start = base + side * rows
            store[index, side, 0:rows] = part[start : start + rows].astype(jnp.float32)
            store[index, side, rows:] = jnp.broadcast_to(extra[side : side + 1], (8, half))
        values = []
        for child in range(2):

            def rows_of(c, start, index=index, child=child):
                return store[index, child * 2 + c, start : start + 8]

            value = contracted(rows_of, rows, bands[0, child])
            values.append((value, waves.at[member ^ mask, child]))
        held = None
        for block in range(rows // 8):
            totals = turned(values, block, chunk * rows)
            if block % 2 == 0:
                held = totals
                continue
            for c in range(2):
                mine[index, c, block * 8 - 8 : block * 8 + 8] = jnp.concatenate(
                    [held[c], totals[c]], axis=0
                ).astype(jnp.bfloat16)
        start = pl.multiple_of(((member ^ mask) * 2 + chunk) * rows, rows)
        for c in range(2):
            copy = pltpu.make_async_copy(
                mine.at[index, c], result.at[c, pl.ds(start, rows)], semaphores.at[index, c]
            )
            copy.start()
            copies.append(copy)
    for copy in copies:
        copy.wait()


def send_order(group):
    far, near = list(range(group - 1, group // 2 - 1, -1)), list(range(group // 2 - 1, 0, -1))
    order = [(mask, 0) for mask in far] + [(mask, 1) for mask in far[:2]]
    return order + [(mask, None) for mask in near] + [(mask, 1) for mask in far[2:]]


def on_device(echoes, steering, sub_map, band_offset, interp_weight, range_frac, phase_rate):
    slabs = lax.axis_size("rng")
    subs = lax.axis_size("sub")
    segments, taps = interp_weight.shape[1], interp_weight.shape[3]
    group = 1 << segments
    groups = subs // group
    angles, pulse_count = steering.shape[1], steering.shape[2]
    half = angles // 2
    slab = lax.axis_index("rng")
    range_rows = echoes.shape[2] * subs
    rows = range_rows // group
    early, late = 2 * (segments - 1), 2

    cut = (2,) + echoes.shape[2:]
    tables_in = (band_offset, interp_weight, range_frac, phase_rate)
    *quarters, early_pack, late_pack = pl.pallas_call(
        functools.partial(cut_kernel, slabs, segments, taps, half),
        out_shape=[pltpu.VMEM(cut, jnp.bfloat16)] * slabs
        + [pltpu.VMEM((pack_rows(terms, taps), angles), jnp.bfloat16) for terms in (early, late)],
        in_specs=[FAR] * 5,
        out_specs=[WHOLE] * (slabs + 2),
        scratch_shapes=[pltpu.VMEM(value.shape, value.dtype) for value in tables_in]
        + [pltpu.SemaphoreType.DMA((slabs, 2)), pltpu.SemaphoreType.DMA((4,))],
        compiler_params=params(2),
        cost_estimate=cost(1_000_000_000),
        name="cut",
    )(*[pltpu.with_memory_space_constraint(value, pltpu.HBM) for value in (echoes,) + tables_in])

    received = [quarters[0]] + [None] * (slabs - 1)
    for mask in range(slabs - 1, 0, -1):
        received[mask] = exchanged(quarters[mask], "rng", mask)

    masks = list(range(group - 1, 1, -1))
    masks = (masks[0::2] + [1], masks[1::2] + [1])
    mine, theirs = [], []
    for step in range(len(masks[0])):
        route = []
        for s in range(subs):
            for q in range(slabs):
                route.append((s * slabs + q, (s ^ masks[q & 1][step]) * slabs + q))
        mine.append(lax.ppermute(early_pack, ("sub", "rng"), route))
    for piece in mine[:-1]:
        theirs.append(exchanged(piece, "rng", 1))

    if groups == 1:
        blocks = received
    else:
        ordered = jnp.zeros((slabs,) + received[0].shape, received[0].dtype)
        for mask, block in enumerate(received):
            ordered = lax.dynamic_update_index_in_dim(ordered, block, slab ^ mask, 0)
        every = jnp.moveaxis(ordered, 0, 2).reshape(2, -1, subs, pulse_count)
        every = jnp.take(every, sub_map, axis=2)
        every = lax.ppermute(
            every,
            "sub",
            [(old, (old % groups) * group + old // groups) for old in range(subs)],
        ).reshape(2, -1, groups, group * pulse_count)
        lanes = [[g * group + m for g in range(groups)] for m in range(group)]
        every = lax.all_to_all(every, "sub", 2, 1, axis_index_groups=lanes, tiled=True)
        blocks = [every.reshape(2, rows, group * pulse_count)]

    edge_rows = jnp.stack([block[:, :HALO] for block in blocks])
    route = []
    for number in range(subs):
        for q in range(slabs):
            if number % group > 0:
                route.append((number * slabs + q, (number - 1) * slabs + q))
            elif q > 0:
                route.append((number * slabs + q, (number + group - 1) * slabs + q - 1))
    edge = lax.ppermute(edge_rows, ("sub", "rng"), route)

    def tables(terms, sources, held, lines, arrays):
        return pl.pallas_call(
            functools.partial(
                table_kernel,
                group,
                terms,
                sources,
                taps,
                half,
                rows,
                lines,
                range_rows,
                slabs * range_rows,
            ),
            out_shape=(
                jax.ShapeDtypeStruct((held, terms, angles, angles), jnp.bfloat16),
                jax.ShapeDtypeStruct((group, terms, 2, lines, angles), jnp.float32),
            ),
            in_specs=[WHOLE] * len(arrays),
            out_specs=(WHOLE, WHOLE),
            scratch_shapes=[
                pltpu.VMEM((group, terms, taps, angles), jnp.float32),
                pltpu.VMEM((group, 3, terms, angles), jnp.float32),
                pltpu.VMEM((15, angles // 128, group * terms, 128), jnp.float32),
            ],
            compiler_params=params(4),
            cost_estimate=cost(2_000_000_000),
        )(*arrays)

    bands, waves = tables(early, masks, group, rows + 8, [early_pack, *mine, *theirs])

    chunk_rows = rows // 2
    near = group // 2

    def form(first, count):
        return pl.pallas_call(
            functools.partial(form_kernel, group, pulse_count, len(blocks), first, count),
            out_shape=jax.ShapeDtypeStruct((group, 2, 2, count, half), jnp.float32),
            in_specs=[SCALARS] + [WHOLE] * (len(blocks) + 1),
            out_specs=WHOLE,
            compiler_params=params(6),
            cost_estimate=cost(1_000_000_000),
        )(sub_map, *blocks, steering)

    piece = 4 * chunk_rows + 8

    def merge(chunk, arrays, sizes):
        edges = [pltpu.VMEM((group, 2, 2, 16, half), jnp.float32)] if chunk == 1 else []
        return pl.pallas_call(
            functools.partial(
                merge_kernel, group, segments, chunk, chunk_rows, pulse_count, len(blocks)
            ),
            out_shape=[jax.ShapeDtypeStruct((size, half), jnp.bfloat16) for size in sizes],
            in_specs=([SCALARS] if chunk == 1 else []) + [WHOLE] * (len(arrays) - chunk),
            out_specs=[WHOLE] * group,
            scratch_shapes=edges
            + [pltpu.VMEM((group, 2, 2, chunk_rows + 16, half), jnp.float32)] * (segments - 1),
            compiler_params=params(8),
            cost_estimate=cost(4_000_000_000),
        )(*arrays)

    order = send_order(group)
    arrived = {}

    def send(mask, chunk, value):
        arrived[mask, chunk] = exchanged(value, "sub", mask)

    upper = merge(0, [form(0, chunk_rows + 16), bands, waves], [piece] * group)
    for mask in range(near, group):
        send(mask, 0, upper[mask])
    lower = merge(
        1,
        [sub_map, form(chunk_rows, chunk_rows), edge, steering, bands, waves]
        + list(upper[:near]),
        [2 * piece] * near + [piece] * near,
    )
    for mask in range(near, group):
        send(mask, 1, lower[mask])
    for mask in range(1, near):
        send(mask, None, lower[mask])
    arrived[0, None] = lower[0]

    last_bands, last_waves = tables(late, None, 1, rows, [late_pack])
    result = None
    turns = [
        [(0, None)] + order[:near],
        order[near:-2],
        order[-2:-1],
        order[-1:],
    ]
    for chosen in turns:
        count = len(chosen)
        jobs = []
        for source, (mask, chunk) in enumerate(chosen):
            if chunk is None:
                jobs += [(source, 0, mask, 0), (source, piece, mask, 1)]
            else:
                jobs.append((source, 0, mask, chunk))
        previous = [] if result is None else [result]
        result = pl.pallas_call(
            functools.partial(final_kernel, jobs, count, group, chunk_rows, result is None),
            out_shape=jax.ShapeDtypeStruct((2, range_rows, angles), jnp.bfloat16),
            in_specs=[WHOLE] * (count + 2) + [FAR] * len(previous),
            out_specs=FAR,
            scratch_shapes=[
                pltpu.VMEM((len(jobs), 4, chunk_rows + 8, half), jnp.float32),
                pltpu.VMEM((len(jobs), 2, chunk_rows, angles), jnp.bfloat16),
                pltpu.SemaphoreType.DMA((len(jobs), 2)),
            ],
            input_output_aliases={count + 2: 0} if previous else {},
            compiler_params=params(6),
            cost_estimate=cost(1_000_000_000),
            name="final",
        )(*[arrived[key] for key in chosen], last_bands, last_waves, *previous)
    return result


def solution(mesh):
    in_specs = (
        P(None, None, "sub", "rng"),
        P(),
        P(),
        P("sub", None, None, None),
        P("sub", None, None, None, None),
        P("sub", None, None, None),
        P("sub", None, None, None),
    )
    return jax.shard_map(
        on_device, mesh=mesh, in_specs=in_specs, out_specs=P(None, "rng", "sub"), check_vma=False
    )
```

```python
import functools

import jax
import jax.numpy as jnp
from jax import lax
from jax.experimental import pallas as pl
from jax.experimental.pallas import tpu as pltpu
from jax.sharding import PartitionSpec as P


HALO = 8
KINDS = 6
MIB = 1 << 20
WHOLE = pl.BlockSpec(memory_space=pltpu.VMEM)
SCALARS = pl.BlockSpec(memory_space=pltpu.SMEM)
FAR = pl.BlockSpec(memory_space=pltpu.HBM)


def exchanged(block, axis, mask):
    count = lax.axis_size(axis)
    return lax.ppermute(block, axis, [(source, source ^ mask) for source in range(count)])


def params(mib):
    return pltpu.CompilerParams(vmem_limit_bytes=mib * MIB)


def cost(flops):
    return pl.CostEstimate(flops=flops, bytes_accessed=MIB, transcendentals=0)


def product(left, right):
    return (
        left[0] * right[0] - left[1] * right[1],
        left[0] * right[1] + left[1] * right[0],
    )


def pack_rows(terms, taps):
    return -(-(terms * (taps + KINDS)) // 8) * 8


def cut_kernel(slabs, segments, taps, half, echoes, offset, weight, fraction, rate, *refs):
    slices, packs = refs[:slabs], refs[slabs : slabs + 2]
    held, semaphores, small = refs[slabs + 2 : slabs + 6], refs[slabs + 6], refs[slabs + 7]
    group = 1 << segments
    member = lax.axis_index("sub") & (group - 1)
    slab = lax.axis_index("rng")
    loads = [
        pltpu.make_async_copy(source, target, small.at[index])
        for index, (source, target) in enumerate(zip((offset, weight, fraction, rate), held))
    ]
    copies = []
    for mask in range(slabs - 1, -1, -1):
        for c in range(2):
            copies.append(
                pltpu.make_async_copy(
                    echoes.at[c, slab ^ mask], slices[mask].at[c], semaphores.at[mask, c]
                )
            )
    for copy in loads + copies:
        copy.start()
    for copy in loads:
        copy.wait()
    offset, weight, fraction, rate = held
    angles = weight.shape[-1]
    for pack, chosen in ((packs[0], range(segments - 1)), (packs[1], (segments - 1,))):
        kinds = [[] for _ in range(KINDS)]
        terms = 2 * len(chosen)
        for index, segment in enumerate(chosen):
            base = ((member >> segment) & 1) * half
            kinds[0].append((offset[0, segment] - base).astype(jnp.float32))
            slot = 1
            for source, count in ((fraction, 2), (rate, 3)):
                rest = source[0, segment]
                for _ in range(count):
                    part = rest.astype(jnp.bfloat16).astype(jnp.float32)
                    kinds[slot].append(part)
                    rest = rest - part
                    slot += 1
            for child in range(2):
                term = index * 2 + child
                pack[term * taps : (term + 1) * taps, :] = weight[0, segment, child]
        rows = [piece for kind in kinds for piece in kind]
        padding = pack_rows(terms, taps) - terms * (taps + KINDS)
        if padding:
            rows.append(jnp.zeros((padding, angles), jnp.float32))
        pack[terms * taps :, :] = jnp.concatenate(rows, axis=0).astype(jnp.bfloat16)
    for copy in copies:
        copy.wait()


def table_kernel(members, terms, masks, taps, half, rows, lines, range_rows, total_range, *refs):
    steps = len(masks[0]) if masks else 0
    swapped = steps - 1 if masks else 0
    own, mine, theirs = refs[0], refs[1 : 1 + steps], refs[1 + steps : 1 + steps + swapped]
    bands, waves, weights, raw, dense = refs[1 + steps + swapped :]
    angles = bands.shape[-1]
    member = lax.axis_index("sub") & (members - 1)
    slab = lax.axis_index("rng")

    def fill(piece, section):
        values = piece[...].astype(jnp.float32)
        for term in range(terms):
            weights[section, term] = values[term * taps : (term + 1) * taps]
        start = terms * taps
        kind = [values[start + k * terms : start + (k + 1) * terms] for k in range(KINDS)]
        raw[section, 0] = kind[0]
        raw[section, 1] = kind[1] + kind[2]
        raw[section, 2] = kind[3] + kind[4] + kind[5]

    if masks:
        core = slab & 1
        fill(own, member)
        for received, holder in ((mine, core), (theirs, 1 - core)):
            for step, piece in enumerate(received):
                fill(piece, member ^ jnp.where(holder == 0, masks[0][step], masks[1][step]))
        first_row, row_step = slab * range_rows + member * rows, 0
    else:
        for section in range(members):
            fill(own, section)
        first_row, row_step = slab * range_rows, rows

    for start in range(0, members * terms, 8):
        place = slice(start, start + 8)
        sections = range(start // terms, (start + 8) // terms)

        def keep(kind, value):
            for part in range(angles // 128):
                dense[kind, part, place] = value[:, part * 128 : (part + 1) * 128]

        given = [
            jnp.concatenate([raw[section, kind] for section in sections], axis=0)
            for kind in range(3)
        ]
        keep(0, given[0])
        keep(1, given[1])
        rate = given[2]
        number = start + lax.broadcasted_iota(jnp.int32, (8, angles), 0)
        first = first_row + (number // terms) * row_step
        angle = first.astype(jnp.float32) / float(total_range) * rate
        keep(3, jnp.cos(angle))
        keep(4, jnp.sin(angle))
        angle = rate / float(total_range)
        turn = jnp.cos(angle), jnp.sin(angle)
        for power in range(5):
            keep(5 + 2 * power, turn[0])
            keep(6 + 2 * power, turn[1])
            turn = product(turn, turn)

    sub_rows = lax.broadcasted_iota(jnp.int32, (8, 128), 0)

    def entry(index, carry):
        section, term = index // terms, index % terms
        for part in range(angles // 128):
            lanes = pl.ds(part * 128, 128)

            def row(kind):
                return dense[kind, part, pl.ds(index, 1), :]

            def bands_of():
                weight = weights[section, term, :, lanes]
                offset = row(0).astype(jnp.int32)
                fraction = row(1)
                tap = sub_rows - offset
                block_of = -(tap >> 3)
                picked = jnp.take_along_axis(weight, tap & 7, axis=0)
                near, far = picked * (1.0 - fraction), picked * fraction
                for block in range(half // 16):
                    hits = [block_of == 2 * block + step for step in range(2)]
                    for source, base in ((near, 0), (far, half)):
                        pair = [jnp.where(hit, source, 0.0) for hit in hits]
                        place = slice(base + block * 16, base + (block + 1) * 16)
                        bands[section, term, place, lanes] = jnp.concatenate(pair, axis=0).astype(
                            jnp.bfloat16
                        )

            if masks:
                bands_of()
            else:
                pl.when(section == 0)(bands_of)
            wave = tuple(jnp.broadcast_to(row(3 + c), (8, 128)) for c in range(2))
            for power in range(3):
                chosen = (sub_rows >> power) & 1 == 1
                wave = product(
                    wave,
                    (
                        jnp.where(chosen, row(5 + 2 * power), 1.0),
                        jnp.where(chosen, row(6 + 2 * power), 0.0),
                    ),
                )
            eight, sixteen = (row(11), row(12)), (row(13), row(14))
            chain = [wave, product(wave, eight)]
            for block in range(lines // 8):
                wave = chain[block % 2]
                for c in range(2):
                    waves[section, term, c, block * 8 : (block + 1) * 8, lanes] = wave[c]
                chain[block % 2] = product(wave, sixteen)
        return carry

    lax.fori_loop(0, members * terms, entry, 0)


def formed(steering, re_parts, im_parts):
    rows = jnp.concatenate(re_parts + im_parts, axis=0)
    count = rows.shape[0] // 2
    by_real, by_imag = [
        lax.dot_general(
            rows, steering[c], (((1,), (1,)), ((), ())), preferred_element_type=jnp.float32
        )
        for c in range(2)
    ]
    return by_real[:count] - by_imag[count:], by_imag[:count] + by_real[count:]


def place_of(sub_map, group, slabs, slab, index):
    if slabs == 1:
        return index
    per_slab = group // slabs
    block = (slab ^ (index // per_slab)) * per_slab + index % per_slab
    place = 0
    for section in range(group):
        place = jnp.where(sub_map[section] == block, section, place)
    return place


def form_kernel(group, pulse_count, sources, first, count, sub_map, *refs):
    blocks, steering, image = refs[:sources], refs[sources], refs[sources + 1]
    half = image.shape[-1]
    per_source = group // sources
    slab = lax.axis_index("rng")
    for source in range(sources):
        for start in range(0, per_source, 2):
            pieces = range(start, min(start + 2, per_source))
            parts = [
                [
                    blocks[source][
                        c, first : first + count, piece * pulse_count : (piece + 1) * pulse_count
                    ]
                    for piece in pieces
                ]
                for c in range(2)
            ]
            values = formed(steering, *parts)
            for index, piece in enumerate(pieces):
                target = place_of(sub_map, group, sources, slab, source * per_source + piece)
                for c in range(2):
                    value = values[c][index * count : (index + 1) * count]
                    for window in range(2):
                        image[target, c, window] = value[:, window * half : (window + 1) * half]


def turned(values, block, first):
    total = None
    for value, wave in values:
        part = value[block * 16 : block * 16 + 8], value[block * 16 + 8 : block * 16 + 16]
        start = first + block * 8
        turn = tuple(wave[c, start : start + 8] for c in range(2))
        term = product(turn, part)
        total = term if total is None else (total[0] + term[0], total[1] + term[1])
    return total


def contracted(rows_of, lines, matrix):
    pieces = []
    for block in range(lines // 8):
        sides = []
        for start in (block * 8, block * 8 + 1):
            both = [rows_of(c, start) for c in range(2)]
            sides.append(jnp.concatenate(both, axis=0).astype(jnp.bfloat16))
        pieces.append(jnp.concatenate(sides, axis=1))
    return jnp.dot(jnp.concatenate(pieces, axis=0), matrix, preferred_element_type=jnp.float32)


def merge_kernel(group, segments, chunk, first, rows, whole, pulse_count, sources, *refs):
    if chunk == 0:
        image, bands, waves = refs[:3]
        refs = refs[3:]
    else:
        sub_map, image, edge, steering, bands, waves = refs[:6]
        kept, refs = dict(zip(whole, refs[6:])), refs[6 + len(whole) :]
        edges, refs = refs[group], refs[:group] + refs[group + 1 :]
    outs, stores = refs[:group], refs[group:]
    half = image.shape[-1]
    member = lax.axis_index("sub") & (group - 1)
    per_source = group // sources

    if chunk == 1:
        below = lax.axis_index("rng")
        if sources > 1:
            below = jnp.minimum(below + jnp.where(member == group - 1, 1, 0), sources - 1)
        parts = [[], []]
        for source in range(sources):
            for piece in range(per_source):
                columns = slice(piece * pulse_count, (piece + 1) * pulse_count)
                for c in range(2):
                    parts[c].append(edge[source, c, :, columns])
        values = formed(steering, *parts)
        for index in range(group):
            target = place_of(sub_map, group, sources, below, index)
            for c in range(2):
                value = values[c][index * HALO : (index + 1) * HALO]
                for window in range(2):
                    edges[target, c, window, 0:HALO] = value[:, window * half : (window + 1) * half]
                    edges[target, c, window, HALO:] = jnp.zeros((8, half), jnp.float32)

    def rows_of(segment, section, window, c, start):
        if segment > 0:
            return stores[segment - 1][section, c, window, start : start + 8]
        if chunk == 0 or start + 8 <= rows:
            return image[section, c, window, start : start + 8]
        if start >= rows:
            return edges[section, c, window, start - rows : start - rows + 8]
        return jnp.concatenate(
            [
                image[section, c, window, start:rows],
                edges[section, c, window, 0 : start + 8 - rows],
            ],
            axis=0,
        )

    for segment in range(segments - 1):

        def step(section, carry, segment=segment):
            low = section & ~(1 << segment)
            window = (section >> segment) & 1
            values = []
            for child in range(2):
                source, term = low | (child << segment), segment * 2 + child
                reader = functools.partial(rows_of, segment, source, window)
                value = contracted(reader, rows + 8, bands[section, term])
                values.append((value, waves.at[section, term]))
            for block in range(rows // 8 + 1):
                for c, total in enumerate(turned(values, block, first)):
                    for side in range(2):
                        stores[segment][section, c, side, block * 8 : block * 8 + 8] = total[
                            :, side * half : (side + 1) * half
                        ]
            for c in range(2):
                for side in range(2):
                    stores[segment][section, c, side, rows + 8 :] = jnp.zeros(
                        (8, half), jnp.float32
                    )
            return carry

        lax.fori_loop(0, group, step, 0, unroll=4)

    last = stores[segments - 2]
    size = 4 * rows + 8
    for mask in range(group):
        section = member ^ mask
        low = section & ~(1 << (segments - 1))
        window = (section >> (segments - 1)) & 1
        base = 0
        if chunk == 1 and mask in whole:
            base = kept[mask].shape[0]
            outs[mask][0:base] = kept[mask][...]
        extra = []
        for child in range(2):
            for c in range(2):
                start = base + (child * 2 + c) * rows
                source = last.at[low | (child << (segments - 1)), c, window]
                outs[mask][start : start + rows] = source[0:rows].astype(jnp.bfloat16)
                extra.append(source[rows : rows + 1])
        extra.append(jnp.zeros((4, half), jnp.float32))
        outs[mask][base + 4 * rows : base + size] = jnp.concatenate(extra, axis=0).astype(
            jnp.bfloat16
        )


def final_kernel(jobs, count, group, block_rows, fresh, *refs):
    parts, (bands, waves) = refs[:count], refs[count : count + 2]
    result, store, mine, semaphores = refs[count + (2 if fresh else 3) :]
    half = store.shape[-1]
    member = lax.axis_index("sub") & (group - 1)
    copies = []
    for index, (source, base, mask, first, rows) in enumerate(jobs):
        part = parts[source]
        extra = part[base + 4 * rows : base + 4 * rows + 8].astype(jnp.float32)
        for side in range(4):
            start = base + side * rows
            store[index, side, 0:rows] = part[start : start + rows].astype(jnp.float32)
            store[index, side, rows : rows + 8] = jnp.broadcast_to(extra[side : side + 1], (8, half))
        values = []
        for child in range(2):

            def rows_of(c, start, index=index, child=child):
                return store[index, child * 2 + c, start : start + 8]

            value = contracted(rows_of, rows, bands[0, child])
            values.append((value, waves.at[member ^ mask, child]))
        held = None
        for block in range(rows // 8):
            totals = turned(values, block, first)
            if block % 2 == 0:
                held = totals
                continue
            for c in range(2):
                mine[index, c, block * 8 - 8 : block * 8 + 8] = jnp.concatenate(
                    [held[c], totals[c]], axis=0
                ).astype(jnp.bfloat16)
        start = pl.multiple_of((member ^ mask) * block_rows + first, 16)
        for c in range(2):
            copy = pltpu.make_async_copy(
                mine.at[index, c, 0:rows], result.at[c, pl.ds(start, rows)], semaphores.at[index, c]
            )
            copy.start()
            copies.append(copy)
    for copy in copies:
        copy.wait()


def send_order(group):
    far, near = list(range(group - 1, group // 2 - 1, -1)), list(range(group // 2 - 1, 0, -1))
    upper = [(mask, 0) for mask in far[:2]]
    rest = [(mask, None) for mask in far[2:3] + near + far[3:]]
    return upper, rest + [(mask, 1) for mask in far[:2]]


def on_device(echoes, steering, sub_map, band_offset, interp_weight, range_frac, phase_rate):
    slabs = lax.axis_size("rng")
    subs = lax.axis_size("sub")
    segments, taps = interp_weight.shape[1], interp_weight.shape[3]
    group = 1 << segments
    groups = subs // group
    angles, pulse_count = steering.shape[1], steering.shape[2]
    half = angles // 2
    slab = lax.axis_index("rng")
    range_rows = echoes.shape[2] * subs
    rows = range_rows // group
    early, late = 2 * (segments - 1), 2

    cut = (2,) + echoes.shape[2:]
    tables_in = (band_offset, interp_weight, range_frac, phase_rate)
    *quarters, early_pack, late_pack = pl.pallas_call(
        functools.partial(cut_kernel, slabs, segments, taps, half),
        out_shape=[pltpu.VMEM(cut, jnp.bfloat16)] * slabs
        + [pltpu.VMEM((pack_rows(terms, taps), angles), jnp.bfloat16) for terms in (early, late)],
        in_specs=[FAR] * 5,
        out_specs=[WHOLE] * (slabs + 2),
        scratch_shapes=[pltpu.VMEM(value.shape, value.dtype) for value in tables_in]
        + [pltpu.SemaphoreType.DMA((slabs, 2)), pltpu.SemaphoreType.DMA((4,))],
        compiler_params=params(2),
        cost_estimate=cost(1_000_000_000),
        name="cut",
    )(*[pltpu.with_memory_space_constraint(value, pltpu.HBM) for value in (echoes,) + tables_in])

    received = [quarters[0]] + [None] * (slabs - 1)
    for mask in range(slabs - 1, 0, -1):
        received[mask] = exchanged(quarters[mask], "rng", mask)

    masks = list(range(group - 1, 1, -1))
    masks = (masks[0::2] + [1], masks[1::2] + [1])
    mine, theirs = [], []
    for step in range(len(masks[0])):
        route = []
        for s in range(subs):
            for q in range(slabs):
                route.append((s * slabs + q, (s ^ masks[q & 1][step]) * slabs + q))
        mine.append(lax.ppermute(early_pack, ("sub", "rng"), route))
    for piece in mine[:-1]:
        theirs.append(exchanged(piece, "rng", 1))

    if groups == 1:
        blocks = received
    else:
        ordered = jnp.zeros((slabs,) + received[0].shape, received[0].dtype)
        for mask, block in enumerate(received):
            ordered = lax.dynamic_update_index_in_dim(ordered, block, slab ^ mask, 0)
        every = jnp.moveaxis(ordered, 0, 2).reshape(2, -1, subs, pulse_count)
        every = jnp.take(every, sub_map, axis=2)
        every = lax.ppermute(
            every,
            "sub",
            [(old, (old % groups) * group + old // groups) for old in range(subs)],
        ).reshape(2, -1, groups, group * pulse_count)
        lanes = [[g * group + m for g in range(groups)] for m in range(group)]
        every = lax.all_to_all(every, "sub", 2, 1, axis_index_groups=lanes, tiled=True)
        blocks = [every.reshape(2, rows, group * pulse_count)]

    edge_rows = jnp.stack([block[:, :HALO] for block in blocks])
    route = []
    for number in range(subs):
        for q in range(slabs):
            if number % group > 0:
                route.append((number * slabs + q, (number - 1) * slabs + q))
            elif q > 0:
                route.append((number * slabs + q, (number + group - 1) * slabs + q - 1))
    edge = lax.ppermute(edge_rows, ("sub", "rng"), route)

    def tables(terms, sources, held, lines, arrays):
        return pl.pallas_call(
            functools.partial(
                table_kernel,
                group,
                terms,
                sources,
                taps,
                half,
                rows,
                lines,
                range_rows,
                slabs * range_rows,
            ),
            out_shape=(
                jax.ShapeDtypeStruct((held, terms, angles, angles), jnp.bfloat16),
                jax.ShapeDtypeStruct((group, terms, 2, lines, angles), jnp.float32),
            ),
            in_specs=[WHOLE] * len(arrays),
            out_specs=(WHOLE, WHOLE),
            scratch_shapes=[
                pltpu.VMEM((group, terms, taps, angles), jnp.float32),
                pltpu.VMEM((group, 3, terms, angles), jnp.float32),
                pltpu.VMEM((15, angles // 128, group * terms, 128), jnp.float32),
            ],
            compiler_params=params(4),
            cost_estimate=cost(2_000_000_000),
        )(*arrays)

    bands, waves = tables(early, masks, group, rows + 8, [early_pack, *mine, *theirs])

    cut_row = -(-rows * 5 // 8 // 16) * 16
    bounds = ((0, cut_row), (cut_row, rows - cut_row))
    pieces = [4 * count + 8 for _, count in bounds]
    upper_order, lower_order = send_order(group)
    split = [mask for mask, _ in upper_order]
    whole_masks = [mask for mask in range(group) if mask not in split]

    def form(first, count):
        return pl.pallas_call(
            functools.partial(form_kernel, group, pulse_count, len(blocks), first, count),
            out_shape=jax.ShapeDtypeStruct((group, 2, 2, count, half), jnp.float32),
            in_specs=[SCALARS] + [WHOLE] * (len(blocks) + 1),
            out_specs=WHOLE,
            compiler_params=params(6),
            cost_estimate=cost(1_000_000_000),
        )(sub_map, *blocks, steering)

    def merge(chunk, arrays, sizes):
        first, count = bounds[chunk]
        edges = [pltpu.VMEM((group, 2, 2, 16, half), jnp.float32)] if chunk == 1 else []
        return pl.pallas_call(
            functools.partial(
                merge_kernel,
                group,
                segments,
                chunk,
                first,
                count,
                whole_masks,
                pulse_count,
                len(blocks),
            ),
            out_shape=[jax.ShapeDtypeStruct((size, half), jnp.bfloat16) for size in sizes],
            in_specs=([SCALARS] if chunk == 1 else []) + [WHOLE] * (len(arrays) - chunk),
            out_specs=[WHOLE] * group,
            scratch_shapes=edges
            + [pltpu.VMEM((group, 2, 2, count + 16, half), jnp.float32)] * (segments - 1),
            compiler_params=params(8),
            cost_estimate=cost(4_000_000_000),
        )(*arrays)

    arrived = {}

    def send(mask, chunk, value):
        arrived[mask, chunk] = exchanged(value, "sub", mask)

    upper = merge(0, [form(0, cut_row + 16), bands, waves], pieces[:1] * group)
    for mask, chunk in upper_order:
        send(mask, chunk, upper[mask])
    lower = merge(
        1,
        [sub_map, form(*bounds[1]), edge, steering, bands, waves]
        + [upper[mask] for mask in whole_masks],
        [sum(pieces) if mask in whole_masks else pieces[1] for mask in range(group)],
    )
    for mask, chunk in lower_order:
        send(mask, chunk, lower[mask])
    arrived[0, None] = lower[0]

    last_bands, last_waves = tables(late, None, 1, rows, [late_pack])
    result = None
    turns = [[(0, None)] + upper_order, lower_order[:-3]] + [[key] for key in lower_order[-3:]]
    for chosen in turns:
        count = len(chosen)
        jobs = []
        for source, (mask, chunk) in enumerate(chosen):
            for part in (0, 1) if chunk is None else (chunk,):
                base = pieces[0] if chunk is None and part == 1 else 0
                jobs.append((source, base, mask) + bounds[part])
        previous = [] if result is None else [result]
        result = pl.pallas_call(
            functools.partial(final_kernel, jobs, count, group, rows, result is None),
            out_shape=jax.ShapeDtypeStruct((2, range_rows, angles), jnp.bfloat16),
            in_specs=[WHOLE] * (count + 2) + [FAR] * len(previous),
            out_specs=FAR,
            scratch_shapes=[
                pltpu.VMEM((len(jobs), 4, cut_row + 8, half), jnp.float32),
                pltpu.VMEM((len(jobs), 2, cut_row, angles), jnp.bfloat16),
                pltpu.SemaphoreType.DMA((len(jobs), 2)),
            ],
            input_output_aliases={count + 2: 0} if previous else {},
            compiler_params=params(6),
            cost_estimate=cost(1_000_000_000),
            name="final",
        )(*[arrived[key] for key in chosen], last_bands, last_waves, *previous)
    return result


def solution(mesh):
    in_specs = (
        P(None, None, "sub", "rng"),
        P(),
        P(),
        P("sub", None, None, None),
        P("sub", None, None, None, None),
        P("sub", None, None, None),
        P("sub", None, None, None),
    )
    return jax.shard_map(
        on_device, mesh=mesh, in_specs=in_specs, out_specs=P(None, "rng", "sub"), check_vma=False
    )
```

```python
import functools

import jax
import jax.numpy as jnp
from jax import lax
from jax.experimental import pallas as pl
from jax.experimental.pallas import tpu as pltpu
from jax.sharding import PartitionSpec as P


HALO = 8
KINDS = 6
MIB = 1 << 20
WHOLE = pl.BlockSpec(memory_space=pltpu.VMEM)
SCALARS = pl.BlockSpec(memory_space=pltpu.SMEM)
FAR = pl.BlockSpec(memory_space=pltpu.HBM)


def exchanged(block, axis, mask):
    count = lax.axis_size(axis)
    return lax.ppermute(block, axis, [(source, source ^ mask) for source in range(count)])


def params(mib):
    return pltpu.CompilerParams(vmem_limit_bytes=mib * MIB)


def cost(flops):
    return pl.CostEstimate(flops=flops, bytes_accessed=MIB, transcendentals=0)


def product(left, right):
    return (
        left[0] * right[0] - left[1] * right[1],
        left[0] * right[1] + left[1] * right[0],
    )


def pack_rows(terms, taps):
    return -(-(terms * (taps + KINDS)) // 8) * 8


def cut_kernel(slabs, segments, taps, half, echoes, offset, weight, fraction, rate, *refs):
    slices, packs = refs[:slabs], refs[slabs : slabs + 2]
    held, semaphores, small = refs[slabs + 2 : slabs + 6], refs[slabs + 6], refs[slabs + 7]
    group = 1 << segments
    member = lax.axis_index("sub") & (group - 1)
    slab = lax.axis_index("rng")
    loads = [
        pltpu.make_async_copy(source, target, small.at[index])
        for index, (source, target) in enumerate(zip((offset, weight, fraction, rate), held))
    ]
    copies = []
    for mask in range(slabs - 1, -1, -1):
        for c in range(2):
            copies.append(
                pltpu.make_async_copy(
                    echoes.at[c, slab ^ mask], slices[mask].at[c], semaphores.at[mask, c]
                )
            )
    for copy in loads + copies:
        copy.start()
    for copy in loads:
        copy.wait()
    offset, weight, fraction, rate = held
    angles = weight.shape[-1]
    for copies_of, chosen in (
        ([packs[0].at[index] for index in range(group)], range(segments - 1)),
        ([packs[1]], (segments - 1,)),
    ):
        kinds = [[] for _ in range(KINDS)]
        terms = 2 * len(chosen)
        for index, segment in enumerate(chosen):
            base = ((member >> segment) & 1) * half
            kinds[0].append((offset[0, segment] - base).astype(jnp.float32))
            slot = 1
            for source, count in ((fraction, 2), (rate, 3)):
                rest = source[0, segment]
                for _ in range(count):
                    part = rest.astype(jnp.bfloat16).astype(jnp.float32)
                    kinds[slot].append(part)
                    rest = rest - part
                    slot += 1
            for child in range(2):
                term = index * 2 + child
                for pack in copies_of:
                    pack[term * taps : (term + 1) * taps, :] = weight[0, segment, child]
        rows = [piece for kind in kinds for piece in kind]
        padding = pack_rows(terms, taps) - terms * (taps + KINDS)
        if padding:
            rows.append(jnp.zeros((padding, angles), jnp.float32))
        tail = jnp.concatenate(rows, axis=0).astype(jnp.bfloat16)
        for pack in copies_of:
            pack[terms * taps :, :] = tail
    for copy in copies:
        copy.wait()


def table_kernel(members, terms, shared, taps, half, rows, lines, range_rows, total_range, *refs):
    packs, bands, waves, weights, raw, dense = refs
    angles = bands.shape[-1]
    member = lax.axis_index("sub") & (members - 1)
    slab = lax.axis_index("rng")

    def fill(piece, section):
        values = piece.astype(jnp.float32)
        for term in range(terms):
            weights[section, term] = values[term * taps : (term + 1) * taps]
        start = terms * taps
        kind = [values[start + k * terms : start + (k + 1) * terms] for k in range(KINDS)]
        raw[section, 0] = kind[0]
        raw[section, 1] = kind[1] + kind[2]
        raw[section, 2] = kind[3] + kind[4] + kind[5]

    for section in range(members):
        fill(packs[section] if shared else packs[...], section)
    if shared:
        first_row, row_step = slab * range_rows + member * rows, 0
    else:
        first_row, row_step = slab * range_rows, rows

    for start in range(0, members * terms, 8):
        place = slice(start, start + 8)
        sections = range(start // terms, (start + 8) // terms)

        def keep(kind, value):
            for part in range(angles // 128):
                dense[kind, part, place] = value[:, part * 128 : (part + 1) * 128]

        given = [
            jnp.concatenate([raw[section, kind] for section in sections], axis=0)
            for kind in range(3)
        ]
        keep(0, given[0])
        keep(1, given[1])
        rate = given[2]
        number = start + lax.broadcasted_iota(jnp.int32, (8, angles), 0)
        first = first_row + (number // terms) * row_step
        angle = first.astype(jnp.float32) / float(total_range) * rate
        keep(3, jnp.cos(angle))
        keep(4, jnp.sin(angle))
        angle = rate / float(total_range)
        turn = jnp.cos(angle), jnp.sin(angle)
        for power in range(5):
            keep(5 + 2 * power, turn[0])
            keep(6 + 2 * power, turn[1])
            turn = product(turn, turn)

    sub_rows = lax.broadcasted_iota(jnp.int32, (8, 128), 0)

    def entry(index, carry):
        section, term = index // terms, index % terms
        for part in range(angles // 128):
            lanes = pl.ds(part * 128, 128)

            def row(kind):
                return dense[kind, part, pl.ds(index, 1), :]

            def bands_of():
                weight = weights[section, term, :, lanes]
                offset = row(0).astype(jnp.int32)
                fraction = row(1)
                tap = sub_rows - offset
                block_of = -(tap >> 3)
                picked = jnp.take_along_axis(weight, tap & 7, axis=0)
                near, far = picked * (1.0 - fraction), picked * fraction
                for block in range(half // 16):
                    hits = [block_of == 2 * block + step for step in range(2)]
                    for source, base in ((near, 0), (far, half)):
                        pair = [jnp.where(hit, source, 0.0) for hit in hits]
                        place = slice(base + block * 16, base + (block + 1) * 16)
                        bands[section, term, place, lanes] = jnp.concatenate(pair, axis=0).astype(
                            jnp.bfloat16
                        )

            if shared:
                bands_of()
            else:
                pl.when(section == 0)(bands_of)
            wave = tuple(jnp.broadcast_to(row(3 + c), (8, 128)) for c in range(2))
            for power in range(3):
                chosen = (sub_rows >> power) & 1 == 1
                wave = product(
                    wave,
                    (
                        jnp.where(chosen, row(5 + 2 * power), 1.0),
                        jnp.where(chosen, row(6 + 2 * power), 0.0),
                    ),
                )
            eight, sixteen = (row(11), row(12)), (row(13), row(14))
            chain = [wave, product(wave, eight)]
            for block in range(lines // 8):
                wave = chain[block % 2]
                for c in range(2):
                    waves[section, term, c, block * 8 : (block + 1) * 8, lanes] = wave[c]
                chain[block % 2] = product(wave, sixteen)
        return carry

    lax.fori_loop(0, members * terms, entry, 0)


def formed(steering, re_parts, im_parts):
    rows = jnp.concatenate(re_parts + im_parts, axis=0)
    count = rows.shape[0] // 2
    by_real, by_imag = [
        lax.dot_general(
            rows, steering[c], (((1,), (1,)), ((), ())), preferred_element_type=jnp.float32
        )
        for c in range(2)
    ]
    return by_real[:count] - by_imag[count:], by_imag[:count] + by_real[count:]


def place_of(sub_map, group, slabs, slab, index):
    if slabs == 1:
        return index
    per_slab = group // slabs
    block = (slab ^ (index // per_slab)) * per_slab + index % per_slab
    place = 0
    for section in range(group):
        place = jnp.where(sub_map[section] == block, section, place)
    return place


def form_kernel(group, pulse_count, sources, first, count, sub_map, *refs):
    blocks, steering, image = refs[:sources], refs[sources], refs[sources + 1]
    half = image.shape[-1]
    per_source = group // sources
    slab = lax.axis_index("rng")
    for source in range(sources):
        for start in range(0, per_source, 2):
            pieces = range(start, min(start + 2, per_source))
            parts = [
                [
                    blocks[source][
                        c, first : first + count, piece * pulse_count : (piece + 1) * pulse_count
                    ]
                    for piece in pieces
                ]
                for c in range(2)
            ]
            values = formed(steering, *parts)
            for index, piece in enumerate(pieces):
                target = place_of(sub_map, group, sources, slab, source * per_source + piece)
                for c in range(2):
                    value = values[c][index * count : (index + 1) * count]
                    for window in range(2):
                        image[target, c, window] = value[:, window * half : (window + 1) * half]


def turned(values, block):
    total = None
    for value, wave in values:
        part = value[block * 16 : block * 16 + 8], value[block * 16 + 8 : block * 16 + 16]
        turn = tuple(wave[c, block * 8 : block * 8 + 8] for c in range(2))
        term = product(turn, part)
        total = term if total is None else (total[0] + term[0], total[1] + term[1])
    return total


def contracted(rows_of, lines, matrix):
    pieces = []
    for block in range(lines // 8):
        sides = []
        for start in (block * 8, block * 8 + 1):
            both = [rows_of(c, start) for c in range(2)]
            sides.append(jnp.concatenate(both, axis=0).astype(jnp.bfloat16))
        pieces.append(jnp.concatenate(sides, axis=1))
    return jnp.dot(jnp.concatenate(pieces, axis=0), matrix, preferred_element_type=jnp.float32)


def merge_kernel(group, segments, rows, pulse_count, sources, sub_map, *refs):
    image, edge, steering, bands, waves = refs[:5]
    outs, edges, stores = refs[5 : 5 + group], refs[5 + group], refs[6 + group :]
    half = image.shape[-1]
    member = lax.axis_index("sub") & (group - 1)
    per_source = group // sources

    below = lax.axis_index("rng")
    if sources > 1:
        below = jnp.minimum(below + jnp.where(member == group - 1, 1, 0), sources - 1)
    parts = [[], []]
    for source in range(sources):
        for piece in range(per_source):
            columns = slice(piece * pulse_count, (piece + 1) * pulse_count)
            for c in range(2):
                parts[c].append(edge[source, c, :, columns])
    values = formed(steering, *parts)
    for index in range(group):
        target = place_of(sub_map, group, sources, below, index)
        for c in range(2):
            value = values[c][index * HALO : (index + 1) * HALO]
            for window in range(2):
                edges[target, c, window, 0:HALO] = value[:, window * half : (window + 1) * half]
                edges[target, c, window, HALO:] = jnp.zeros((8, half), jnp.float32)

    def rows_of(segment, section, window, c, start):
        if segment > 0:
            return stores[segment - 1][section, c, window, start : start + 8]
        if start + 8 <= rows:
            return image[section, c, window, start : start + 8]
        if start >= rows:
            return edges[section, c, window, start - rows : start - rows + 8]
        return jnp.concatenate(
            [
                image[section, c, window, start:rows],
                edges[section, c, window, 0 : start + 8 - rows],
            ],
            axis=0,
        )

    for segment in range(segments - 1):

        def step(section, carry, segment=segment):
            low = section & ~(1 << segment)
            window = (section >> segment) & 1
            values = []
            for child in range(2):
                source, term = low | (child << segment), segment * 2 + child
                reader = functools.partial(rows_of, segment, source, window)
                value = contracted(reader, rows + 8, bands[section, term])
                values.append((value, waves.at[section, term]))
            for block in range(rows // 8 + 1):
                for c, total in enumerate(turned(values, block)):
                    for side in range(2):
                        stores[segment][section, c, side, block * 8 : block * 8 + 8] = total[
                            :, side * half : (side + 1) * half
                        ]
            for c in range(2):
                for side in range(2):
                    stores[segment][section, c, side, rows + 8 :] = jnp.zeros(
                        (8, half), jnp.float32
                    )
            return carry

        lax.fori_loop(0, group, step, 0, unroll=4)

    last = stores[segments - 2]
    for mask in range(group):
        section = member ^ mask
        low = section & ~(1 << (segments - 1))
        window = (section >> (segments - 1)) & 1
        extra = []
        for child in range(2):
            for c in range(2):
                start = (child * 2 + c) * rows
                source = last.at[low | (child << (segments - 1)), c, window]
                outs[mask][start : start + rows] = source[0:rows].astype(jnp.bfloat16)
                extra.append(source[rows : rows + 1])
        extra.append(jnp.zeros((4, half), jnp.float32))
        outs[mask][4 * rows :] = jnp.concatenate(extra, axis=0).astype(jnp.bfloat16)


def final_kernel(masks, group, rows, first, *refs):
    count = len(masks)
    parts, (bands, waves) = refs[:count], refs[count : count + 2]
    result, store, mine, semaphores = refs[count + (2 if first else 3) :]
    half = store.shape[-1]
    member = lax.axis_index("sub") & (group - 1)
    copies = []
    for index, mask in enumerate(masks):
        part = parts[index]
        extra = part[4 * rows :].astype(jnp.float32)
        for side in range(4):
            store[index, side, 0:rows] = part[side * rows : (side + 1) * rows].astype(jnp.float32)
            store[index, side, rows:] = jnp.broadcast_to(extra[side : side + 1], (8, half))
        values = []
        for child in range(2):

            def rows_of(c, start, index=index, child=child):
                return store[index, child * 2 + c, start : start + 8]

            value = contracted(rows_of, rows, bands[0, child])
            values.append((value, waves.at[member ^ mask, child]))
        held = None
        for block in range(rows // 8):
            totals = turned(values, block)
            if block % 2 == 0:
                held = totals
                continue
            for c in range(2):
                mine[index, c, block * 8 - 8 : block * 8 + 8] = jnp.concatenate(
                    [held[c], totals[c]], axis=0
                ).astype(jnp.bfloat16)
        start = pl.multiple_of((member ^ mask) * rows, rows)
        for c in range(2):
            copy = pltpu.make_async_copy(
                mine.at[index, c], result.at[c, pl.ds(start, rows)], semaphores.at[index, c]
            )
            copy.start()
            copies.append(copy)
    for copy in copies:
        copy.wait()


def send_order(group):
    far, near = list(range(group - 1, group // 2 - 1, -1)), list(range(group // 2 - 1, 0, -1))
    return far[:1] + near[:-1] + far[1:2] + near[-1:] + far[2:]


def on_device(echoes, steering, sub_map, band_offset, interp_weight, range_frac, phase_rate):
    slabs = lax.axis_size("rng")
    subs = lax.axis_size("sub")
    segments, taps = interp_weight.shape[1], interp_weight.shape[3]
    group = 1 << segments
    groups = subs // group
    angles, pulse_count = steering.shape[1], steering.shape[2]
    half = angles // 2
    slab = lax.axis_index("rng")
    range_rows = echoes.shape[2] * subs
    rows = range_rows // group
    early, late = 2 * (segments - 1), 2

    cut = (2,) + echoes.shape[2:]
    tables_in = (band_offset, interp_weight, range_frac, phase_rate)
    *quarters, early_pack, late_pack = pl.pallas_call(
        functools.partial(cut_kernel, slabs, segments, taps, half),
        out_shape=[pltpu.VMEM(cut, jnp.bfloat16)] * slabs
        + [
            pltpu.VMEM((group, pack_rows(early, taps), angles), jnp.bfloat16),
            pltpu.VMEM((pack_rows(late, taps), angles), jnp.bfloat16),
        ],
        in_specs=[FAR] * 5,
        out_specs=[WHOLE] * (slabs + 2),
        scratch_shapes=[pltpu.VMEM(value.shape, value.dtype) for value in tables_in]
        + [pltpu.SemaphoreType.DMA((slabs, 2)), pltpu.SemaphoreType.DMA((4,))],
        compiler_params=params(2),
        cost_estimate=cost(1_000_000_000),
        name="cut",
    )(*[pltpu.with_memory_space_constraint(value, pltpu.HBM) for value in (echoes,) + tables_in])

    received = [quarters[0]] + [None] * (slabs - 1)
    for mask in range(slabs - 1, 0, -1):
        received[mask] = exchanged(quarters[mask], "rng", mask)

    members = None
    if groups > 1:
        members = [[g * group + m for m in range(group)] for g in range(groups)]
    packs = lax.all_to_all(early_pack, "sub", 0, 0, axis_index_groups=members, tiled=True)

    if groups == 1:
        blocks = received
    else:
        ordered = jnp.zeros((slabs,) + received[0].shape, received[0].dtype)
        for mask, block in enumerate(received):
            ordered = lax.dynamic_update_index_in_dim(ordered, block, slab ^ mask, 0)
        every = jnp.moveaxis(ordered, 0, 2).reshape(2, -1, subs, pulse_count)
        every = jnp.take(every, sub_map, axis=2)
        every = lax.ppermute(
            every,
            "sub",
            [(old, (old % groups) * group + old // groups) for old in range(subs)],
        ).reshape(2, -1, groups, group * pulse_count)
        lanes = [[g * group + m for g in range(groups)] for m in range(group)]
        every = lax.all_to_all(every, "sub", 2, 1, axis_index_groups=lanes, tiled=True)
        blocks = [every.reshape(2, rows, group * pulse_count)]

    edge_rows = jnp.stack([block[:, :HALO] for block in blocks])
    route = []
    for number in range(subs):
        for q in range(slabs):
            if number % group > 0:
                route.append((number * slabs + q, (number - 1) * slabs + q))
            elif q > 0:
                route.append((number * slabs + q, (number + group - 1) * slabs + q - 1))
    edge = lax.ppermute(edge_rows, ("sub", "rng"), route)

    def tables(terms, shared, held, lines, pack):
        return pl.pallas_call(
            functools.partial(
                table_kernel,
                group,
                terms,
                shared,
                taps,
                half,
                rows,
                lines,
                range_rows,
                slabs * range_rows,
            ),
            out_shape=(
                jax.ShapeDtypeStruct((held, terms, angles, angles), jnp.bfloat16),
                jax.ShapeDtypeStruct((group, terms, 2, lines, angles), jnp.float32),
            ),
            in_specs=[WHOLE],
            out_specs=(WHOLE, WHOLE),
            scratch_shapes=[
                pltpu.VMEM((group, terms, taps, angles), jnp.float32),
                pltpu.VMEM((group, 3, terms, angles), jnp.float32),
                pltpu.VMEM((15, angles // 128, group * terms, 128), jnp.float32),
            ],
            compiler_params=params(4),
            cost_estimate=cost(2_000_000_000),
        )(pack)

    bands, waves = tables(early, True, group, rows + 8, packs)

    image = pl.pallas_call(
        functools.partial(form_kernel, group, pulse_count, len(blocks), 0, rows),
        out_shape=jax.ShapeDtypeStruct((group, 2, 2, rows, half), jnp.float32),
        in_specs=[SCALARS] + [WHOLE] * (len(blocks) + 1),
        out_specs=WHOLE,
        compiler_params=params(8),
        cost_estimate=cost(1_000_000_000),
        name="form",
    )(sub_map, *blocks, steering)

    sent = pl.pallas_call(
        functools.partial(merge_kernel, group, segments, rows, pulse_count, len(blocks)),
        out_shape=[jax.ShapeDtypeStruct((4 * rows + 8, half), jnp.bfloat16)] * group,
        in_specs=[SCALARS] + [WHOLE] * 5,
        out_specs=[WHOLE] * group,
        scratch_shapes=[pltpu.VMEM((group, 2, 2, 16, half), jnp.float32)]
        + [pltpu.VMEM((group, 2, 2, rows + 16, half), jnp.float32)] * (segments - 1),
        compiler_params=params(12),
        cost_estimate=cost(4_000_000_000),
        name="merge",
    )(sub_map, image, edge, steering, bands, waves)

    order = send_order(group)
    arrived = {0: sent[0]}
    for mask in order:
        arrived[mask] = exchanged(sent[mask], "sub", mask)

    last_bands, last_waves = tables(late, False, 1, rows, late_pack)
    result = None
    turns = [[0] + [mask for mask in order[:-2] if mask != order[3]], [order[3], order[-2]]]
    for chosen in turns + [order[-1:]]:
        count = len(chosen)
        previous = [] if result is None else [result]
        result = pl.pallas_call(
            functools.partial(final_kernel, chosen, group, rows, result is None),
            out_shape=jax.ShapeDtypeStruct((2, range_rows, angles), jnp.bfloat16),
            in_specs=[WHOLE] * (count + 2) + [FAR] * len(previous),
            out_specs=FAR,
            scratch_shapes=[
                pltpu.VMEM((count, 4, rows + 8, half), jnp.float32),
                pltpu.VMEM((count, 2, rows, angles), jnp.bfloat16),
                pltpu.SemaphoreType.DMA((count, 2)),
            ],
            input_output_aliases={count + 2: 0} if previous else {},
            compiler_params=params(6),
            cost_estimate=cost(1_000_000_000),
            name="final",
        )(*[arrived[mask] for mask in chosen], last_bands, last_waves, *previous)
    return result


def solution(mesh):
    in_specs = (
        P(None, None, "sub", "rng"),
        P(),
        P(),
        P("sub", None, None, None),
        P("sub", None, None, None, None),
        P("sub", None, None, None),
        P("sub", None, None, None),
    )
    return jax.shard_map(
        on_device, mesh=mesh, in_specs=in_specs, out_specs=P(None, "rng", "sub"), check_vma=False
    )
```

```python
import functools

import jax
import jax.numpy as jnp
from jax import lax
from jax.experimental import pallas as pl
from jax.experimental.pallas import tpu as pltpu
from jax.sharding import PartitionSpec as P


HALO = 8
KINDS = 6
MIB = 1 << 20
WHOLE = pl.BlockSpec(memory_space=pltpu.VMEM)
SCALARS = pl.BlockSpec(memory_space=pltpu.SMEM)
FAR = pl.BlockSpec(memory_space=pltpu.HBM)


def exchanged(block, axis, mask):
    count = lax.axis_size(axis)
    return lax.ppermute(block, axis, [(source, source ^ mask) for source in range(count)])


def params(mib):
    return pltpu.CompilerParams(vmem_limit_bytes=mib * MIB)


def cost(flops):
    return pl.CostEstimate(flops=flops, bytes_accessed=MIB, transcendentals=0)


def product(left, right):
    return (
        left[0] * right[0] - left[1] * right[1],
        left[0] * right[1] + left[1] * right[0],
    )


def pack_rows(terms, taps):
    return -(-(terms * (taps + KINDS)) // 8) * 8


def cut_kernel(slabs, segments, taps, half, echoes, offset, weight, fraction, rate, *refs):
    slices, packs = refs[:slabs], refs[slabs : slabs + 2]
    held, semaphores, small = refs[slabs + 2 : slabs + 6], refs[slabs + 6], refs[slabs + 7]
    group = 1 << segments
    member = lax.axis_index("sub") & (group - 1)
    slab = lax.axis_index("rng")
    loads = [
        pltpu.make_async_copy(source, target, small.at[index])
        for index, (source, target) in enumerate(zip((offset, weight, fraction, rate), held))
    ]
    copies = []
    for mask in range(slabs - 1, -1, -1):
        for c in range(2):
            copies.append(
                pltpu.make_async_copy(
                    echoes.at[c, slab ^ mask], slices[mask].at[c], semaphores.at[mask, c]
                )
            )
    for copy in loads + copies:
        copy.start()
    for copy in loads:
        copy.wait()
    offset, weight, fraction, rate = held
    angles = weight.shape[-1]
    for pack, chosen in ((packs[0], range(segments - 1)), (packs[1], (segments - 1,))):
        kinds = [[] for _ in range(KINDS)]
        terms = 2 * len(chosen)
        for index, segment in enumerate(chosen):
            base = ((member >> segment) & 1) * half
            kinds[0].append((offset[0, segment] - base).astype(jnp.float32))
            slot = 1
            for source, count in ((fraction, 2), (rate, 3)):
                rest = source[0, segment]
                for _ in range(count):
                    part = rest.astype(jnp.bfloat16).astype(jnp.float32)
                    kinds[slot].append(part)
                    rest = rest - part
                    slot += 1
            for child in range(2):
                term = index * 2 + child
                pack[term * taps : (term + 1) * taps, :] = weight[0, segment, child]
        rows = [piece for kind in kinds for piece in kind]
        padding = pack_rows(terms, taps) - terms * (taps + KINDS)
        if padding:
            rows.append(jnp.zeros((padding, angles), jnp.float32))
        pack[terms * taps :, :] = jnp.concatenate(rows, axis=0).astype(jnp.bfloat16)
    for copy in copies:
        copy.wait()


def table_kernel(members, terms, masks, taps, half, rows, lines, range_rows, total_range, *refs):
    steps = len(masks[0]) if masks else 0
    swapped = steps - 1 if masks else 0
    own, mine, theirs = refs[0], refs[1 : 1 + steps], refs[1 + steps : 1 + steps + swapped]
    bands, waves, weights, raw, dense = refs[1 + steps + swapped :]
    angles = bands.shape[-1]
    member = lax.axis_index("sub") & (members - 1)
    slab = lax.axis_index("rng")

    def fill(piece, section):
        values = piece[...].astype(jnp.float32)
        for term in range(terms):
            weights[section, term] = values[term * taps : (term + 1) * taps]
        start = terms * taps
        kind = [values[start + k * terms : start + (k + 1) * terms] for k in range(KINDS)]
        raw[section, 0] = kind[0]
        raw[section, 1] = kind[1] + kind[2]
        raw[section, 2] = kind[3] + kind[4] + kind[5]

    if masks:
        core = slab & 1
        fill(own, member)
        for received, holder in ((mine, core), (theirs, 1 - core)):
            for step, piece in enumerate(received):
                fill(piece, member ^ jnp.where(holder == 0, masks[0][step], masks[1][step]))
        first_row, row_step = slab * range_rows + member * rows, 0
    else:
        for section in range(members):
            fill(own, section)
        first_row, row_step = slab * range_rows, rows

    for start in range(0, members * terms, 8):
        place = slice(start, start + 8)
        sections = range(start // terms, (start + 8) // terms)

        def keep(kind, value):
            for part in range(angles // 128):
                dense[kind, part, place] = value[:, part * 128 : (part + 1) * 128]

        given = [
            jnp.concatenate([raw[section, kind] for section in sections], axis=0)
            for kind in range(3)
        ]
        keep(0, given[0])
        keep(1, given[1])
        rate = given[2]
        number = start + lax.broadcasted_iota(jnp.int32, (8, angles), 0)
        first = first_row + (number // terms) * row_step
        angle = first.astype(jnp.float32) / float(total_range) * rate
        keep(3, jnp.cos(angle))
        keep(4, jnp.sin(angle))
        angle = rate / float(total_range)
        turn = jnp.cos(angle), jnp.sin(angle)
        for power in range(5):
            keep(5 + 2 * power, turn[0])
            keep(6 + 2 * power, turn[1])
            turn = product(turn, turn)

    sub_rows = lax.broadcasted_iota(jnp.int32, (8, 128), 0)

    def entry(index, carry):
        section, term = index // terms, index % terms
        for part in range(angles // 128):
            lanes = pl.ds(part * 128, 128)

            def row(kind):
                return dense[kind, part, pl.ds(index, 1), :]

            def bands_of():
                weight = weights[section, term, :, lanes]
                offset = row(0).astype(jnp.int32)
                fraction = row(1)
                tap = sub_rows - offset
                block_of = -(tap >> 3)
                picked = jnp.take_along_axis(weight, tap & 7, axis=0)
                near, far = picked * (1.0 - fraction), picked * fraction
                for block in range(half // 16):
                    hits = [block_of == 2 * block + step for step in range(2)]
                    for source, base in ((near, 0), (far, half)):
                        pair = [jnp.where(hit, source, 0.0) for hit in hits]
                        place = slice(base + block * 16, base + (block + 1) * 16)
                        bands[section, term, place, lanes] = jnp.concatenate(pair, axis=0).astype(
                            jnp.bfloat16
                        )

            if masks:
                bands_of()
            else:
                pl.when(section == 0)(bands_of)
            wave = tuple(jnp.broadcast_to(row(3 + c), (8, 128)) for c in range(2))
            for power in range(3):
                chosen = (sub_rows >> power) & 1 == 1
                wave = product(
                    wave,
                    (
                        jnp.where(chosen, row(5 + 2 * power), 1.0),
                        jnp.where(chosen, row(6 + 2 * power), 0.0),
                    ),
                )
            eight, sixteen = (row(11), row(12)), (row(13), row(14))
            chain = [wave, product(wave, eight)]
            for block in range(lines // 8):
                wave = chain[block % 2]
                for c in range(2):
                    waves[section, term, c, block * 8 : (block + 1) * 8, lanes] = wave[c]
                chain[block % 2] = product(wave, sixteen)
        return carry

    lax.fori_loop(0, members * terms, entry, 0)


def formed(steering, re_parts, im_parts):
    rows = jnp.concatenate(re_parts + im_parts, axis=0)
    count = rows.shape[0] // 2
    by_real, by_imag = [
        lax.dot_general(
            rows, steering[c], (((1,), (1,)), ((), ())), preferred_element_type=jnp.float32
        )
        for c in range(2)
    ]
    return by_real[:count] - by_imag[count:], by_imag[:count] + by_real[count:]


def place_of(sub_map, group, slabs, slab, index):
    if slabs == 1:
        return index
    per_slab = group // slabs
    block = (slab ^ (index // per_slab)) * per_slab + index % per_slab
    place = 0
    for section in range(group):
        place = jnp.where(sub_map[section] == block, section, place)
    return place


def form_kernel(group, pulse_count, sources, first, count, sub_map, *refs):
    blocks, steering, image = refs[:sources], refs[sources], refs[sources + 1]
    half = image.shape[-1]
    per_source = group // sources
    slab = lax.axis_index("rng")
    for source in range(sources):
        for start in range(0, per_source, 2):
            pieces = range(start, min(start + 2, per_source))
            parts = [
                [
                    blocks[source][
                        c, first : first + count, piece * pulse_count : (piece + 1) * pulse_count
                    ]
                    for piece in pieces
                ]
                for c in range(2)
            ]
            values = formed(steering, *parts)
            for index, piece in enumerate(pieces):
                target = place_of(sub_map, group, sources, slab, source * per_source + piece)
                for c in range(2):
                    value = values[c][index * count : (index + 1) * count]
                    for window in range(2):
                        image[target, c, window] = value[:, window * half : (window + 1) * half]


def turned(values, block, first):
    total = None
    for value, wave in values:
        part = value[block * 16 : block * 16 + 8], value[block * 16 + 8 : block * 16 + 16]
        start = first + block * 8
        turn = tuple(wave[c, start : start + 8] for c in range(2))
        term = product(turn, part)
        total = term if total is None else (total[0] + term[0], total[1] + term[1])
    return total


def contracted(rows_of, lines, matrix):
    pieces = []
    for block in range(lines // 8):
        sides = []
        for start in (block * 8, block * 8 + 1):
            both = [rows_of(c, start) for c in range(2)]
            sides.append(jnp.concatenate(both, axis=0).astype(jnp.bfloat16))
        pieces.append(jnp.concatenate(sides, axis=1))
    return jnp.dot(jnp.concatenate(pieces, axis=0), matrix, preferred_element_type=jnp.float32)


def merge_kernel(group, segments, chunk, first, rows, whole, pulse_count, sources, *refs):
    if chunk == 0:
        image, bands, waves = refs[:3]
        refs = refs[3:]
    else:
        sub_map, image, edge, steering, bands, waves = refs[:6]
        kept, refs = dict(zip(whole, refs[6:])), refs[6 + len(whole) :]
        edges, refs = refs[group], refs[:group] + refs[group + 1 :]
    outs, stores = refs[:group], refs[group:]
    half = image.shape[-1]
    member = lax.axis_index("sub") & (group - 1)
    per_source = group // sources

    if chunk == 1:
        below = lax.axis_index("rng")
        if sources > 1:
            below = jnp.minimum(below + jnp.where(member == group - 1, 1, 0), sources - 1)
        parts = [[], []]
        for source in range(sources):
            for piece in range(per_source):
                columns = slice(piece * pulse_count, (piece + 1) * pulse_count)
                for c in range(2):
                    parts[c].append(edge[source, c, :, columns])
        values = formed(steering, *parts)
        for index in range(group):
            target = place_of(sub_map, group, sources, below, index)
            for c in range(2):
                value = values[c][index * HALO : (index + 1) * HALO]
                for window in range(2):
                    edges[target, c, window, 0:HALO] = value[:, window * half : (window + 1) * half]
                    edges[target, c, window, HALO:] = jnp.zeros((8, half), jnp.float32)

    def rows_of(segment, section, window, c, start):
        if segment > 0:
            return stores[segment - 1][section, c, window, start : start + 8]
        if chunk == 0 or start + 8 <= rows:
            return image[section, c, window, start : start + 8]
        if start >= rows:
            return edges[section, c, window, start - rows : start - rows + 8]
        return jnp.concatenate(
            [
                image[section, c, window, start:rows],
                edges[section, c, window, 0 : start + 8 - rows],
            ],
            axis=0,
        )

    for segment in range(segments - 1):

        def step(section, carry, segment=segment):
            low = section & ~(1 << segment)
            window = (section >> segment) & 1
            values = []
            for child in range(2):
                source, term = low | (child << segment), segment * 2 + child
                reader = functools.partial(rows_of, segment, source, window)
                value = contracted(reader, rows + 8, bands[section, term])
                values.append((value, waves.at[section, term]))
            for block in range(rows // 8 + 1):
                for c, total in enumerate(turned(values, block, first)):
                    for side in range(2):
                        stores[segment][section, c, side, block * 8 : block * 8 + 8] = total[
                            :, side * half : (side + 1) * half
                        ]
            for c in range(2):
                for side in range(2):
                    stores[segment][section, c, side, rows + 8 :] = jnp.zeros(
                        (8, half), jnp.float32
                    )
            return carry

        lax.fori_loop(0, group, step, 0, unroll=4)

    last = stores[segments - 2]
    size = 4 * rows + 8
    for mask in range(group):
        section = member ^ mask
        low = section & ~(1 << (segments - 1))
        window = (section >> (segments - 1)) & 1
        base = 0
        if chunk == 1 and mask in whole:
            base = kept[mask].shape[0]
            outs[mask][0:base] = kept[mask][...]
        extra = []
        for child in range(2):
            for c in range(2):
                start = base + (child * 2 + c) * rows
                source = last.at[low | (child << (segments - 1)), c, window]
                outs[mask][start : start + rows] = source[0:rows].astype(jnp.bfloat16)
                extra.append(source[rows : rows + 1])
        extra.append(jnp.zeros((4, half), jnp.float32))
        outs[mask][base + 4 * rows : base + size] = jnp.concatenate(extra, axis=0).astype(
            jnp.bfloat16
        )


def final_kernel(jobs, count, group, block_rows, fresh, *refs):
    parts, (bands, waves) = refs[:count], refs[count : count + 2]
    result, store, mine, semaphores = refs[count + (2 if fresh else 3) :]
    half = store.shape[-1]
    member = lax.axis_index("sub") & (group - 1)
    copies = []
    for index, (source, base, mask, first, rows) in enumerate(jobs):
        part = parts[source]
        extra = part[base + 4 * rows : base + 4 * rows + 8].astype(jnp.float32)
        for side in range(4):
            start = base + side * rows
            store[index, side, 0:rows] = part[start : start + rows].astype(jnp.float32)
            store[index, side, rows : rows + 8] = jnp.broadcast_to(extra[side : side + 1], (8, half))
        values = []
        for child in range(2):

            def rows_of(c, start, index=index, child=child):
                return store[index, child * 2 + c, start : start + 8]

            value = contracted(rows_of, rows, bands[0, child])
            values.append((value, waves.at[member ^ mask, child]))
        held = None
        for block in range(rows // 8):
            totals = turned(values, block, first)
            if block % 2 == 0:
                held = totals
                continue
            for c in range(2):
                mine[index, c, block * 8 - 8 : block * 8 + 8] = jnp.concatenate(
                    [held[c], totals[c]], axis=0
                ).astype(jnp.bfloat16)
        start = pl.multiple_of((member ^ mask) * block_rows + first, 16)
        for c in range(2):
            copy = pltpu.make_async_copy(
                mine.at[index, c, 0:rows], result.at[c, pl.ds(start, rows)], semaphores.at[index, c]
            )
            copy.start()
            copies.append(copy)
    for copy in copies:
        copy.wait()


def send_order(group):
    far, near = list(range(group - 1, group // 2 - 1, -1)), list(range(group // 2 - 1, 0, -1))
    upper = [(mask, 0) for mask in far[:2]]
    rest = [(mask, None) for mask in far[2:3] + near + far[3:]]
    return upper, rest + [(mask, 1) for mask in far[:2]]


def on_device(echoes, steering, sub_map, band_offset, interp_weight, range_frac, phase_rate):
    slabs = lax.axis_size("rng")
    subs = lax.axis_size("sub")
    segments, taps = interp_weight.shape[1], interp_weight.shape[3]
    group = 1 << segments
    groups = subs // group
    angles, pulse_count = steering.shape[1], steering.shape[2]
    half = angles // 2
    slab = lax.axis_index("rng")
    range_rows = echoes.shape[2] * subs
    rows = range_rows // group
    early, late = 2 * (segments - 1), 2

    cut = (2,) + echoes.shape[2:]
    tables_in = (band_offset, interp_weight, range_frac, phase_rate)
    *quarters, early_pack, late_pack = pl.pallas_call(
        functools.partial(cut_kernel, slabs, segments, taps, half),
        out_shape=[pltpu.VMEM(cut, jnp.bfloat16)] * slabs
        + [pltpu.VMEM((pack_rows(terms, taps), angles), jnp.bfloat16) for terms in (early, late)],
        in_specs=[FAR] * 5,
        out_specs=[WHOLE] * (slabs + 2),
        scratch_shapes=[pltpu.VMEM(value.shape, value.dtype) for value in tables_in]
        + [pltpu.SemaphoreType.DMA((slabs, 2)), pltpu.SemaphoreType.DMA((4,))],
        compiler_params=params(2),
        cost_estimate=cost(1_000_000_000),
        name="cut",
    )(*[pltpu.with_memory_space_constraint(value, pltpu.HBM) for value in (echoes,) + tables_in])

    received = [quarters[0]] + [None] * (slabs - 1)
    for mask in range(slabs - 1, 0, -1):
        received[mask] = exchanged(quarters[mask], "rng", mask)

    masks = list(range(group - 1, 1, -1))
    masks = (masks[0::2] + [1], masks[1::2] + [1])
    mine, theirs = [], []
    for step in range(len(masks[0])):
        route = []
        for s in range(subs):
            for q in range(slabs):
                route.append((s * slabs + q, (s ^ masks[q & 1][step]) * slabs + q))
        mine.append(lax.ppermute(early_pack, ("sub", "rng"), route))
    for piece in mine[:-1]:
        theirs.append(exchanged(piece, "rng", 1))

    if groups == 1:
        blocks = received
    else:
        ordered = jnp.zeros((slabs,) + received[0].shape, received[0].dtype)
        for mask, block in enumerate(received):
            ordered = lax.dynamic_update_index_in_dim(ordered, block, slab ^ mask, 0)
        every = jnp.moveaxis(ordered, 0, 2).reshape(2, -1, subs, pulse_count)
        every = jnp.take(every, sub_map, axis=2)
        every = lax.ppermute(
            every,
            "sub",
            [(old, (old % groups) * group + old // groups) for old in range(subs)],
        ).reshape(2, -1, groups, group * pulse_count)
        lanes = [[g * group + m for g in range(groups)] for m in range(group)]
        every = lax.all_to_all(every, "sub", 2, 1, axis_index_groups=lanes, tiled=True)
        blocks = [every.reshape(2, rows, group * pulse_count)]

    edge_rows = jnp.stack([block[:, :HALO] for block in blocks])
    route = []
    for number in range(subs):
        for q in range(slabs):
            if number % group > 0:
                route.append((number * slabs + q, (number - 1) * slabs + q))
            elif q > 0:
                route.append((number * slabs + q, (number + group - 1) * slabs + q - 1))
    edge = lax.ppermute(edge_rows, ("sub", "rng"), route)

    def tables(terms, sources, held, lines, arrays):
        return pl.pallas_call(
            functools.partial(
                table_kernel,
                group,
                terms,
                sources,
                taps,
                half,
                rows,
                lines,
                range_rows,
                slabs * range_rows,
            ),
            out_shape=(
                jax.ShapeDtypeStruct((held, terms, angles, angles), jnp.bfloat16),
                jax.ShapeDtypeStruct((group, terms, 2, lines, angles), jnp.float32),
            ),
            in_specs=[WHOLE] * len(arrays),
            out_specs=(WHOLE, WHOLE),
            scratch_shapes=[
                pltpu.VMEM((group, terms, taps, angles), jnp.float32),
                pltpu.VMEM((group, 3, terms, angles), jnp.float32),
                pltpu.VMEM((15, angles // 128, group * terms, 128), jnp.float32),
            ],
            compiler_params=params(4),
            cost_estimate=cost(2_000_000_000),
        )(*arrays)

    bands, waves = tables(early, masks, group, rows + 8, [early_pack, *mine, *theirs])

    cut_row = -(-rows * 5 // 8 // 16) * 16
    bounds = ((0, cut_row), (cut_row, rows - cut_row))
    pieces = [4 * count + 8 for _, count in bounds]
    upper_order, lower_order = send_order(group)
    split = [mask for mask, _ in upper_order]
    whole_masks = [mask for mask in range(group) if mask not in split]

    def form(first, count):
        return pl.pallas_call(
            functools.partial(form_kernel, group, pulse_count, len(blocks), first, count),
            out_shape=jax.ShapeDtypeStruct((group, 2, 2, count, half), jnp.float32),
            in_specs=[SCALARS] + [WHOLE] * (len(blocks) + 1),
            out_specs=WHOLE,
            compiler_params=params(6),
            cost_estimate=cost(1_000_000_000),
        )(sub_map, *blocks, steering)

    def merge(chunk, arrays, sizes):
        first, count = bounds[chunk]
        edges = [pltpu.VMEM((group, 2, 2, 16, half), jnp.float32)] if chunk == 1 else []
        return pl.pallas_call(
            functools.partial(
                merge_kernel,
                group,
                segments,
                chunk,
                first,
                count,
                whole_masks,
                pulse_count,
                len(blocks),
            ),
            out_shape=[jax.ShapeDtypeStruct((size, half), jnp.bfloat16) for size in sizes],
            in_specs=([SCALARS] if chunk == 1 else []) + [WHOLE] * (len(arrays) - chunk),
            out_specs=[WHOLE] * group,
            scratch_shapes=edges
            + [pltpu.VMEM((group, 2, 2, count + 16, half), jnp.float32)] * (segments - 1),
            compiler_params=params(8),
            cost_estimate=cost(4_000_000_000),
        )(*arrays)

    arrived = {}

    def send(mask, chunk, value):
        arrived[mask, chunk] = exchanged(value, "sub", mask)

    upper = merge(0, [form(0, cut_row + 16), bands, waves], pieces[:1] * group)
    for mask, chunk in upper_order:
        send(mask, chunk, upper[mask])
    lower = merge(
        1,
        [sub_map, form(*bounds[1]), edge, steering, bands, waves]
        + [upper[mask] for mask in whole_masks],
        [sum(pieces) if mask in whole_masks else pieces[1] for mask in range(group)],
    )
    for mask, chunk in lower_order:
        send(mask, chunk, lower[mask])
    arrived[0, None] = lower[0]

    last_bands, last_waves = tables(late, None, 1, rows, [late_pack])
    result = None
    middle, slow = lower_order[:1], lower_order[-3:]
    for key in lower_order[1:-3]:
        (slow if key[0] == 2 else middle).append(key)
    turns = [[(0, None)] + upper_order, middle, slow]
    for chosen in turns:
        count = len(chosen)
        jobs = []
        for source, (mask, chunk) in enumerate(chosen):
            for part in (0, 1) if chunk is None else (chunk,):
                base = pieces[0] if chunk is None and part == 1 else 0
                jobs.append((source, base, mask) + bounds[part])
        previous = [] if result is None else [result]
        result = pl.pallas_call(
            functools.partial(final_kernel, jobs, count, group, rows, result is None),
            out_shape=jax.ShapeDtypeStruct((2, range_rows, angles), jnp.bfloat16),
            in_specs=[WHOLE] * (count + 2) + [FAR] * len(previous),
            out_specs=FAR,
            scratch_shapes=[
                pltpu.VMEM((len(jobs), 4, cut_row + 8, half), jnp.float32),
                pltpu.VMEM((len(jobs), 2, cut_row, angles), jnp.bfloat16),
                pltpu.SemaphoreType.DMA((len(jobs), 2)),
            ],
            input_output_aliases={count + 2: 0} if previous else {},
            compiler_params=params(6),
            cost_estimate=cost(1_000_000_000),
            name="final",
        )(*[arrived[key] for key in chosen], last_bands, last_waves, *previous)
    return result


def solution(mesh):
    in_specs = (
        P(None, None, "sub", "rng"),
        P(),
        P(),
        P("sub", None, None, None),
        P("sub", None, None, None, None),
        P("sub", None, None, None),
        P("sub", None, None, None),
    )
    return jax.shard_map(
        on_device, mesh=mesh, in_specs=in_specs, out_specs=P(None, "rng", "sub"), check_vma=False
    )
```

```python
import functools

import jax
import jax.numpy as jnp
from jax import lax
from jax.experimental import pallas as pl
from jax.experimental.pallas import tpu as pltpu
from jax.sharding import PartitionSpec as P


HALO = 8
KINDS = 6
MIB = 1 << 20
WHOLE = pl.BlockSpec(memory_space=pltpu.VMEM)
SCALARS = pl.BlockSpec(memory_space=pltpu.SMEM)
FAR = pl.BlockSpec(memory_space=pltpu.HBM)


def exchanged(block, axis, mask):
    count = lax.axis_size(axis)
    return lax.ppermute(block, axis, [(source, source ^ mask) for source in range(count)])


def params(mib):
    return pltpu.CompilerParams(vmem_limit_bytes=mib * MIB)


def cost(flops):
    return pl.CostEstimate(flops=flops, bytes_accessed=MIB, transcendentals=0)


def product(left, right):
    return (
        left[0] * right[0] - left[1] * right[1],
        left[0] * right[1] + left[1] * right[0],
    )


def pack_rows(terms, taps):
    return -(-(terms * (taps + KINDS)) // 8) * 8


def cut_kernel(slabs, segments, taps, half, echoes, offset, weight, fraction, rate, *refs):
    slices, packs = refs[:slabs], refs[slabs : slabs + 2]
    held, semaphores, small = refs[slabs + 2 : slabs + 6], refs[slabs + 6], refs[slabs + 7]
    group = 1 << segments
    member = lax.axis_index("sub") & (group - 1)
    slab = lax.axis_index("rng")
    loads = [
        pltpu.make_async_copy(source, target, small.at[index])
        for index, (source, target) in enumerate(zip((offset, weight, fraction, rate), held))
    ]
    copies = []
    for mask in range(slabs - 1, -1, -1):
        for c in range(2):
            copies.append(
                pltpu.make_async_copy(
                    echoes.at[c, slab ^ mask], slices[mask].at[c], semaphores.at[mask, c]
                )
            )
    for copy in loads + copies:
        copy.start()
    for copy in loads:
        copy.wait()
    offset, weight, fraction, rate = held
    angles = weight.shape[-1]
    for pack, chosen in ((packs[0], range(segments - 1)), (packs[1], (segments - 1,))):
        kinds = [[] for _ in range(KINDS)]
        terms = 2 * len(chosen)
        for index, segment in enumerate(chosen):
            base = ((member >> segment) & 1) * half
            kinds[0].append((offset[0, segment] - base).astype(jnp.float32))
            slot = 1
            for source, count in ((fraction, 2), (rate, 3)):
                rest = source[0, segment]
                for _ in range(count):
                    part = rest.astype(jnp.bfloat16).astype(jnp.float32)
                    kinds[slot].append(part)
                    rest = rest - part
                    slot += 1
            for child in range(2):
                term = index * 2 + child
                pack[term * taps : (term + 1) * taps, :] = weight[0, segment, child]
        rows = [piece for kind in kinds for piece in kind]
        padding = pack_rows(terms, taps) - terms * (taps + KINDS)
        if padding:
            rows.append(jnp.zeros((padding, angles), jnp.float32))
        pack[terms * taps :, :] = jnp.concatenate(rows, axis=0).astype(jnp.bfloat16)
    for copy in copies:
        copy.wait()


def table_kernel(members, terms, masks, taps, half, rows, lines, range_rows, total_range, *refs):
    steps = len(masks[0]) if masks else 0
    swapped = steps - 1 if masks else 0
    own, mine, theirs = refs[0], refs[1 : 1 + steps], refs[1 + steps : 1 + steps + swapped]
    bands, waves, weights, raw, dense = refs[1 + steps + swapped :]
    angles = bands.shape[-1]
    member = lax.axis_index("sub") & (members - 1)
    slab = lax.axis_index("rng")

    def fill(piece, section):
        values = piece[...].astype(jnp.float32)
        for term in range(terms):
            weights[section, term] = values[term * taps : (term + 1) * taps]
        start = terms * taps
        kind = [values[start + k * terms : start + (k + 1) * terms] for k in range(KINDS)]
        raw[section, 0] = kind[0]
        raw[section, 1] = kind[1] + kind[2]
        raw[section, 2] = kind[3] + kind[4] + kind[5]

    if masks:
        core = slab & 1
        fill(own, member)
        for received, holder in ((mine, core), (theirs, 1 - core)):
            for step, piece in enumerate(received):
                fill(piece, member ^ jnp.where(holder == 0, masks[0][step], masks[1][step]))
        first_row, row_step = slab * range_rows + member * rows, 0
    else:
        for section in range(members):
            fill(own, section)
        first_row, row_step = slab * range_rows, rows

    for start in range(0, members * terms, 8):
        place = slice(start, start + 8)
        sections = range(start // terms, (start + 8) // terms)

        def keep(kind, value):
            for part in range(angles // 128):
                dense[kind, part, place] = value[:, part * 128 : (part + 1) * 128]

        given = [
            jnp.concatenate([raw[section, kind] for section in sections], axis=0)
            for kind in range(3)
        ]
        keep(0, given[0])
        keep(1, given[1])
        rate = given[2]
        number = start + lax.broadcasted_iota(jnp.int32, (8, angles), 0)
        first = first_row + (number // terms) * row_step
        angle = first.astype(jnp.float32) / float(total_range) * rate
        keep(3, jnp.cos(angle))
        keep(4, jnp.sin(angle))
        angle = rate / float(total_range)
        turn = jnp.cos(angle), jnp.sin(angle)
        for power in range(5):
            keep(5 + 2 * power, turn[0])
            keep(6 + 2 * power, turn[1])
            turn = product(turn, turn)

    sub_rows = lax.broadcasted_iota(jnp.int32, (8, 128), 0)

    def entry(index, carry):
        section, term = index // terms, index % terms
        for part in range(angles // 128):
            lanes = pl.ds(part * 128, 128)

            def row(kind):
                return dense[kind, part, pl.ds(index, 1), :]

            def bands_of():
                weight = weights[section, term, :, lanes]
                offset = row(0).astype(jnp.int32)
                fraction = row(1)
                tap = sub_rows - offset
                block_of = -(tap >> 3)
                picked = jnp.take_along_axis(weight, tap & 7, axis=0)
                near, far = picked * (1.0 - fraction), picked * fraction
                for block in range(half // 16):
                    hits = [block_of == 2 * block + step for step in range(2)]
                    for source, base in ((near, 0), (far, half)):
                        pair = [jnp.where(hit, source, 0.0) for hit in hits]
                        place = slice(base + block * 16, base + (block + 1) * 16)
                        bands[section, term, place, lanes] = jnp.concatenate(pair, axis=0).astype(
                            jnp.bfloat16
                        )

            if masks:
                bands_of()
            else:
                pl.when(section == 0)(bands_of)
            wave = tuple(jnp.broadcast_to(row(3 + c), (8, 128)) for c in range(2))
            for power in range(3):
                chosen = (sub_rows >> power) & 1 == 1
                wave = product(
                    wave,
                    (
                        jnp.where(chosen, row(5 + 2 * power), 1.0),
                        jnp.where(chosen, row(6 + 2 * power), 0.0),
                    ),
                )
            eight, sixteen = (row(11), row(12)), (row(13), row(14))
            chain = [wave, product(wave, eight)]
            for block in range(lines // 8):
                wave = chain[block % 2]
                for c in range(2):
                    waves[section, term, c, block * 8 : (block + 1) * 8, lanes] = wave[c]
                chain[block % 2] = product(wave, sixteen)
        return carry

    lax.fori_loop(0, members * terms, entry, 0)


def formed(steering, re_parts, im_parts):
    rows = jnp.concatenate(re_parts + im_parts, axis=0)
    count = rows.shape[0] // 2
    by_real, by_imag = [
        lax.dot_general(
            rows, steering[c], (((1,), (1,)), ((), ())), preferred_element_type=jnp.float32
        )
        for c in range(2)
    ]
    return by_real[:count] - by_imag[count:], by_imag[:count] + by_real[count:]


def place_of(sub_map, group, slabs, slab, index):
    if slabs == 1:
        return index
    per_slab = group // slabs
    block = (slab ^ (index // per_slab)) * per_slab + index % per_slab
    place = 0
    for section in range(group):
        place = jnp.where(sub_map[section] == block, section, place)
    return place


def form_rows(group, pulse_count, sources, first, sub_map, blocks, steering, image):
    half, count = image.shape[-1], image.shape[-2]
    per_source = group // sources
    slab = lax.axis_index("rng")
    for source in range(sources):
        for start in range(0, per_source, 2):
            pieces = range(start, min(start + 2, per_source))
            parts = [
                [
                    blocks[source][
                        c, first : first + count, piece * pulse_count : (piece + 1) * pulse_count
                    ]
                    for piece in pieces
                ]
                for c in range(2)
            ]
            values = formed(steering, *parts)
            for index, piece in enumerate(pieces):
                target = place_of(sub_map, group, sources, slab, source * per_source + piece)
                for c in range(2):
                    value = values[c][index * count : (index + 1) * count]
                    for window in range(2):
                        image[target, c, window] = value[:, window * half : (window + 1) * half]


def turned(values, block, first):
    total = None
    for value, wave in values:
        part = value[block * 16 : block * 16 + 8], value[block * 16 + 8 : block * 16 + 16]
        start = first + block * 8
        turn = tuple(wave[c, start : start + 8] for c in range(2))
        term = product(turn, part)
        total = term if total is None else (total[0] + term[0], total[1] + term[1])
    return total


def contracted(rows_of, lines, matrix):
    pieces = []
    for block in range(lines // 8):
        sides = []
        for start in (block * 8, block * 8 + 1):
            both = [rows_of(c, start) for c in range(2)]
            sides.append(jnp.concatenate(both, axis=0).astype(jnp.bfloat16))
        pieces.append(jnp.concatenate(sides, axis=1))
    return jnp.dot(jnp.concatenate(pieces, axis=0), matrix, preferred_element_type=jnp.float32)


def merge_kernel(
    group, segments, chunk, first, rows, whole, pulse_count, sources, sub_map, *refs
):
    blocks, refs = refs[:sources], refs[sources:]
    steering, bands, waves, refs = refs[0], refs[1], refs[2], refs[3:]
    if chunk == 1:
        edge, kept, refs = refs[0], dict(zip(whole, refs[1:])), refs[1 + len(whole) :]
    outs, image, refs = refs[:group], refs[group], refs[group + 1 :]
    if chunk == 1:
        edges, refs = refs[0], refs[1:]
    stores = refs
    form_rows(group, pulse_count, sources, first, sub_map, blocks, steering, image)
    half = image.shape[-1]
    member = lax.axis_index("sub") & (group - 1)
    per_source = group // sources

    if chunk == 1:
        below = lax.axis_index("rng")
        if sources > 1:
            below = jnp.minimum(below + jnp.where(member == group - 1, 1, 0), sources - 1)
        parts = [[], []]
        for source in range(sources):
            for piece in range(per_source):
                columns = slice(piece * pulse_count, (piece + 1) * pulse_count)
                for c in range(2):
                    parts[c].append(edge[source, c, :, columns])
        values = formed(steering, *parts)
        for index in range(group):
            target = place_of(sub_map, group, sources, below, index)
            for c in range(2):
                value = values[c][index * HALO : (index + 1) * HALO]
                for window in range(2):
                    edges[target, c, window, 0:HALO] = value[:, window * half : (window + 1) * half]
                    edges[target, c, window, HALO:] = jnp.zeros((8, half), jnp.float32)

    def rows_of(segment, section, window, c, start):
        if segment > 0:
            return stores[segment - 1][section, c, window, start : start + 8]
        if chunk == 0 or start + 8 <= rows:
            return image[section, c, window, start : start + 8]
        if start >= rows:
            return edges[section, c, window, start - rows : start - rows + 8]
        return jnp.concatenate(
            [
                image[section, c, window, start:rows],
                edges[section, c, window, 0 : start + 8 - rows],
            ],
            axis=0,
        )

    for segment in range(segments - 1):

        def step(section, carry, segment=segment):
            low = section & ~(1 << segment)
            window = (section >> segment) & 1
            values = []
            for child in range(2):
                source, term = low | (child << segment), segment * 2 + child
                reader = functools.partial(rows_of, segment, source, window)
                value = contracted(reader, rows + 8, bands[section, term])
                values.append((value, waves.at[section, term]))
            for block in range(rows // 8 + 1):
                for c, total in enumerate(turned(values, block, first)):
                    for side in range(2):
                        stores[segment][section, c, side, block * 8 : block * 8 + 8] = total[
                            :, side * half : (side + 1) * half
                        ]
            for c in range(2):
                for side in range(2):
                    stores[segment][section, c, side, rows + 8 :] = jnp.zeros(
                        (8, half), jnp.float32
                    )
            return carry

        lax.fori_loop(0, group, step, 0, unroll=4)

    last = stores[segments - 2]
    size = 4 * rows + 8
    for mask in range(group):
        section = member ^ mask
        low = section & ~(1 << (segments - 1))
        window = (section >> (segments - 1)) & 1
        base = 0
        if chunk == 1 and mask in whole:
            base = kept[mask].shape[0]
            outs[mask][0:base] = kept[mask][...]
        extra = []
        for child in range(2):
            for c in range(2):
                start = base + (child * 2 + c) * rows
                source = last.at[low | (child << (segments - 1)), c, window]
                outs[mask][start : start + rows] = source[0:rows].astype(jnp.bfloat16)
                extra.append(source[rows : rows + 1])
        extra.append(jnp.zeros((4, half), jnp.float32))
        outs[mask][base + 4 * rows : base + size] = jnp.concatenate(extra, axis=0).astype(
            jnp.bfloat16
        )


def final_kernel(jobs, count, group, block_rows, fresh, *refs):
    parts, (bands, waves) = refs[:count], refs[count : count + 2]
    result, store, mine, semaphores = refs[count + (2 if fresh else 3) :]
    half = store.shape[-1]
    member = lax.axis_index("sub") & (group - 1)
    copies = []
    for index, (source, base, mask, first, rows) in enumerate(jobs):
        part = parts[source]
        extra = part[base + 4 * rows : base + 4 * rows + 8].astype(jnp.float32)
        for side in range(4):
            start = base + side * rows
            store[index, side, 0:rows] = part[start : start + rows].astype(jnp.float32)
            store[index, side, rows : rows + 8] = jnp.broadcast_to(extra[side : side + 1], (8, half))
        values = []
        for child in range(2):

            def rows_of(c, start, index=index, child=child):
                return store[index, child * 2 + c, start : start + 8]

            value = contracted(rows_of, rows, bands[0, child])
            values.append((value, waves.at[member ^ mask, child]))
        held = None
        for block in range(rows // 8):
            totals = turned(values, block, first)
            if block % 2 == 0:
                held = totals
                continue
            for c in range(2):
                mine[index, c, block * 8 - 8 : block * 8 + 8] = jnp.concatenate(
                    [held[c], totals[c]], axis=0
                ).astype(jnp.bfloat16)
        start = pl.multiple_of((member ^ mask) * block_rows + first, 16)
        for c in range(2):
            copy = pltpu.make_async_copy(
                mine.at[index, c, 0:rows], result.at[c, pl.ds(start, rows)], semaphores.at[index, c]
            )
            copy.start()
            copies.append(copy)
    for copy in copies:
        copy.wait()


def send_order(group):
    far, near = list(range(group - 1, group // 2 - 1, -1)), list(range(group // 2 - 1, 0, -1))
    upper = [(mask, 0) for mask in far[:2]]
    rest = [(mask, None) for mask in far[2:3] + near + far[3:]]
    return upper, rest + [(mask, 1) for mask in far[:2]]


def on_device(echoes, steering, sub_map, band_offset, interp_weight, range_frac, phase_rate):
    slabs = lax.axis_size("rng")
    subs = lax.axis_size("sub")
    segments, taps = interp_weight.shape[1], interp_weight.shape[3]
    group = 1 << segments
    groups = subs // group
    angles, pulse_count = steering.shape[1], steering.shape[2]
    half = angles // 2
    slab = lax.axis_index("rng")
    range_rows = echoes.shape[2] * subs
    rows = range_rows // group
    early, late = 2 * (segments - 1), 2

    cut = (2,) + echoes.shape[2:]
    tables_in = (band_offset, interp_weight, range_frac, phase_rate)
    *quarters, early_pack, late_pack = pl.pallas_call(
        functools.partial(cut_kernel, slabs, segments, taps, half),
        out_shape=[pltpu.VMEM(cut, jnp.bfloat16)] * slabs
        + [pltpu.VMEM((pack_rows(terms, taps), angles), jnp.bfloat16) for terms in (early, late)],
        in_specs=[FAR] * 5,
        out_specs=[WHOLE] * (slabs + 2),
        scratch_shapes=[pltpu.VMEM(value.shape, value.dtype) for value in tables_in]
        + [pltpu.SemaphoreType.DMA((slabs, 2)), pltpu.SemaphoreType.DMA((4,))],
        compiler_params=params(2),
        cost_estimate=cost(1_000_000_000),
        name="cut",
    )(*[pltpu.with_memory_space_constraint(value, pltpu.HBM) for value in (echoes,) + tables_in])

    received = [quarters[0]] + [None] * (slabs - 1)
    for mask in range(slabs - 1, 0, -1):
        received[mask] = exchanged(quarters[mask], "rng", mask)

    masks = list(range(group - 1, 1, -1))
    masks = (masks[0::2] + [1], masks[1::2] + [1])
    mine, theirs = [], []
    for step in range(len(masks[0])):
        route = []
        for s in range(subs):
            for q in range(slabs):
                route.append((s * slabs + q, (s ^ masks[q & 1][step]) * slabs + q))
        mine.append(lax.ppermute(early_pack, ("sub", "rng"), route))
    for piece in mine[:-1]:
        theirs.append(exchanged(piece, "rng", 1))

    if groups == 1:
        blocks = received
    else:
        ordered = jnp.zeros((slabs,) + received[0].shape, received[0].dtype)
        for mask, block in enumerate(received):
            ordered = lax.dynamic_update_index_in_dim(ordered, block, slab ^ mask, 0)
        every = jnp.moveaxis(ordered, 0, 2).reshape(2, -1, subs, pulse_count)
        every = jnp.take(every, sub_map, axis=2)
        every = lax.ppermute(
            every,
            "sub",
            [(old, (old % groups) * group + old // groups) for old in range(subs)],
        ).reshape(2, -1, groups, group * pulse_count)
        lanes = [[g * group + m for g in range(groups)] for m in range(group)]
        every = lax.all_to_all(every, "sub", 2, 1, axis_index_groups=lanes, tiled=True)
        blocks = [every.reshape(2, rows, group * pulse_count)]

    edge_rows = jnp.stack([block[:, :HALO] for block in blocks])
    route = []
    for number in range(subs):
        for q in range(slabs):
            if number % group > 0:
                route.append((number * slabs + q, (number - 1) * slabs + q))
            elif q > 0:
                route.append((number * slabs + q, (number + group - 1) * slabs + q - 1))
    edge = lax.ppermute(edge_rows, ("sub", "rng"), route)

    def tables(terms, sources, held, lines, arrays):
        return pl.pallas_call(
            functools.partial(
                table_kernel,
                group,
                terms,
                sources,
                taps,
                half,
                rows,
                lines,
                range_rows,
                slabs * range_rows,
            ),
            out_shape=(
                jax.ShapeDtypeStruct((held, terms, angles, angles), jnp.bfloat16),
                jax.ShapeDtypeStruct((group, terms, 2, lines, angles), jnp.float32),
            ),
            in_specs=[WHOLE] * len(arrays),
            out_specs=(WHOLE, WHOLE),
            scratch_shapes=[
                pltpu.VMEM((group, terms, taps, angles), jnp.float32),
                pltpu.VMEM((group, 3, terms, angles), jnp.float32),
                pltpu.VMEM((15, angles // 128, group * terms, 128), jnp.float32),
            ],
            compiler_params=params(4),
            cost_estimate=cost(2_000_000_000),
        )(*arrays)

    bands, waves = tables(early, masks, group, rows + 8, [early_pack, *mine, *theirs])

    cut_row = -(-rows * 5 // 8 // 16) * 16
    bounds = ((0, cut_row), (cut_row, rows - cut_row))
    pieces = [4 * count + 8 for _, count in bounds]
    upper_order, lower_order = send_order(group)
    split = [mask for mask, _ in upper_order]
    whole_masks = [mask for mask in range(group) if mask not in split]

    def merge(chunk, arrays, sizes):
        first, count = bounds[chunk]
        held = count if chunk == 1 else count + 16
        scratch = [pltpu.VMEM((group, 2, 2, held, half), jnp.float32)]
        if chunk == 1:
            scratch.append(pltpu.VMEM((group, 2, 2, 16, half), jnp.float32))
        return pl.pallas_call(
            functools.partial(
                merge_kernel,
                group,
                segments,
                chunk,
                first,
                count,
                whole_masks,
                pulse_count,
                len(blocks),
            ),
            out_shape=[jax.ShapeDtypeStruct((size, half), jnp.bfloat16) for size in sizes],
            in_specs=[SCALARS] + [WHOLE] * (len(blocks) + 3 + len(arrays)),
            out_specs=[WHOLE] * group,
            scratch_shapes=scratch
            + [pltpu.VMEM((group, 2, 2, count + 16, half), jnp.float32)] * (segments - 1),
            compiler_params=params(10),
            cost_estimate=cost(4_000_000_000),
        )(sub_map, *blocks, steering, bands, waves, *arrays)

    arrived = {}

    def send(mask, chunk, value):
        arrived[mask, chunk] = exchanged(value, "sub", mask)

    upper = merge(0, [], pieces[:1] * group)
    for mask, chunk in upper_order:
        send(mask, chunk, upper[mask])
    lower = merge(
        1,
        [edge] + [upper[mask] for mask in whole_masks],
        [sum(pieces) if mask in whole_masks else pieces[1] for mask in range(group)],
    )
    for mask, chunk in lower_order:
        send(mask, chunk, lower[mask])
    arrived[0, None] = lower[0]

    last_bands, last_waves = tables(late, None, 1, rows, [late_pack])
    result = None
    middle, slow = lower_order[:1], lower_order[-3:]
    for key in lower_order[1:-3]:
        (slow if key[0] == 2 else middle).append(key)
    turns = [[(0, None)] + upper_order, middle, slow]
    for chosen in turns:
        count = len(chosen)
        jobs = []
        for source, (mask, chunk) in enumerate(chosen):
            for part in (0, 1) if chunk is None else (chunk,):
                base = pieces[0] if chunk is None and part == 1 else 0
                jobs.append((source, base, mask) + bounds[part])
        previous = [] if result is None else [result]
        result = pl.pallas_call(
            functools.partial(final_kernel, jobs, count, group, rows, result is None),
            out_shape=jax.ShapeDtypeStruct((2, range_rows, angles), jnp.bfloat16),
            in_specs=[WHOLE] * (count + 2) + [FAR] * len(previous),
            out_specs=FAR,
            scratch_shapes=[
                pltpu.VMEM((len(jobs), 4, cut_row + 8, half), jnp.float32),
                pltpu.VMEM((len(jobs), 2, cut_row, angles), jnp.bfloat16),
                pltpu.SemaphoreType.DMA((len(jobs), 2)),
            ],
            input_output_aliases={count + 2: 0} if previous else {},
            compiler_params=params(6),
            cost_estimate=cost(1_000_000_000),
            name="final",
        )(*[arrived[key] for key in chosen], last_bands, last_waves, *previous)
    return result


def solution(mesh):
    in_specs = (
        P(None, None, "sub", "rng"),
        P(),
        P(),
        P("sub", None, None, None),
        P("sub", None, None, None, None),
        P("sub", None, None, None),
        P("sub", None, None, None),
    )
    return jax.shard_map(
        on_device, mesh=mesh, in_specs=in_specs, out_specs=P(None, "rng", "sub"), check_vma=False
    )
```

```python
import functools

import jax
import jax.numpy as jnp
from jax import lax
from jax.experimental import pallas as pl
from jax.experimental.pallas import tpu as pltpu
from jax.sharding import PartitionSpec as P


HALO = 8
KINDS = 6
MIB = 1 << 20
WHOLE = pl.BlockSpec(memory_space=pltpu.VMEM)
FAR = pl.BlockSpec(memory_space=pltpu.HBM)


def exchanged(block, axis, mask):
    count = lax.axis_size(axis)
    return lax.ppermute(block, axis, [(source, source ^ mask) for source in range(count)])


def params(mib):
    return pltpu.CompilerParams(vmem_limit_bytes=mib * MIB)


def cost(flops):
    return pl.CostEstimate(flops=flops, bytes_accessed=MIB, transcendentals=0)


def product(left, right):
    return (
        left[0] * right[0] - left[1] * right[1],
        left[0] * right[1] + left[1] * right[0],
    )


def pack_rows(terms, taps):
    return -(-(terms * (taps + KINDS)) // 8) * 8


def cut_kernel(slabs, segments, taps, half, echoes, offset, weight, fraction, rate, *refs):
    slices, packs = refs[:slabs], refs[slabs : slabs + 2]
    held, semaphores, small = refs[slabs + 2 : slabs + 6], refs[slabs + 6], refs[slabs + 7]
    group = 1 << segments
    member = lax.axis_index("sub") & (group - 1)
    slab = lax.axis_index("rng")
    loads = [
        pltpu.make_async_copy(source, target, small.at[index])
        for index, (source, target) in enumerate(zip((offset, weight, fraction, rate), held))
    ]
    copies = []
    for mask in range(slabs - 1, -1, -1):
        for c in range(2):
            copies.append(
                pltpu.make_async_copy(
                    echoes.at[c, slab ^ mask], slices[mask].at[c], semaphores.at[mask, c]
                )
            )
    for copy in loads + copies:
        copy.start()
    for copy in loads:
        copy.wait()
    offset, weight, fraction, rate = held
    angles = weight.shape[-1]
    for pack, chosen in ((packs[0], range(segments - 1)), (packs[1], (segments - 1,))):
        kinds = [[] for _ in range(KINDS)]
        terms = 2 * len(chosen)
        for index, segment in enumerate(chosen):
            base = ((member >> segment) & 1) * half
            kinds[0].append((offset[0, segment] - base).astype(jnp.float32))
            slot = 1
            for source, count in ((fraction, 2), (rate, 3)):
                rest = source[0, segment]
                for _ in range(count):
                    part = rest.astype(jnp.bfloat16).astype(jnp.float32)
                    kinds[slot].append(part)
                    rest = rest - part
                    slot += 1
            for child in range(2):
                term = index * 2 + child
                pack[term * taps : (term + 1) * taps, :] = weight[0, segment, child]
        rows = [piece for kind in kinds for piece in kind]
        padding = pack_rows(terms, taps) - terms * (taps + KINDS)
        if padding:
            rows.append(jnp.zeros((padding, angles), jnp.float32))
        pack[terms * taps :, :] = jnp.concatenate(rows, axis=0).astype(jnp.bfloat16)
    for copy in copies:
        copy.wait()


def table_kernel(members, terms, masks, taps, half, rows, lines, range_rows, total_range, *refs):
    steps = len(masks[0]) if masks else 0
    swapped = steps - 1 if masks else 0
    own, mine, theirs = refs[0], refs[1 : 1 + steps], refs[1 + steps : 1 + steps + swapped]
    bands, waves, weights, raw, dense = refs[1 + steps + swapped :]
    angles = bands.shape[-1]
    member = lax.axis_index("sub") & (members - 1)
    slab = lax.axis_index("rng")

    def fill(piece, section):
        values = piece[...].astype(jnp.float32)
        for term in range(terms):
            weights[section, term] = values[term * taps : (term + 1) * taps]
        start = terms * taps
        kind = [values[start + k * terms : start + (k + 1) * terms] for k in range(KINDS)]
        raw[section, 0] = kind[0]
        raw[section, 1] = kind[1] + kind[2]
        raw[section, 2] = kind[3] + kind[4] + kind[5]

    if masks:
        core = slab & 1
        fill(own, member)
        for received, holder in ((mine, core), (theirs, 1 - core)):
            for step, piece in enumerate(received):
                fill(piece, member ^ jnp.where(holder == 0, masks[0][step], masks[1][step]))
        first_row, row_step = slab * range_rows + member * rows, 0
    else:
        for section in range(members):
            fill(own, section)
        first_row, row_step = slab * range_rows, rows

    for start in range(0, members * terms, 8):
        place = slice(start, start + 8)
        sections = range(start // terms, (start + 8) // terms)

        def keep(kind, value):
            for part in range(angles // 128):
                dense[kind, part, place] = value[:, part * 128 : (part + 1) * 128]

        given = [
            jnp.concatenate([raw[section, kind] for section in sections], axis=0)
            for kind in range(3)
        ]
        keep(0, given[0])
        keep(1, given[1])
        rate = given[2]
        number = start + lax.broadcasted_iota(jnp.int32, (8, angles), 0)
        first = first_row + (number // terms) * row_step
        angle = first.astype(jnp.float32) / float(total_range) * rate
        keep(3, jnp.cos(angle))
        keep(4, jnp.sin(angle))
        angle = rate / float(total_range)
        turn = jnp.cos(angle), jnp.sin(angle)
        for power in range(5):
            keep(5 + 2 * power, turn[0])
            keep(6 + 2 * power, turn[1])
            turn = product(turn, turn)

    sub_rows = lax.broadcasted_iota(jnp.int32, (8, 128), 0)

    def entry(index, carry):
        section, term = index // terms, index % terms
        for part in range(angles // 128):
            lanes = pl.ds(part * 128, 128)

            def row(kind):
                return dense[kind, part, pl.ds(index, 1), :]

            def bands_of():
                weight = weights[section, term, :, lanes]
                offset = row(0).astype(jnp.int32)
                fraction = row(1)
                tap = sub_rows - offset
                block_of = -(tap >> 3)
                picked = jnp.take_along_axis(weight, tap & 7, axis=0)
                near, far = picked * (1.0 - fraction), picked * fraction
                for block in range(half // 16):
                    hits = [block_of == 2 * block + step for step in range(2)]
                    for source, base in ((near, 0), (far, half)):
                        pair = [jnp.where(hit, source, 0.0) for hit in hits]
                        place = slice(base + block * 16, base + (block + 1) * 16)
                        bands[section, term, place, lanes] = jnp.concatenate(pair, axis=0).astype(
                            jnp.bfloat16
                        )

            if masks:
                bands_of()
            else:
                pl.when(section == 0)(bands_of)
            wave = tuple(jnp.broadcast_to(row(3 + c), (8, 128)) for c in range(2))
            for power in range(3):
                chosen = (sub_rows >> power) & 1 == 1
                wave = product(
                    wave,
                    (
                        jnp.where(chosen, row(5 + 2 * power), 1.0),
                        jnp.where(chosen, row(6 + 2 * power), 0.0),
                    ),
                )
            eight, sixteen = (row(11), row(12)), (row(13), row(14))
            chain = [wave, product(wave, eight)]
            for block in range(lines // 8):
                wave = chain[block % 2]
                for c in range(2):
                    waves[section, term, c, block * 8 : (block + 1) * 8, lanes] = wave[c]
                chain[block % 2] = product(wave, sixteen)
        return carry

    lax.fori_loop(0, members * terms, entry, 0)


def formed(steering, re_parts, im_parts):
    rows = jnp.concatenate(re_parts + im_parts, axis=0)
    count = rows.shape[0] // 2
    by_real, by_imag = [
        lax.dot_general(
            rows, steering[c], (((1,), (1,)), ((), ())), preferred_element_type=jnp.float32
        )
        for c in range(2)
    ]
    return by_real[:count] - by_imag[count:], by_imag[:count] + by_real[count:]


def place_of(sub_map, group, slabs, slab, index):
    if slabs == 1:
        return index
    per_slab = group // slabs
    block = (slab ^ (index // per_slab)) * per_slab + index % per_slab
    number = lax.broadcasted_iota(jnp.int32, sub_map.shape, 1).astype(jnp.float32)
    return jnp.sum(jnp.where(sub_map[...] == block, number, 0.0)).astype(jnp.int32)


def form_rows(group, pulse_count, sources, first, sub_map, blocks, steering, image):
    half, count = image.shape[-1], image.shape[-2]
    per_source = group // sources
    slab = lax.axis_index("rng")
    for source in range(sources):
        for start in range(0, per_source, 2):
            pieces = range(start, min(start + 2, per_source))
            parts = [
                [
                    blocks[source][
                        c, first : first + count, piece * pulse_count : (piece + 1) * pulse_count
                    ]
                    for piece in pieces
                ]
                for c in range(2)
            ]
            values = formed(steering, *parts)
            for index, piece in enumerate(pieces):
                target = place_of(sub_map, group, sources, slab, source * per_source + piece)
                for c in range(2):
                    value = values[c][index * count : (index + 1) * count]
                    for window in range(2):
                        image[target, c, window] = value[:, window * half : (window + 1) * half]


def turned(values, block, first):
    total = None
    for value, wave in values:
        part = value[block * 16 : block * 16 + 8], value[block * 16 + 8 : block * 16 + 16]
        start = first + block * 8
        turn = tuple(wave[c, start : start + 8] for c in range(2))
        term = product(turn, part)
        total = term if total is None else (total[0] + term[0], total[1] + term[1])
    return total


def contracted(rows_of, lines, matrix):
    pieces = []
    for block in range(lines // 8):
        sides = []
        for start in (block * 8, block * 8 + 1):
            both = [rows_of(c, start) for c in range(2)]
            sides.append(jnp.concatenate(both, axis=0).astype(jnp.bfloat16))
        pieces.append(jnp.concatenate(sides, axis=1))
    return jnp.dot(jnp.concatenate(pieces, axis=0), matrix, preferred_element_type=jnp.float32)


def merge_kernel(
    group, segments, chunk, first, rows, whole, pulse_count, sources, sub_map, *refs
):
    blocks, refs = refs[:sources], refs[sources:]
    steering, bands, waves, refs = refs[0], refs[1], refs[2], refs[3:]
    if chunk == 1:
        edge, kept, refs = refs[0], dict(zip(whole, refs[1:])), refs[1 + len(whole) :]
    outs, image, refs = refs[:group], refs[group], refs[group + 1 :]
    if chunk == 1:
        edges, refs = refs[0], refs[1:]
    stores = refs
    form_rows(group, pulse_count, sources, first, sub_map, blocks, steering, image)
    half = image.shape[-1]
    member = lax.axis_index("sub") & (group - 1)
    per_source = group // sources

    if chunk == 1:
        below = lax.axis_index("rng")
        if sources > 1:
            below = jnp.minimum(below + jnp.where(member == group - 1, 1, 0), sources - 1)
        parts = [[], []]
        for source in range(sources):
            for piece in range(per_source):
                columns = slice(piece * pulse_count, (piece + 1) * pulse_count)
                for c in range(2):
                    parts[c].append(edge[source, c, :, columns])
        values = formed(steering, *parts)
        for index in range(group):
            target = place_of(sub_map, group, sources, below, index)
            for c in range(2):
                value = values[c][index * HALO : (index + 1) * HALO]
                for window in range(2):
                    edges[target, c, window, 0:HALO] = value[:, window * half : (window + 1) * half]
                    edges[target, c, window, HALO:] = jnp.zeros((8, half), jnp.float32)

    def rows_of(segment, section, window, c, start):
        if segment > 0:
            return stores[segment - 1][section, c, window, start : start + 8]
        if chunk == 0 or start + 8 <= rows:
            return image[section, c, window, start : start + 8]
        if start >= rows:
            return edges[section, c, window, start - rows : start - rows + 8]
        return jnp.concatenate(
            [
                image[section, c, window, start:rows],
                edges[section, c, window, 0 : start + 8 - rows],
            ],
            axis=0,
        )

    for segment in range(segments - 1):

        def step(section, carry, segment=segment):
            low = section & ~(1 << segment)
            window = (section >> segment) & 1
            values = []
            for child in range(2):
                source, term = low | (child << segment), segment * 2 + child
                reader = functools.partial(rows_of, segment, source, window)
                value = contracted(reader, rows + 8, bands[section, term])
                values.append((value, waves.at[section, term]))
            for block in range(rows // 8 + 1):
                for c, total in enumerate(turned(values, block, first)):
                    for side in range(2):
                        stores[segment][section, c, side, block * 8 : block * 8 + 8] = total[
                            :, side * half : (side + 1) * half
                        ]
            for c in range(2):
                for side in range(2):
                    stores[segment][section, c, side, rows + 8 :] = jnp.zeros(
                        (8, half), jnp.float32
                    )
            return carry

        lax.fori_loop(0, group, step, 0, unroll=4)

    last = stores[segments - 2]
    size = 4 * rows + 8
    for mask in range(group):
        section = member ^ mask
        low = section & ~(1 << (segments - 1))
        window = (section >> (segments - 1)) & 1
        base = 0
        if chunk == 1 and mask in whole:
            base = kept[mask].shape[0]
            outs[mask][0:base] = kept[mask][...]
        extra = []
        for child in range(2):
            for c in range(2):
                start = base + (child * 2 + c) * rows
                source = last.at[low | (child << (segments - 1)), c, window]
                outs[mask][start : start + rows] = source[0:rows].astype(jnp.bfloat16)
                extra.append(source[rows : rows + 1])
        extra.append(jnp.zeros((4, half), jnp.float32))
        outs[mask][base + 4 * rows : base + size] = jnp.concatenate(extra, axis=0).astype(
            jnp.bfloat16
        )


def final_kernel(jobs, count, group, block_rows, fresh, *refs):
    parts, (bands, waves) = refs[:count], refs[count : count + 2]
    result, store, mine, semaphores = refs[count + (2 if fresh else 3) :]
    half = store.shape[-1]
    member = lax.axis_index("sub") & (group - 1)
    copies = []
    for index, (source, base, mask, first, rows) in enumerate(jobs):
        part = parts[source]
        extra = part[base + 4 * rows : base + 4 * rows + 8].astype(jnp.float32)
        for side in range(4):
            start = base + side * rows
            store[index, side, 0:rows] = part[start : start + rows].astype(jnp.float32)
            store[index, side, rows : rows + 8] = jnp.broadcast_to(extra[side : side + 1], (8, half))
        values = []
        for child in range(2):

            def rows_of(c, start, index=index, child=child):
                return store[index, child * 2 + c, start : start + 8]

            value = contracted(rows_of, rows, bands[0, child])
            values.append((value, waves.at[member ^ mask, child]))
        held = None
        for block in range(rows // 8):
            totals = turned(values, block, first)
            if block % 2 == 0:
                held = totals
                continue
            for c in range(2):
                mine[index, c, block * 8 - 8 : block * 8 + 8] = jnp.concatenate(
                    [held[c], totals[c]], axis=0
                ).astype(jnp.bfloat16)
        start = pl.multiple_of((member ^ mask) * block_rows + first, 16)
        for c in range(2):
            copy = pltpu.make_async_copy(
                mine.at[index, c, 0:rows], result.at[c, pl.ds(start, rows)], semaphores.at[index, c]
            )
            copy.start()
            copies.append(copy)
    for copy in copies:
        copy.wait()


def send_order(group):
    far, near = list(range(group - 1, group // 2 - 1, -1)), list(range(group // 2 - 1, 0, -1))
    upper = [(mask, 0) for mask in far[:2]]
    rest = [(mask, None) for mask in far[2:3] + near + far[3:]]
    return upper, rest + [(mask, 1) for mask in far[:2]]


def on_device(echoes, steering, sub_map, band_offset, interp_weight, range_frac, phase_rate):
    slabs = lax.axis_size("rng")
    subs = lax.axis_size("sub")
    segments, taps = interp_weight.shape[1], interp_weight.shape[3]
    group = 1 << segments
    groups = subs // group
    angles, pulse_count = steering.shape[1], steering.shape[2]
    half = angles // 2
    slab = lax.axis_index("rng")
    range_rows = echoes.shape[2] * subs
    rows = range_rows // group
    early, late = 2 * (segments - 1), 2

    cut = (2,) + echoes.shape[2:]
    tables_in = (band_offset, interp_weight, range_frac, phase_rate)
    *quarters, early_pack, late_pack = pl.pallas_call(
        functools.partial(cut_kernel, slabs, segments, taps, half),
        out_shape=[pltpu.VMEM(cut, jnp.bfloat16)] * slabs
        + [pltpu.VMEM((pack_rows(terms, taps), angles), jnp.bfloat16) for terms in (early, late)],
        in_specs=[FAR] * 5,
        out_specs=[WHOLE] * (slabs + 2),
        scratch_shapes=[pltpu.VMEM(value.shape, value.dtype) for value in tables_in]
        + [pltpu.SemaphoreType.DMA((slabs, 2)), pltpu.SemaphoreType.DMA((4,))],
        compiler_params=params(2),
        cost_estimate=cost(1_000_000_000),
        name="cut",
    )(*[pltpu.with_memory_space_constraint(value, pltpu.HBM) for value in (echoes,) + tables_in])

    received = [quarters[0]] + [None] * (slabs - 1)
    for mask in range(slabs - 1, 0, -1):
        received[mask] = exchanged(quarters[mask], "rng", mask)

    masks = list(range(group - 1, 1, -1))
    masks = (masks[0::2] + [1], masks[1::2] + [1])
    mine, theirs = [], []
    for step in range(len(masks[0])):
        route = []
        for s in range(subs):
            for q in range(slabs):
                route.append((s * slabs + q, (s ^ masks[q & 1][step]) * slabs + q))
        mine.append(lax.ppermute(early_pack, ("sub", "rng"), route))
    for piece in mine[:-1]:
        theirs.append(exchanged(piece, "rng", 1))

    if groups == 1:
        blocks = received
    else:
        ordered = jnp.zeros((slabs,) + received[0].shape, received[0].dtype)
        for mask, block in enumerate(received):
            ordered = lax.dynamic_update_index_in_dim(ordered, block, slab ^ mask, 0)
        every = jnp.moveaxis(ordered, 0, 2).reshape(2, -1, subs, pulse_count)
        every = jnp.take(every, sub_map, axis=2)
        every = lax.ppermute(
            every,
            "sub",
            [(old, (old % groups) * group + old // groups) for old in range(subs)],
        ).reshape(2, -1, groups, group * pulse_count)
        lanes = [[g * group + m for g in range(groups)] for m in range(group)]
        every = lax.all_to_all(every, "sub", 2, 1, axis_index_groups=lanes, tiled=True)
        blocks = [every.reshape(2, rows, group * pulse_count)]

    edge_rows = jnp.stack([block[:, :HALO] for block in blocks])
    route = []
    for number in range(subs):
        for q in range(slabs):
            if number % group > 0:
                route.append((number * slabs + q, (number - 1) * slabs + q))
            elif q > 0:
                route.append((number * slabs + q, (number + group - 1) * slabs + q - 1))
    edge = lax.ppermute(edge_rows, ("sub", "rng"), route)

    def tables(terms, sources, held, lines, arrays):
        return pl.pallas_call(
            functools.partial(
                table_kernel,
                group,
                terms,
                sources,
                taps,
                half,
                rows,
                lines,
                range_rows,
                slabs * range_rows,
            ),
            out_shape=(
                jax.ShapeDtypeStruct((held, terms, angles, angles), jnp.bfloat16),
                jax.ShapeDtypeStruct((group, terms, 2, lines, angles), jnp.float32),
            ),
            in_specs=[WHOLE] * len(arrays),
            out_specs=(WHOLE, WHOLE),
            scratch_shapes=[
                pltpu.VMEM((group, terms, taps, angles), jnp.float32),
                pltpu.VMEM((group, 3, terms, angles), jnp.float32),
                pltpu.VMEM((15, angles // 128, group * terms, 128), jnp.float32),
            ],
            compiler_params=params(4),
            cost_estimate=cost(2_000_000_000),
        )(*arrays)

    bands, waves = tables(early, masks, group, rows + 8, [early_pack, *mine, *theirs])

    cut_row = -(-rows // 2 // 16) * 16
    bounds = ((0, cut_row), (cut_row, rows - cut_row))
    pieces = [4 * count + 8 for _, count in bounds]
    upper_order, lower_order = send_order(group)
    split = [mask for mask, _ in upper_order]
    whole_masks = [mask for mask in range(group) if mask not in split]

    def merge(chunk, arrays, sizes):
        first, count = bounds[chunk]
        held = count if chunk == 1 else count + 16
        scratch = [pltpu.VMEM((group, 2, 2, held, half), jnp.float32)]
        if chunk == 1:
            scratch.append(pltpu.VMEM((group, 2, 2, 16, half), jnp.float32))
        return pl.pallas_call(
            functools.partial(
                merge_kernel,
                group,
                segments,
                chunk,
                first,
                count,
                whole_masks,
                pulse_count,
                len(blocks),
            ),
            out_shape=[jax.ShapeDtypeStruct((size, half), jnp.bfloat16) for size in sizes],
            in_specs=[WHOLE] * (len(blocks) + 4 + len(arrays)),
            out_specs=[WHOLE] * group,
            scratch_shapes=scratch
            + [pltpu.VMEM((group, 2, 2, count + 16, half), jnp.float32)] * (segments - 1),
            compiler_params=params(10),
            cost_estimate=cost(4_000_000_000),
        )(sub_map[None], *blocks, steering, bands, waves, *arrays)

    arrived = {}

    def send(mask, chunk, value):
        arrived[mask, chunk] = exchanged(value, "sub", mask)

    upper = merge(0, [], pieces[:1] * group)
    for mask, chunk in upper_order:
        send(mask, chunk, upper[mask])
    lower = merge(
        1,
        [edge] + [upper[mask] for mask in whole_masks],
        [sum(pieces) if mask in whole_masks else pieces[1] for mask in range(group)],
    )
    for mask, chunk in lower_order:
        send(mask, chunk, lower[mask])
    arrived[0, None] = lower[0]

    last_bands, last_waves = tables(late, None, 1, rows, [late_pack])
    result = None
    middle, slow = lower_order[:1], lower_order[-3:]
    for key in lower_order[1:-3]:
        (slow if key[0] == 2 else middle).append(key)
    turns = [[(0, None)] + upper_order, middle, slow]
    for chosen in turns:
        count = len(chosen)
        jobs = []
        for source, (mask, chunk) in enumerate(chosen):
            for part in (0, 1) if chunk is None else (chunk,):
                base = pieces[0] if chunk is None and part == 1 else 0
                jobs.append((source, base, mask) + bounds[part])
        previous = [] if result is None else [result]
        result = pl.pallas_call(
            functools.partial(final_kernel, jobs, count, group, rows, result is None),
            out_shape=jax.ShapeDtypeStruct((2, range_rows, angles), jnp.bfloat16),
            in_specs=[WHOLE] * (count + 2) + [FAR] * len(previous),
            out_specs=FAR,
            scratch_shapes=[
                pltpu.VMEM((len(jobs), 4, cut_row + 8, half), jnp.float32),
                pltpu.VMEM((len(jobs), 2, cut_row, angles), jnp.bfloat16),
                pltpu.SemaphoreType.DMA((len(jobs), 2)),
            ],
            input_output_aliases={count + 2: 0} if previous else {},
            compiler_params=params(6),
            cost_estimate=cost(1_000_000_000),
            name="final",
        )(*[arrived[key] for key in chosen], last_bands, last_waves, *previous)
    return result


def solution(mesh):
    in_specs = (
        P(None, None, "sub", "rng"),
        P(),
        P(),
        P("sub", None, None, None),
        P("sub", None, None, None, None),
        P("sub", None, None, None),
        P("sub", None, None, None),
    )
    return jax.shard_map(
        on_device, mesh=mesh, in_specs=in_specs, out_specs=P(None, "rng", "sub"), check_vma=False
    )
```

```python
import functools

import jax
import jax.numpy as jnp
from jax import lax
from jax.experimental import pallas as pl
from jax.experimental.pallas import tpu as pltpu
from jax.sharding import PartitionSpec as P


HALO = 8
KINDS = 6
MIB = 1 << 20
WHOLE = pl.BlockSpec(memory_space=pltpu.VMEM)
FAR = pl.BlockSpec(memory_space=pltpu.HBM)


def exchanged(block, axis, mask):
    count = lax.axis_size(axis)
    return lax.ppermute(block, axis, [(source, source ^ mask) for source in range(count)])


def params(mib):
    return pltpu.CompilerParams(vmem_limit_bytes=mib * MIB)


def cost(flops):
    return pl.CostEstimate(flops=flops, bytes_accessed=MIB, transcendentals=0)


def product(left, right):
    return (
        left[0] * right[0] - left[1] * right[1],
        left[0] * right[1] + left[1] * right[0],
    )


def pack_rows(terms, taps):
    return -(-(terms * (taps + KINDS)) // 8) * 8


def cut_kernel(slabs, splits, segments, taps, half, echoes, offset, weight, fraction, rate, *refs):
    count = slabs * len(splits)
    slices, packs = refs[:count], refs[count : count + 2]
    held, semaphores, small = refs[count + 2 : count + 6], refs[count + 6], refs[count + 7]
    group = 1 << segments
    member = lax.axis_index("sub") & (group - 1)
    slab = lax.axis_index("rng")
    loads = [
        pltpu.make_async_copy(source, target, small.at[index])
        for index, (source, target) in enumerate(zip((offset, weight, fraction, rate), held))
    ]
    copies = []
    for mask in range(slabs - 1, -1, -1):
        for index, (start, rows) in enumerate(splits):
            slot = mask * len(splits) + index
            for c in range(2):
                copies.append(
                    pltpu.make_async_copy(
                        echoes.at[c, slab ^ mask, start : start + rows],
                        slices[slot].at[c],
                        semaphores.at[slot, c],
                    )
                )
    for copy in loads + copies:
        copy.start()
    for copy in loads:
        copy.wait()
    offset, weight, fraction, rate = held
    angles = weight.shape[-1]
    for pack, chosen in ((packs[0], range(segments - 1)), (packs[1], (segments - 1,))):
        kinds = [[] for _ in range(KINDS)]
        terms = 2 * len(chosen)
        for index, segment in enumerate(chosen):
            base = ((member >> segment) & 1) * half
            kinds[0].append((offset[0, segment] - base).astype(jnp.float32))
            slot = 1
            for source, count in ((fraction, 2), (rate, 3)):
                rest = source[0, segment]
                for _ in range(count):
                    part = rest.astype(jnp.bfloat16).astype(jnp.float32)
                    kinds[slot].append(part)
                    rest = rest - part
                    slot += 1
            for child in range(2):
                term = index * 2 + child
                pack[term * taps : (term + 1) * taps, :] = weight[0, segment, child]
        rows = [piece for kind in kinds for piece in kind]
        padding = pack_rows(terms, taps) - terms * (taps + KINDS)
        if padding:
            rows.append(jnp.zeros((padding, angles), jnp.float32))
        pack[terms * taps :, :] = jnp.concatenate(rows, axis=0).astype(jnp.bfloat16)
    for copy in copies:
        copy.wait()


def table_kernel(members, terms, masks, taps, half, rows, lines, range_rows, total_range, *refs):
    steps = len(masks[0]) if masks else 0
    swapped = steps - 1 if masks else 0
    own, mine, theirs = refs[0], refs[1 : 1 + steps], refs[1 + steps : 1 + steps + swapped]
    bands, waves, weights, raw, dense = refs[1 + steps + swapped :]
    angles = bands.shape[-1]
    member = lax.axis_index("sub") & (members - 1)
    slab = lax.axis_index("rng")

    def fill(piece, section):
        values = piece[...].astype(jnp.float32)
        for term in range(terms):
            weights[section, term] = values[term * taps : (term + 1) * taps]
        start = terms * taps
        kind = [values[start + k * terms : start + (k + 1) * terms] for k in range(KINDS)]
        raw[section, 0] = kind[0]
        raw[section, 1] = kind[1] + kind[2]
        raw[section, 2] = kind[3] + kind[4] + kind[5]

    if masks:
        core = slab & 1
        fill(own, member)
        for received, holder in ((mine, core), (theirs, 1 - core)):
            for step, piece in enumerate(received):
                fill(piece, member ^ jnp.where(holder == 0, masks[0][step], masks[1][step]))
        first_row, row_step = slab * range_rows + member * rows, 0
    else:
        for section in range(members):
            fill(own, section)
        first_row, row_step = slab * range_rows, rows

    for start in range(0, members * terms, 8):
        place = slice(start, start + 8)
        sections = range(start // terms, (start + 8) // terms)

        def keep(kind, value):
            for part in range(angles // 128):
                dense[kind, part, place] = value[:, part * 128 : (part + 1) * 128]

        given = [
            jnp.concatenate([raw[section, kind] for section in sections], axis=0)
            for kind in range(3)
        ]
        keep(0, given[0])
        keep(1, given[1])
        rate = given[2]
        number = start + lax.broadcasted_iota(jnp.int32, (8, angles), 0)
        first = first_row + (number // terms) * row_step
        angle = first.astype(jnp.float32) / float(total_range) * rate
        keep(3, jnp.cos(angle))
        keep(4, jnp.sin(angle))
        angle = rate / float(total_range)
        turn = jnp.cos(angle), jnp.sin(angle)
        for power in range(5):
            keep(5 + 2 * power, turn[0])
            keep(6 + 2 * power, turn[1])
            turn = product(turn, turn)

    sub_rows = lax.broadcasted_iota(jnp.int32, (8, 128), 0)

    def entry(index, carry):
        section, term = index // terms, index % terms
        for part in range(angles // 128):
            lanes = pl.ds(part * 128, 128)

            def row(kind):
                return dense[kind, part, pl.ds(index, 1), :]

            def bands_of():
                weight = weights[section, term, :, lanes]
                offset = row(0).astype(jnp.int32)
                fraction = row(1)
                tap = sub_rows - offset
                block_of = -(tap >> 3)
                picked = jnp.take_along_axis(weight, tap & 7, axis=0)
                near, far = picked * (1.0 - fraction), picked * fraction
                for block in range(half // 16):
                    hits = [block_of == 2 * block + step for step in range(2)]
                    for source, base in ((near, 0), (far, half)):
                        pair = [jnp.where(hit, source, 0.0) for hit in hits]
                        place = slice(base + block * 16, base + (block + 1) * 16)
                        bands[section, term, place, lanes] = jnp.concatenate(pair, axis=0).astype(
                            jnp.bfloat16
                        )

            if masks:
                bands_of()
            else:
                pl.when(section == 0)(bands_of)
            wave = tuple(jnp.broadcast_to(row(3 + c), (8, 128)) for c in range(2))
            for power in range(3):
                chosen = (sub_rows >> power) & 1 == 1
                wave = product(
                    wave,
                    (
                        jnp.where(chosen, row(5 + 2 * power), 1.0),
                        jnp.where(chosen, row(6 + 2 * power), 0.0),
                    ),
                )
            eight, sixteen = (row(11), row(12)), (row(13), row(14))
            chain = [wave, product(wave, eight)]
            for block in range(lines // 8):
                wave = chain[block % 2]
                for c in range(2):
                    waves[section, term, c, block * 8 : (block + 1) * 8, lanes] = wave[c]
                chain[block % 2] = product(wave, sixteen)
        return carry

    lax.fori_loop(0, members * terms, entry, 0)


def formed(steering, re_parts, im_parts):
    rows = jnp.concatenate(re_parts + im_parts, axis=0)
    count = rows.shape[0] // 2
    by_real, by_imag = [
        lax.dot_general(
            rows, steering[c], (((1,), (1,)), ((), ())), preferred_element_type=jnp.float32
        )
        for c in range(2)
    ]
    return by_real[:count] - by_imag[count:], by_imag[:count] + by_real[count:]


def place_of(sub_map, group, slabs, slab, index):
    if slabs == 1:
        return index
    per_slab = group // slabs
    block = (slab ^ (index // per_slab)) * per_slab + index % per_slab
    number = lax.broadcasted_iota(jnp.int32, sub_map.shape, 1).astype(jnp.float32)
    return jnp.sum(jnp.where(sub_map[...] == block, number, 0.0)).astype(jnp.int32)


def form_rows(group, pulse_count, sources, first, sub_map, blocks, steering, image):
    half, count = image.shape[-1], image.shape[-2]
    per_source = group // sources
    slab = lax.axis_index("rng")

    def rows_from(parts, c, piece):
        columns = slice(piece * pulse_count, (piece + 1) * pulse_count)
        found, start = [], 0
        for part in parts:
            low, high = max(first - start, 0), min(first + count - start, part.shape[1])
            if low < high:
                found.append(part[c, low:high, columns])
            start += part.shape[1]
        return found[0] if len(found) == 1 else jnp.concatenate(found, axis=0)

    for source in range(sources):
        for start in range(0, per_source, 2):
            pieces = range(start, min(start + 2, per_source))
            parts = [[rows_from(blocks[source], c, piece) for piece in pieces] for c in range(2)]
            values = formed(steering, *parts)
            for index, piece in enumerate(pieces):
                target = place_of(sub_map, group, sources, slab, source * per_source + piece)
                for c in range(2):
                    value = values[c][index * count : (index + 1) * count]
                    for window in range(2):
                        image[target, c, window] = value[:, window * half : (window + 1) * half]


def turned(values, block, first):
    total = None
    for value, wave in values:
        part = value[block * 16 : block * 16 + 8], value[block * 16 + 8 : block * 16 + 16]
        start = first + block * 8
        turn = tuple(wave[c, start : start + 8] for c in range(2))
        term = product(turn, part)
        total = term if total is None else (total[0] + term[0], total[1] + term[1])
    return total


def contracted(rows_of, lines, matrix):
    pieces = []
    for block in range(lines // 8):
        sides = []
        for start in (block * 8, block * 8 + 1):
            both = [rows_of(c, start) for c in range(2)]
            sides.append(jnp.concatenate(both, axis=0).astype(jnp.bfloat16))
        pieces.append(jnp.concatenate(sides, axis=1))
    return jnp.dot(jnp.concatenate(pieces, axis=0), matrix, preferred_element_type=jnp.float32)


def merge_kernel(
    group, segments, chunk, first, rows, whole, pulse_count, sources, split_count, sub_map, *refs
):
    count = sources * (1 if chunk == 0 else split_count)
    blocks, refs = refs[:count], refs[count:]
    per = count // sources
    blocks = [blocks[index * per : (index + 1) * per] for index in range(sources)]
    steering, bands, waves, refs = refs[0], refs[1], refs[2], refs[3:]
    if chunk == 1:
        edge, kept, refs = refs[0], dict(zip(whole, refs[1:])), refs[1 + len(whole) :]
    outs, image, refs = refs[:group], refs[group], refs[group + 1 :]
    if chunk == 1:
        edges, refs = refs[0], refs[1:]
    stores = refs
    form_rows(group, pulse_count, sources, first, sub_map, blocks, steering, image)
    half = image.shape[-1]
    member = lax.axis_index("sub") & (group - 1)
    per_source = group // sources

    if chunk == 1:
        below = lax.axis_index("rng")
        if sources > 1:
            below = jnp.minimum(below + jnp.where(member == group - 1, 1, 0), sources - 1)
        parts = [[], []]
        for source in range(sources):
            for piece in range(per_source):
                columns = slice(piece * pulse_count, (piece + 1) * pulse_count)
                for c in range(2):
                    parts[c].append(edge[source, c, :, columns])
        values = formed(steering, *parts)
        for index in range(group):
            target = place_of(sub_map, group, sources, below, index)
            for c in range(2):
                value = values[c][index * HALO : (index + 1) * HALO]
                for window in range(2):
                    edges[target, c, window, 0:HALO] = value[:, window * half : (window + 1) * half]
                    edges[target, c, window, HALO:] = jnp.zeros((8, half), jnp.float32)

    def rows_of(segment, section, window, c, start):
        if segment > 0:
            return stores[segment - 1][section, c, window, start : start + 8]
        if chunk == 0 or start + 8 <= rows:
            return image[section, c, window, start : start + 8]
        if start >= rows:
            return edges[section, c, window, start - rows : start - rows + 8]
        return jnp.concatenate(
            [
                image[section, c, window, start:rows],
                edges[section, c, window, 0 : start + 8 - rows],
            ],
            axis=0,
        )

    for segment in range(segments - 1):

        def step(section, carry, segment=segment):
            low = section & ~(1 << segment)
            window = (section >> segment) & 1
            values = []
            for child in range(2):
                source, term = low | (child << segment), segment * 2 + child
                reader = functools.partial(rows_of, segment, source, window)
                value = contracted(reader, rows + 8, bands[section, term])
                values.append((value, waves.at[section, term]))
            for block in range(rows // 8 + 1):
                for c, total in enumerate(turned(values, block, first)):
                    for side in range(2):
                        stores[segment][section, c, side, block * 8 : block * 8 + 8] = total[
                            :, side * half : (side + 1) * half
                        ]
            for c in range(2):
                for side in range(2):
                    stores[segment][section, c, side, rows + 8 :] = jnp.zeros(
                        (8, half), jnp.float32
                    )
            return carry

        lax.fori_loop(0, group, step, 0, unroll=4)

    last = stores[segments - 2]
    size = 4 * rows + 8
    for mask in range(group):
        section = member ^ mask
        low = section & ~(1 << (segments - 1))
        window = (section >> (segments - 1)) & 1
        base = 0
        if chunk == 1 and mask in whole:
            base = kept[mask].shape[0]
            outs[mask][0:base] = kept[mask][...]
        extra = []
        for child in range(2):
            for c in range(2):
                start = base + (child * 2 + c) * rows
                source = last.at[low | (child << (segments - 1)), c, window]
                outs[mask][start : start + rows] = source[0:rows].astype(jnp.bfloat16)
                extra.append(source[rows : rows + 1])
        extra.append(jnp.zeros((4, half), jnp.float32))
        outs[mask][base + 4 * rows : base + size] = jnp.concatenate(extra, axis=0).astype(
            jnp.bfloat16
        )


def final_kernel(jobs, count, group, block_rows, fresh, *refs):
    parts, (bands, waves) = refs[:count], refs[count : count + 2]
    result, store, mine, semaphores = refs[count + (2 if fresh else 3) :]
    half = store.shape[-1]
    member = lax.axis_index("sub") & (group - 1)
    copies = []
    for index, (source, base, mask, first, rows) in enumerate(jobs):
        part = parts[source]
        extra = part[base + 4 * rows : base + 4 * rows + 8].astype(jnp.float32)
        for side in range(4):
            start = base + side * rows
            store[index, side, 0:rows] = part[start : start + rows].astype(jnp.float32)
            store[index, side, rows : rows + 8] = jnp.broadcast_to(extra[side : side + 1], (8, half))
        values = []
        for child in range(2):

            def rows_of(c, start, index=index, child=child):
                return store[index, child * 2 + c, start : start + 8]

            value = contracted(rows_of, rows, bands[0, child])
            values.append((value, waves.at[member ^ mask, child]))
        held = None
        for block in range(rows // 8):
            totals = turned(values, block, first)
            if block % 2 == 0:
                held = totals
                continue
            for c in range(2):
                mine[index, c, block * 8 - 8 : block * 8 + 8] = jnp.concatenate(
                    [held[c], totals[c]], axis=0
                ).astype(jnp.bfloat16)
        start = pl.multiple_of((member ^ mask) * block_rows + first, 16)
        for c in range(2):
            copy = pltpu.make_async_copy(
                mine.at[index, c, 0:rows], result.at[c, pl.ds(start, rows)], semaphores.at[index, c]
            )
            copy.start()
            copies.append(copy)
    for copy in copies:
        copy.wait()


def send_order(group):
    far, near = list(range(group - 1, group // 2 - 1, -1)), list(range(group // 2 - 1, 0, -1))
    upper = [(mask, 0) for mask in far[:2]]
    rest = [(mask, None) for mask in far[2:3] + near + far[3:]]
    return upper, rest + [(mask, 1) for mask in far[:2]]


def on_device(echoes, steering, sub_map, band_offset, interp_weight, range_frac, phase_rate):
    slabs = lax.axis_size("rng")
    subs = lax.axis_size("sub")
    segments, taps = interp_weight.shape[1], interp_weight.shape[3]
    group = 1 << segments
    groups = subs // group
    angles, pulse_count = steering.shape[1], steering.shape[2]
    half = angles // 2
    slab = lax.axis_index("rng")
    range_rows = echoes.shape[2] * subs
    rows = range_rows // group
    early, late = 2 * (segments - 1), 2

    cut_row = -(-rows // 2 // 16) * 16
    splits = ((0, echoes.shape[2]),)
    if groups == 1:
        splits = ((0, cut_row + 16), (cut_row + 16, rows - cut_row - 16))
    shapes = [(2, count, echoes.shape[3]) for _, count in splits]
    tables_in = (band_offset, interp_weight, range_frac, phase_rate)
    *slices, early_pack, late_pack = pl.pallas_call(
        functools.partial(cut_kernel, slabs, splits, segments, taps, half),
        out_shape=[pltpu.VMEM(shape, jnp.bfloat16) for shape in shapes] * slabs
        + [pltpu.VMEM((pack_rows(terms, taps), angles), jnp.bfloat16) for terms in (early, late)],
        in_specs=[FAR] * 5,
        out_specs=[WHOLE] * (slabs * len(splits) + 2),
        scratch_shapes=[pltpu.VMEM(value.shape, value.dtype) for value in tables_in]
        + [pltpu.SemaphoreType.DMA((slabs * len(splits), 2)), pltpu.SemaphoreType.DMA((4,))],
        compiler_params=params(2),
        cost_estimate=cost(1_000_000_000),
        name="cut",
    )(*[pltpu.with_memory_space_constraint(value, pltpu.HBM) for value in (echoes,) + tables_in])

    received = []
    for part in range(len(splits)):
        arrays = [slices[mask * len(splits) + part] for mask in range(slabs)]
        for mask in range(slabs - 1, 0, -1):
            arrays[mask] = exchanged(arrays[mask], "rng", mask)
        received.append(arrays)

    masks = list(range(group - 1, 1, -1))
    masks = (masks[0::2] + [1], masks[1::2] + [1])
    mine, theirs = [], []
    for step in range(len(masks[0])):
        route = []
        for s in range(subs):
            for q in range(slabs):
                route.append((s * slabs + q, (s ^ masks[q & 1][step]) * slabs + q))
        mine.append(lax.ppermute(early_pack, ("sub", "rng"), route))
    for piece in mine[:-1]:
        theirs.append(exchanged(piece, "rng", 1))

    if groups == 1:
        blocks = list(zip(*received))
    else:
        ordered = jnp.zeros((slabs,) + received[0][0].shape, jnp.bfloat16)
        for mask, block in enumerate(received[0]):
            ordered = lax.dynamic_update_index_in_dim(ordered, block, slab ^ mask, 0)
        every = jnp.moveaxis(ordered, 0, 2).reshape(2, -1, subs, pulse_count)
        every = jnp.take(every, sub_map, axis=2)
        every = lax.ppermute(
            every,
            "sub",
            [(old, (old % groups) * group + old // groups) for old in range(subs)],
        ).reshape(2, -1, groups, group * pulse_count)
        lanes = [[g * group + m for g in range(groups)] for m in range(group)]
        every = lax.all_to_all(every, "sub", 2, 1, axis_index_groups=lanes, tiled=True)
        blocks = [(every.reshape(2, rows, group * pulse_count),)]

    edge_rows = jnp.stack([block[0][:, :HALO] for block in blocks])
    route = []
    for number in range(subs):
        for q in range(slabs):
            if number % group > 0:
                route.append((number * slabs + q, (number - 1) * slabs + q))
            elif q > 0:
                route.append((number * slabs + q, (number + group - 1) * slabs + q - 1))
    edge = lax.ppermute(edge_rows, ("sub", "rng"), route)

    def tables(terms, sources, held, lines, arrays):
        return pl.pallas_call(
            functools.partial(
                table_kernel,
                group,
                terms,
                sources,
                taps,
                half,
                rows,
                lines,
                range_rows,
                slabs * range_rows,
            ),
            out_shape=(
                jax.ShapeDtypeStruct((held, terms, angles, angles), jnp.bfloat16),
                jax.ShapeDtypeStruct((group, terms, 2, lines, angles), jnp.float32),
            ),
            in_specs=[WHOLE] * len(arrays),
            out_specs=(WHOLE, WHOLE),
            scratch_shapes=[
                pltpu.VMEM((group, terms, taps, angles), jnp.float32),
                pltpu.VMEM((group, 3, terms, angles), jnp.float32),
                pltpu.VMEM((15, angles // 128, group * terms, 128), jnp.float32),
            ],
            compiler_params=params(4),
            cost_estimate=cost(2_000_000_000),
        )(*arrays)

    bands, waves = tables(early, masks, group, rows + 8, [early_pack, *mine, *theirs])

    bounds = ((0, cut_row), (cut_row, rows - cut_row))
    pieces = [4 * count + 8 for _, count in bounds]
    upper_order, lower_order = send_order(group)
    split = [mask for mask, _ in upper_order]
    whole_masks = [mask for mask in range(group) if mask not in split]

    def merge(chunk, arrays, sizes):
        first, count = bounds[chunk]
        held = count if chunk == 1 else count + 16
        used = [parts[:1] if chunk == 0 else parts for parts in blocks]
        given = [part for parts in used for part in parts]
        scratch = [pltpu.VMEM((group, 2, 2, held, half), jnp.float32)]
        if chunk == 1:
            scratch.append(pltpu.VMEM((group, 2, 2, 16, half), jnp.float32))
        return pl.pallas_call(
            functools.partial(
                merge_kernel,
                group,
                segments,
                chunk,
                first,
                count,
                whole_masks,
                pulse_count,
                len(blocks),
                len(splits),
            ),
            out_shape=[jax.ShapeDtypeStruct((size, half), jnp.bfloat16) for size in sizes],
            in_specs=[WHOLE] * (len(given) + 4 + len(arrays)),
            out_specs=[WHOLE] * group,
            scratch_shapes=scratch
            + [pltpu.VMEM((group, 2, 2, count + 16, half), jnp.float32)] * (segments - 1),
            compiler_params=params(10),
            cost_estimate=cost(4_000_000_000),
        )(sub_map[None], *given, steering, bands, waves, *arrays)

    arrived = {}

    def send(mask, chunk, value):
        arrived[mask, chunk] = exchanged(value, "sub", mask)

    upper = merge(0, [], pieces[:1] * group)
    for mask, chunk in upper_order:
        send(mask, chunk, upper[mask])
    lower = merge(
        1,
        [edge] + [upper[mask] for mask in whole_masks],
        [sum(pieces) if mask in whole_masks else pieces[1] for mask in range(group)],
    )
    for mask, chunk in lower_order:
        send(mask, chunk, lower[mask])
    arrived[0, None] = lower[0]

    last_bands, last_waves = tables(late, None, 1, rows, [late_pack])
    result = None
    middle, slow = lower_order[:1], lower_order[-3:]
    for key in lower_order[1:-3]:
        (slow if key[0] == 2 else middle).append(key)
    turns = [[(0, None)] + upper_order, middle, slow]
    for chosen in turns:
        count = len(chosen)
        jobs = []
        for source, (mask, chunk) in enumerate(chosen):
            for part in (0, 1) if chunk is None else (chunk,):
                base = pieces[0] if chunk is None and part == 1 else 0
                jobs.append((source, base, mask) + bounds[part])
        previous = [] if result is None else [result]
        result = pl.pallas_call(
            functools.partial(final_kernel, jobs, count, group, rows, result is None),
            out_shape=jax.ShapeDtypeStruct((2, range_rows, angles), jnp.bfloat16),
            in_specs=[WHOLE] * (count + 2) + [FAR] * len(previous),
            out_specs=FAR,
            scratch_shapes=[
                pltpu.VMEM((len(jobs), 4, cut_row + 8, half), jnp.float32),
                pltpu.VMEM((len(jobs), 2, cut_row, angles), jnp.bfloat16),
                pltpu.SemaphoreType.DMA((len(jobs), 2)),
            ],
            input_output_aliases={count + 2: 0} if previous else {},
            compiler_params=params(6),
            cost_estimate=cost(1_000_000_000),
            name="final",
        )(*[arrived[key] for key in chosen], last_bands, last_waves, *previous)
    return result


def solution(mesh):
    in_specs = (
        P(None, None, "sub", "rng"),
        P(),
        P(),
        P("sub", None, None, None),
        P("sub", None, None, None, None),
        P("sub", None, None, None),
        P("sub", None, None, None),
    )
    return jax.shard_map(
        on_device, mesh=mesh, in_specs=in_specs, out_specs=P(None, "rng", "sub"), check_vma=False
    )
```
